32 devices in a mesh: my: 8 (over z, y), mx: 4 (over x, core).
Axes of the slice: x: 2, y: 2, z: 4, core: 2. Of those that a mesh axis runs over, the one named last changes fastest.
Arguments:
- x_in: bfloat16 [192, 5120], P(None, 'mx')
- seq_lens: int32 [192], P('mx')
- gain_attn: bfloat16 [5120], P('mx')
- gain_mlp: bfloat16 [5120], P('mx')
- w_q: bfloat16 [5120, 5120], P('mx', 'my')
- b_q: bfloat16 [5120], P('my')
- w_k: bfloat16 [5120, 1024], P('mx', 'my')
- b_k: bfloat16 [1024], P('my')
- w_v: bfloat16 [5120, 1024], P('mx', 'my')
- b_v: bfloat16 [1024], P('my')
- w_o: bfloat16 [5120, 5120], P('my', 'mx')
- w_gate: bfloat16 [5120, 27392], P('mx', 'my')
- w_up: bfloat16 [5120, 27392], P('mx', 'my')
- w_down: bfloat16 [27392, 5120], P('my', 'mx')
- k_cache: bfloat16 [192, 384, 8, 128], P('mx', None, 'my')
- v_cache: bfloat16 [192, 384, 8, 128], P('mx', None, 'my')
Outputs:
- output 1: bfloat16 [192, 5120], P(None, 'mx')
- output 2: bfloat16 [192, 384, 8, 128], P('mx', None, 'my')
- output 3: bfloat16 [192, 384, 8, 128], P('mx', None, 'my')
All inputs are finite; a program needn't handle non-finite values.
Results may differ from the reference program's by a relative error of at most 0.0177699.
Values are sent between devices in bfloat16 or wider.
A program may use at most 1 GiB of HBM per device.

```python
import jax
import jax.numpy as jnp
from jax import lax

D = 5120
HEADS = 40
KV_HEADS = 8
HEAD = 128
FF = 27392
BATCH = 192
SEQ = 384
NORM_EPS = 1e-6
ROPE_THETA = 1000000.0
GROUP = HEADS // KV_HEADS


def setup_inputs(seed: int = 0) -> dict:
    key_list = jax.random.split(jax.random.key(seed), 17)
    q_width = HEADS * HEAD
    kv_width = KV_HEADS * HEAD
    cache_shape = (BATCH, SEQ, KV_HEADS, HEAD)

    def normal(key_index, shape, scale, offset=0.0):
        samples = jax.random.normal(key_list[key_index], shape, jnp.float32)
        return (offset + scale * samples).astype(jnp.bfloat16)

    lens_draw = jax.random.randint(key_list[0], (BATCH,), 0, SEQ)
    full_row = jax.random.randint(key_list[1], (), 0, BATCH)
    seq_lens = jnp.where(jnp.arange(BATCH) == full_row, SEQ - 1, lens_draw).astype(jnp.int32)
    return {
        "x_in": normal(2, (BATCH, D), 1.0),
        "seq_lens": seq_lens,
        "gain_attn": normal(3, (D,), 0.3, 1.0),
        "gain_mlp": normal(4, (D,), 0.3, 1.0),
        "w_q": normal(5, (D, q_width), 2.0 * D ** -0.5),
        "b_q": normal(6, (q_width,), 1.0),
        "w_k": normal(7, (D, kv_width), D ** -0.5),
        "b_k": normal(8, (kv_width,), 1.0),
        "w_v": normal(9, (D, kv_width), D ** -0.5),
        "b_v": normal(10, (kv_width,), 1.0),
        "w_o": normal(11, (q_width, D), q_width ** -0.5),
        "w_gate": normal(12, (D, FF), D ** -0.5),
        "w_up": normal(13, (D, FF), D ** -0.5),
        "w_down": normal(14, (FF, D), FF ** -0.5),
        "k_cache": normal(15, cache_shape, 1.0),
        "v_cache": normal(16, cache_shape, 1.0),
    }


def rms_norm(rows_in, gain_vec):
    rows_f32 = rows_in.astype(jnp.float32)
    mean_sq = jnp.mean(rows_f32 * rows_f32, axis=-1, keepdims=True)
    return (rows_f32 * lax.rsqrt(mean_sq + NORM_EPS) * gain_vec.astype(jnp.float32)).astype(jnp.bfloat16)


def apply_rotary(vectors, positions):
    half_dim = HEAD // 2
    inv_freq = ROPE_THETA ** (-2.0 * jnp.arange(half_dim, dtype=jnp.float32) / HEAD)
    angles = positions.astype(jnp.float32)[:, None, None] * inv_freq
    cos_tab = jnp.cos(angles)
    sin_tab = jnp.sin(angles)
    lower_half = vectors[..., :half_dim]
    upper_half = vectors[..., half_dim:]
    return jnp.concatenate([lower_half * cos_tab - upper_half * sin_tab, upper_half * cos_tab + lower_half * sin_tab], axis=-1)


def attend_one(row_inputs):
    q_row, k_rows, v_rows, length = row_inputs
    q_grouped = q_row.reshape(KV_HEADS, GROUP, HEAD).astype(jnp.float32)
    scores = jnp.einsum("kgd,skd->kgs", q_grouped, k_rows.astype(jnp.float32)) * HEAD ** -0.5
    visible = (jnp.arange(SEQ) <= length)[None, None, :]
    scores = jnp.where(visible, scores, -jnp.inf)
    weights = jnp.exp(scores - jnp.max(scores, axis=-1, keepdims=True))
    weight_sum = jnp.sum(weights, axis=-1, keepdims=True)
    weighted = jnp.einsum("kgs,skd->kgd", weights.astype(jnp.bfloat16).astype(jnp.float32), v_rows.astype(jnp.float32))
    return (weighted / weight_sum).astype(jnp.bfloat16).reshape(HEADS * HEAD)


def reference(x_in, seq_lens, gain_attn, gain_mlp, w_q, b_q, w_k, b_k, w_v, b_v, w_o, w_gate, w_up, w_down, k_cache, v_cache):
    normed = rms_norm(x_in, gain_attn)
    q_vals = jnp.dot(normed, w_q, preferred_element_type=jnp.float32) + b_q.astype(jnp.float32)
    k_vals = jnp.dot(normed, w_k, preferred_element_type=jnp.float32) + b_k.astype(jnp.float32)
    v_vals = jnp.dot(normed, w_v, preferred_element_type=jnp.float32) + b_v.astype(jnp.float32)
    q_rot = apply_rotary(q_vals.reshape(BATCH, HEADS, HEAD), seq_lens).astype(jnp.bfloat16)
    k_rot = apply_rotary(k_vals.reshape(BATCH, KV_HEADS, HEAD), seq_lens).astype(jnp.bfloat16)
    v_new = v_vals.reshape(BATCH, KV_HEADS, HEAD).astype(jnp.bfloat16)
    at_slot = (jnp.arange(SEQ)[None, :] == seq_lens[:, None])[:, :, None, None]
    k_cache_out = jnp.where(at_slot, k_rot[:, None], k_cache)
    v_cache_out = jnp.where(at_slot, v_new[:, None], v_cache)
    attn_rows = lax.map(attend_one, (q_rot, k_cache_out, v_cache_out, seq_lens))
    x_mid = (x_in.astype(jnp.float32) + jnp.dot(attn_rows, w_o, preferred_element_type=jnp.float32)).astype(jnp.bfloat16)
    normed_mlp = rms_norm(x_mid, gain_mlp)
    gate_proj = jnp.dot(normed_mlp, w_gate, preferred_element_type=jnp.float32)
    up_proj = jnp.dot(normed_mlp, w_up, preferred_element_type=jnp.float32)
    hidden_act = (jax.nn.silu(gate_proj) * up_proj).astype(jnp.bfloat16)
    x_out = (x_mid.astype(jnp.float32) + jnp.dot(hidden_act, w_down, preferred_element_type=jnp.float32)).astype(jnp.bfloat16)
    return (x_out, k_cache_out, v_cache_out)
```

```python
import functools

import jax
import jax.numpy as jnp
from jax import lax
from jax.experimental import pallas as pl
from jax.experimental.pallas import tpu as pltpu
from jax.sharding import PartitionSpec as P

HEAD = 128
NORM_EPS = 1e-6
ROPE_THETA = 1000000.0
MESH = pl.DeviceIdType.MESH
CHUNK = 512
ROWS = 64
LAG_B, LAG_C, LAG_D, LAG_E = 1, 4, 7, 8
VMEM_LIMIT = 66 * 1024 * 1000


def rcopy(src, dst, send_sem, recv_sem, dev):
    return pltpu.make_async_remote_copy(src_ref=src, dst_ref=dst, send_sem=send_sem, recv_sem=recv_sem, device_id=dev, device_id_type=MESH)


def lane_ids():
    return lax.broadcasted_iota(jnp.int32, (8, 128), 1)


def pack_column(blocks):
    tile = jnp.zeros((8, 128), jnp.float32)
    lanes = lane_ids()
    for k, block in enumerate(blocks):
        tile = jnp.where(lanes == k, block, tile)
    return tile


def unpack_column(tile, k):
    return jnp.sum(jnp.where(lane_ids() == k, tile, 0.0), axis=1, keepdims=True)


def qkv_kernel(hidden, x_hbm, gain_ref, wq_hbm, wk_hbm, wv_hbm, out_ref, x_v, wq_v, wk_v, wv_v, st_own, st_in, nrm, pp, dr, own, xs, xr, ld_sem, send_sem, st_sem, d_sem, x_sem):
    mx = lax.axis_index("mx")
    xi, ci = mx // 2, mx % 2
    partner, xpeer = 2 * xi + (1 - ci), 2 * (1 - xi) + ci
    loads = [pltpu.make_async_copy(s, d, ld_sem.at[i]) for i, (s, d) in enumerate([(x_hbm, x_v), (wq_hbm, wq_v), (wk_hbm, wk_v), (wv_hbm, wv_v)])]
    for ld in loads:
        ld.start()
    barrier = pltpu.get_barrier_semaphore()
    for d in range(1, 4):
        pl.semaphore_signal(barrier, inc=1, device_id={"mx": (mx + d) % 4}, device_id_type=MESH)
    pl.semaphore_wait(barrier, 3)

    rows = x_v.shape[0]
    loads[0].wait()
    blocks = []
    for k in range(rows // 8):
        v = x_v[8 * k:8 * k + 8, :].astype(jnp.float32)
        blocks.append(jnp.sum(v * v, axis=1, keepdims=True))
    tile = pack_column(blocks)
    st_own[...] = tile
    st_in[mx] = tile
    for d in range(1, 4):
        rcopy(st_own, st_in.at[mx], send_sem.at[0], st_sem, {"mx": (mx + d) % 4}).start()
    for ld in loads[1:]:
        ld.wait()
    rcopy(st_in.at[pl.ds(0, 3)], st_in.at[pl.ds(0, 3)], send_sem.at[0], st_sem, {"mx": partner}).wait()
    total = st_in[0] + st_in[1] + st_in[2] + st_in[3]
    scale = lax.rsqrt(total / hidden + NORM_EPS)
    gain = gain_ref[...].astype(jnp.float32)
    for k in range(0, rows // 8, 2):
        col = jnp.concatenate([unpack_column(scale, k), unpack_column(scale, k + 1)], axis=0)
        nrm[8 * k:8 * k + 16, :] = (x_v[8 * k:8 * k + 16, :].astype(jnp.float32) * col * gain).astype(jnp.bfloat16)

    lhs = nrm[...]
    part = rows // 4
    off = 0
    for w in (wq_v, wk_v, wv_v):
        width = w.shape[1]
        for c0 in range(0, width, 256):
            cw = min(256, width - c0)
            r = jnp.dot(lhs, w[:, c0:c0 + cw], preferred_element_type=jnp.float32).astype(jnp.bfloat16)
            for m in range(4):
                pp[m % 2, m // 2, :, off + c0:off + c0 + cw] = r[m * part:(m + 1) * part]
        off += width
    rcopy(pp.at[1 - ci], dr, send_sem.at[1], d_sem, {"mx": partner}).start()
    rcopy(pp.at[1 - ci], dr, send_sem.at[1], d_sem, {"mx": partner}).wait_recv()
    xs[...] = (pp[ci, 1 - xi].astype(jnp.float32) + dr[1 - xi].astype(jnp.float32)).astype(jnp.bfloat16)
    out = rcopy(xs, xr, send_sem.at[2], x_sem, {"mx": xpeer})
    out.start()
    own[...] = pp[ci, xi].astype(jnp.float32) + dr[xi].astype(jnp.float32)
    out.wait_recv()
    out_ref[...] = own[...] + xr[...].astype(jnp.float32)
    out.wait_send()
    rcopy(pp.at[1 - ci], dr, send_sem.at[1], d_sem, {"mx": partner}).wait_send()


def qkv_call(x_in, gain, w_q, w_k, w_v, hidden):
    rows, cols = x_in.shape
    width = w_q.shape[1] + w_k.shape[1] + w_v.shape[1]
    bf, f32 = jnp.bfloat16, jnp.float32
    any_spec, vmem = pl.BlockSpec(memory_space=pl.ANY), pl.BlockSpec(memory_space=pltpu.VMEM)
    part = rows // 4
    return pl.pallas_call(
        functools.partial(qkv_kernel, hidden),
        name="qkv",
        out_shape=jax.ShapeDtypeStruct((part, width), f32),
        in_specs=[any_spec, vmem, any_spec, any_spec, any_spec],
        out_specs=vmem,
        scratch_shapes=[
            pltpu.VMEM((rows, cols), bf), pltpu.VMEM(w_q.shape, bf), pltpu.VMEM(w_k.shape, bf), pltpu.VMEM(w_v.shape, bf),
            pltpu.VMEM((8, 128), f32), pltpu.VMEM((4, 8, 128), f32), pltpu.VMEM((rows, cols), bf),
            pltpu.VMEM((2, 2, part, width), bf), pltpu.VMEM((2, part, width), bf), pltpu.VMEM((part, width), f32),
            pltpu.VMEM((part, width), bf), pltpu.VMEM((part, width), bf),
            pltpu.SemaphoreType.DMA((4,)), pltpu.SemaphoreType.DMA((3,)), pltpu.SemaphoreType.DMA, pltpu.SemaphoreType.DMA, pltpu.SemaphoreType.DMA,
        ],
        compiler_params=pltpu.CompilerParams(collective_id=0, has_side_effects=True, vmem_limit_bytes=32 * 1024 * 1024),
    )(x_in, gain, w_q, w_k, w_v)


def mlp_kernel(hidden, x_hbm, gain_ref, attn_ref, wo_hbm, wg_hbm, wu_hbm, wd_hbm, out_ref,
               x_v, wo_v, wg_v, wu_v, wd_v, attn_v, p1, rs1, mp, ag1, st_own, st_in, h2,
               pp, dr, own, xs, xr, act, dacc, p2, rs2, mo, ag2,
               ld_sem, send_sem, at_sem, rs1_sem, ag1_sem, st_sem, rs2_sem, ag2_sem, d_sem, x_sem, ax_sem, ad_sem, af_sem):
    my, mx = lax.axis_index("my"), lax.axis_index("mx")
    n_my = 8
    xi, ci = mx // 2, mx % 2
    zi, yi = my // 2, my % 2
    partner, xpeer = 2 * xi + (1 - ci), 2 * (1 - xi) + ci
    core_dev, x_dev = {"mx": partner}, {"mx": xpeer}
    n_h = h2.shape[0]
    ff = wg_v.shape[1]
    n_j = pl.cdiv(ff, CHUNK)
    tail = ff - CHUNK * (n_j - 1)
    steps = n_h * n_j
    half = x_v.shape[1] // 2
    brows = attn_ref.shape[0]
    f32, bf = jnp.float32, jnp.bfloat16

    loads = [pltpu.make_async_copy(s, d, ld_sem.at[i]) for i, (s, d) in enumerate([
        (wo_hbm, wo_v), (x_hbm, x_v), (wg_hbm, wg_v), (wu_hbm, wu_v), (wd_hbm, wd_v.at[pl.ds(0, ff)])])]
    for ld in loads:
        ld.start()
    barrier = pltpu.get_barrier_semaphore()
    for d in range(1, 4):
        pl.semaphore_signal(barrier, inc=1, device_id={"mx": (mx + d) % 4}, device_id_type=MESH)
    for d in range(1, n_my):
        pl.semaphore_signal(barrier, inc=1, device_id={"my": (my + d) % n_my}, device_id_type=MESH)
    pl.semaphore_wait(barrier, 3 + n_my - 1)

    my_rows = pl.ds(pl.multiple_of(mx * brows, 16), brows)
    for d in range(1, 4):
        rcopy(attn_ref, attn_v.at[my_rows], send_sem.at[0], at_sem, {"mx": (mx + d) % 4}).start()
    attn_v[my_rows, :] = attn_ref[...]
    dacc[...] = jnp.zeros_like(dacc)
    wd_v[ff:, :] = jnp.zeros((wd_v.shape[0] - ff, wd_v.shape[1]), bf)
    loads[0].wait()
    gathered = attn_v.at[pl.ds(0, 3 * brows)]
    rcopy(gathered, gathered, send_sem.at[0], at_sem, core_dev).wait()

    for y in range(2):
        r = jnp.dot(attn_v[...], wo_v[:, y * half:(y + 1) * half], preferred_element_type=f32).astype(bf)
        for h in range(n_h):
            for z in range(4):
                r0 = h * ROWS + z * 16
                p1[h, 2 * z + y] = r[r0:r0 + 16]

    def send_rs(p, rs, h, ssem, rsem):
        for d in range(1, n_my):
            peer = (my + d) % n_my
            rcopy(p.at[h, peer], rs.at[h, d - 1], ssem, rsem.at[h], {"my": peer}).start()

    def finish_rs(p, rs, h, ssem, rsem, base):
        rcopy(rs.at[h], rs.at[h], ssem, rsem.at[h], {"my": my}).wait_recv()
        total = p[h, my].astype(f32)
        for i in range(n_my - 1):
            total += rs[h, i].astype(f32)
        return (base + total).astype(bf)

    def send_ag(piece, ag, h, ssem, rsem):
        for d in range(1, n_my):
            rcopy(piece.at[h], ag.at[h, my], ssem, rsem.at[h], {"my": (my + d) % n_my}).start()

    def wait_ag(ag, h, ssem, rsem):
        seven = ag.at[h, pl.ds(0, n_my - 1)]
        rcopy(seven, seven, ssem, rsem.at[h], {"my": my}).wait_recv()

    def rs1_send(h):
        send_rs(p1, rs1, h, send_sem.at[1], rs1_sem)

    def rs1_finish(h):
        r0 = pl.multiple_of(h * ROWS + zi * 16, 16)
        base = x_v[pl.ds(r0, 16), pl.ds(pl.multiple_of(yi * half, 128), half)].astype(f32)
        m = finish_rs(p1, rs1, h, send_sem.at[1], rs1_sem, base)
        mp[h] = m
        ag1[h, my] = m
        send_ag(mp, ag1, h, send_sem.at[2], ag1_sem)

    def stat_send(h):
        wait_ag(ag1, h, send_sem.at[2], ag1_sem)
        blocks = []
        for z in range(4):
            a, b = ag1[h, 2 * z].astype(f32), ag1[h, 2 * z + 1].astype(f32)
            ss = jnp.sum(a * a, axis=1, keepdims=True) + jnp.sum(b * b, axis=1, keepdims=True)
            blocks += [ss[:8], ss[8:]]
        tile = pack_column(blocks)
        st_own[h] = tile
        st_in[h, mx] = tile
        for d in range(1, 4):
            rcopy(st_own.at[h], st_in.at[h, mx], send_sem.at[3], st_sem.at[h], {"mx": (mx + d) % 4}).start()

    def norm(h):
        three = st_in.at[h, pl.ds(0, 3)]
        rcopy(three, three, send_sem.at[3], st_sem.at[h], core_dev).wait_recv()
        total = st_in[h, 0] + st_in[h, 1] + st_in[h, 2] + st_in[h, 3]
        scale = lax.rsqrt(total / hidden + NORM_EPS)
        for z in range(4):
            col = jnp.concatenate([unpack_column(scale, 2 * z), unpack_column(scale, 2 * z + 1)], axis=0)
            for y in range(2):
                gain = gain_ref[:, y * half:(y + 1) * half].astype(f32)
                h2[h, 16 * z:16 * z + 16, y * half:(y + 1) * half] = (ag1[h, 2 * z + y].astype(f32) * col * gain).astype(bf)

    def stage_a(s):
        h, j = s // n_j, s % n_j

        def put(val, lo, width):
            for m in range(4):
                pp[s, m % 2, m // 2, :, lo:lo + width] = val[16 * m:16 * m + 16]

        @pl.when(j < n_j - 1)
        def _():
            cols = pl.ds(pl.multiple_of(j * CHUNK, CHUNK), CHUNK)
            lhs = h2[h]
            put(jnp.dot(lhs, wg_v[:, cols], preferred_element_type=f32).astype(bf), 0, CHUNK)
            put(jnp.dot(lhs, wu_v[:, cols], preferred_element_type=f32).astype(bf), CHUNK, CHUNK)

        @pl.when(j == n_j - 1)
        def _():
            lhs = h2[h]
            fill = (tail // 128) * 128
            for i, w in enumerate((wg_v, wu_v)):
                if fill < CHUNK:
                    put(jnp.zeros((ROWS, CHUNK - fill), bf), i * CHUNK + fill, CHUNK - fill)
                put(jnp.dot(lhs, w[:, CHUNK * (n_j - 1):ff], preferred_element_type=f32).astype(bf), i * CHUNK, tail)

        rcopy(pp.at[s, 1 - ci], dr.at[s], send_sem.at[4], d_sem.at[s], core_dev).start()

    def stage_b(s):
        rcopy(pp.at[s, 1 - ci], dr.at[s], send_sem.at[4], d_sem.at[s], core_dev).wait_recv()
        xs[s] = (pp[s, ci, 1 - xi].astype(f32) + dr[s, 1 - xi].astype(f32)).astype(bf)
        rcopy(xs.at[s], xr.at[s], send_sem.at[5], x_sem.at[s], x_dev).start()
        own[s] = pp[s, ci, xi].astype(f32) + dr[s, xi].astype(f32)

    def stage_c(s):
        rcopy(xs.at[s], xr.at[s], send_sem.at[5], x_sem.at[s], x_dev).wait_recv()
        g = own[s, :, :CHUNK] + xr[s, :, :CHUNK].astype(f32)
        u = own[s, :, CHUNK:] + xr[s, :, CHUNK:].astype(f32)
        act[s, mx] = (jax.nn.silu(g) * u).astype(bf)
        rcopy(act.at[s, mx], act.at[s, mx], send_sem.at[6], ax_sem.at[s], x_dev).start()
        rcopy(act.at[s, mx], act.at[s, mx], send_sem.at[7], ad_sem.at[s], core_dev).start()

    def stage_d(s):
        rcopy(act.at[s, xpeer], act.at[s, xpeer], send_sem.at[6], ax_sem.at[s], x_dev).wait_recv()
        rcopy(act.at[s, xpeer], act.at[s, xpeer], send_sem.at[8], af_sem.at[s], core_dev).start()

    def stage_e(s):
        h, j = s // n_j, s % n_j
        rcopy(act.at[s, 0], act.at[s, 0], send_sem.at[7], ad_sem.at[s], core_dev).wait_recv()
        rcopy(act.at[s, 0], act.at[s, 0], send_sem.at[8], af_sem.at[s], core_dev).wait_recv()
        lhs = act[s].reshape(ROWS, CHUNK)
        dacc[h] += jnp.dot(lhs, wd_v[pl.ds(pl.multiple_of(j * CHUNK, CHUNK), CHUNK), :], preferred_element_type=f32)

    def rs2_send(h):
        for z in range(4):
            for y in range(2):
                p2[h, 2 * z + y] = dacc[h, 16 * z:16 * z + 16, y * half:(y + 1) * half].astype(bf)
        send_rs(p2, rs2, h, send_sem.at[9], rs2_sem)

    def rs2_finish(h):
        o = finish_rs(p2, rs2, h, send_sem.at[9], rs2_sem, mp[h].astype(f32))
        mo[h] = o
        ag2[h, my] = o
        send_ag(mo, ag2, h, send_sem.at[10], ag2_sem)

    rs1_send(0)
    loads[1].wait()
    rs1_finish(0)
    rs1_send(1)
    stat_send(0)
    for ld in loads[2:4]:
        ld.wait()
    norm(0)

    lag2 = 5

    def body(t, carry):
        h_now, j_now = t // n_j, t % n_j

        @pl.when((h_now + 1 < n_h) & (j_now == 1))
        def _():
            rs1_finish(h_now + 1)

        @pl.when((h_now + 2 < n_h) & (j_now == 2))
        def _():
            rs1_send(h_now + 2)

        @pl.when((h_now + 1 < n_h) & (j_now == 4))
        def _():
            stat_send(h_now + 1)

        @pl.when((t < steps) & (j_now == 0) & (t > 0))
        def _():
            norm(h_now)

        @pl.when(t < steps)
        def _():
            stage_a(t)

        @pl.when((t >= LAG_B) & (t < steps + LAG_B))
        def _():
            stage_b(t - LAG_B)

        @pl.when((t >= LAG_C) & (t < steps + LAG_C))
        def _():
            stage_c(t - LAG_C)

        @pl.when((t >= LAG_D) & (t < steps + LAG_D))
        def _():
            stage_d(t - LAG_D)

        @pl.when(t == LAG_E)
        def _():
            loads[4].wait()

        @pl.when(t >= LAG_E)
        def _():
            s = t - LAG_E
            stage_e(s)

            @pl.when(s % n_j == n_j - 1)
            def _():
                rs2_send(s // n_j)

        @pl.when((t >= LAG_E + n_j - 1 + lag2) & ((t - LAG_E - (n_j - 1) - lag2) % n_j == 0))
        def _():
            rs2_finish((t - LAG_E - (n_j - 1) - lag2) // n_j)

        return carry

    total_t = steps + LAG_E
    lax.fori_loop(0, total_t, body, 0)
    done = len([h for h in range(n_h) if LAG_E + n_j - 1 + lag2 + h * n_j < total_t])
    for h in range(done, n_h):
        rs2_finish(h)
    for h in range(n_h):
        wait_ag(ag2, h, send_sem.at[10], ag2_sem)
        for z in range(4):
            for y in range(2):
                r0 = h * ROWS + z * 16
                out_ref[r0:r0 + 16, y * half:(y + 1) * half] = ag2[h, 2 * z + y]
    for k, ref in ((1, rs1), (2, rs1), (3, st_in.at[:, pl.ds(0, 3)]), (4, dr), (5, xs), (6, act.at[:, 0]), (7, act.at[:, 0]), (8, act.at[:, 0]), (9, rs2), (10, rs2)):
        rcopy(ref, ref, send_sem.at[k], at_sem, core_dev).wait_send()


def mlp_call(x_in, gain, attn, w_o, w_gate, w_up, w_down, hidden):
    rows, cols = x_in.shape
    ff = w_gate.shape[1]
    n_j = pl.cdiv(ff, CHUNK)
    n_h = rows // ROWS
    steps = n_h * n_j
    half = cols // 2
    bf, f32 = jnp.bfloat16, jnp.float32
    any_spec, vmem = pl.BlockSpec(memory_space=pl.ANY), pl.BlockSpec(memory_space=pltpu.VMEM)
    dma = pltpu.SemaphoreType.DMA
    return pl.pallas_call(
        functools.partial(mlp_kernel, hidden),
        name="mlp",
        out_shape=jax.ShapeDtypeStruct((rows, cols), bf),
        in_specs=[any_spec, vmem, vmem, any_spec, any_spec, any_spec, any_spec],
        out_specs=vmem,
        scratch_shapes=[
            pltpu.VMEM((rows, cols), bf), pltpu.VMEM(w_o.shape, bf), pltpu.VMEM(w_gate.shape, bf), pltpu.VMEM(w_up.shape, bf),
            pltpu.VMEM((n_j * CHUNK, cols), bf), pltpu.VMEM((rows, attn.shape[1]), bf),
            pltpu.VMEM((n_h, 8, 16, half), bf), pltpu.VMEM((n_h, 7, 16, half), bf), pltpu.VMEM((n_h, 16, half), bf), pltpu.VMEM((n_h, 8, 16, half), bf),
            pltpu.VMEM((n_h, 8, 128), f32), pltpu.VMEM((n_h, 4, 8, 128), f32), pltpu.VMEM((n_h, ROWS, cols), bf),
            pltpu.VMEM((steps, 2, 2, 16, 2 * CHUNK), bf), pltpu.VMEM((steps, 2, 16, 2 * CHUNK), bf), pltpu.VMEM((steps, 16, 2 * CHUNK), f32),
            pltpu.VMEM((steps, 16, 2 * CHUNK), bf), pltpu.VMEM((steps, 16, 2 * CHUNK), bf), pltpu.VMEM((steps, 4, 16, CHUNK), bf),
            pltpu.VMEM((n_h, ROWS, cols), f32),
            pltpu.VMEM((n_h, 8, 16, half), bf), pltpu.VMEM((n_h, 7, 16, half), bf), pltpu.VMEM((n_h, 16, half), bf), pltpu.VMEM((n_h, 8, 16, half), bf),
            dma((5,)), dma((11,)), dma, dma((n_h,)), dma((n_h,)), dma((n_h,)), dma((n_h,)), dma((n_h,)),
            dma((steps,)), dma((steps,)), dma((steps,)), dma((steps,)), dma((steps,)),
        ],
        compiler_params=pltpu.CompilerParams(collective_id=1, has_side_effects=True, vmem_limit_bytes=VMEM_LIMIT),
    )(x_in, gain, attn, w_o, w_gate, w_up, w_down)


def apply_rotary(vectors, positions):
    half_dim = HEAD // 2
    inv_freq = ROPE_THETA ** (-2.0 * jnp.arange(half_dim, dtype=jnp.float32) / HEAD)
    angles = positions.astype(jnp.float32)[:, None, None] * inv_freq
    cos_tab = jnp.cos(angles)
    sin_tab = jnp.sin(angles)
    lower_half = vectors[..., :half_dim]
    upper_half = vectors[..., half_dim:]
    return jnp.concatenate([lower_half * cos_tab - upper_half * sin_tab, upper_half * cos_tab + lower_half * sin_tab], axis=-1)


def attend_local(q_rot, k_cache_out, v_cache_out, seq_lens):
    row_count, seq_len, kv_heads, _ = k_cache_out.shape
    q_heads = q_rot.shape[1]
    q_grouped = q_rot.reshape(row_count, kv_heads, q_heads // kv_heads, HEAD)
    scores = jnp.einsum("bkgd,bskd->bkgs", q_grouped, k_cache_out, preferred_element_type=jnp.float32) * HEAD ** -0.5
    visible = (jnp.arange(seq_len)[None, :] <= seq_lens[:, None])[:, None, None, :]
    scores = jnp.where(visible, scores, -jnp.inf)
    weights = jnp.exp(scores - jnp.max(scores, axis=-1, keepdims=True))
    weight_sum = jnp.sum(weights, axis=-1, keepdims=True)
    weighted = jnp.einsum("bkgs,bskd->bkgd", weights.astype(jnp.bfloat16), v_cache_out, preferred_element_type=jnp.float32)
    return (weighted / weight_sum).astype(jnp.bfloat16).reshape(row_count, q_heads * HEAD)


def solution(mesh):
    mx_size = mesh.shape["mx"]
    act_spec = P(None, "mx")
    cache_spec = P("mx", None, "my", None)
    in_specs = (act_spec, P("mx"), P("mx"), P("mx"), P("mx", "my"), P("my"), P("mx", "my"), P("my"), P("mx", "my"), P("my"), P("my", "mx"), P("mx", "my"), P("mx", "my"), P("my", "mx"), cache_spec, cache_spec)
    out_specs = (act_spec, cache_spec, cache_spec)

    def local_layer(x_in, seq_lens, gain_attn, gain_mlp, w_q, b_q, w_k, b_k, w_v, b_v, w_o, w_gate, w_up, w_down, k_cache, v_cache):
        hidden = x_in.shape[1] * mx_size
        projected = qkv_call(x_in, gain_attn[None], w_q, w_k, w_v, hidden)
        q_cols = w_q.shape[1]
        kv_cols = w_k.shape[1]
        row_count = projected.shape[0]
        kv_heads = kv_cols // HEAD
        q_vals = projected[:, :q_cols] + b_q.astype(jnp.float32)
        k_vals = projected[:, q_cols:q_cols + kv_cols] + b_k.astype(jnp.float32)
        v_vals = projected[:, q_cols + kv_cols:] + b_v.astype(jnp.float32)
        q_rot = apply_rotary(q_vals.reshape(row_count, q_cols // HEAD, HEAD), seq_lens).astype(jnp.bfloat16)
        k_rot = apply_rotary(k_vals.reshape(row_count, kv_heads, HEAD), seq_lens).astype(jnp.bfloat16)
        v_new = v_vals.reshape(row_count, kv_heads, HEAD).astype(jnp.bfloat16)
        at_slot = (jnp.arange(k_cache.shape[1])[None, :] == seq_lens[:, None])[:, :, None, None]
        k_cache_out = jnp.where(at_slot, k_rot[:, None], k_cache)
        v_cache_out = jnp.where(at_slot, v_new[:, None], v_cache)
        attn_rows = attend_local(q_rot, k_cache_out, v_cache_out, seq_lens)
        x_out = mlp_call(x_in, gain_mlp[None], attn_rows, w_o, w_gate, w_up, w_down, hidden)
        return x_out, k_cache_out, v_cache_out

    return jax.shard_map(local_layer, mesh=mesh, in_specs=in_specs, out_specs=out_specs, check_vma=False)
```

```python
import functools

import jax
import jax.numpy as jnp
import numpy as np
from jax import lax
from jax.experimental import pallas as pl
from jax.experimental.pallas import tpu as pltpu
from jax.sharding import PartitionSpec as P

HEAD = 128
NORM_EPS = 1e-6
ROPE_THETA = 1000000.0
MESH = pl.DeviceIdType.MESH
CHUNK = 512
ROWS = 64
LAG_B, LAG_C, LAG_D, LAG_E = 1, 4, 7, 8
VMEM_LIMIT = 66 * 1024 * 1000


def rcopy(src, dst, send_sem, recv_sem, dev):
    return pltpu.make_async_remote_copy(src_ref=src, dst_ref=dst, send_sem=send_sem, recv_sem=recv_sem, device_id=dev, device_id_type=MESH)


def lane_ids():
    return lax.broadcasted_iota(jnp.int32, (8, 128), 1)


def pack_column(blocks):
    tile = jnp.zeros((8, 128), jnp.float32)
    lanes = lane_ids()
    for k, block in enumerate(blocks):
        tile = jnp.where(lanes == k, block, tile)
    return tile


def unpack_column(tile, k):
    return jnp.sum(jnp.where(lane_ids() == k, tile, 0.0), axis=1, keepdims=True)


def qkv_kernel(hidden, x_hbm, gain_ref, wq_hbm, wk_hbm, wv_hbm, out_ref, x_v, wq_v, wk_v, wv_v, st_own, st_in, nrm, pp, dr, own, xs, xr, ld_sem, send_sem, st_sem, d_sem, x_sem):
    mx = lax.axis_index("mx")
    xi, ci = mx // 2, mx % 2
    partner, xpeer = 2 * xi + (1 - ci), 2 * (1 - xi) + ci
    loads = [pltpu.make_async_copy(s, d, ld_sem.at[i]) for i, (s, d) in enumerate([(x_hbm, x_v), (wq_hbm, wq_v), (wk_hbm, wk_v), (wv_hbm, wv_v)])]
    for ld in loads:
        ld.start()
    barrier = pltpu.get_barrier_semaphore()
    for d in range(1, 4):
        pl.semaphore_signal(barrier, inc=1, device_id={"mx": (mx + d) % 4}, device_id_type=MESH)
    pl.semaphore_wait(barrier, 3)

    rows = x_v.shape[0]
    loads[0].wait()
    blocks = []
    for k in range(rows // 8):
        v = x_v[8 * k:8 * k + 8, :].astype(jnp.float32)
        blocks.append(jnp.sum(v * v, axis=1, keepdims=True))
    tile = pack_column(blocks)
    st_own[...] = tile
    st_in[mx] = tile
    for d in range(1, 4):
        rcopy(st_own, st_in.at[mx], send_sem.at[0], st_sem, {"mx": (mx + d) % 4}).start()
    for ld in loads[1:]:
        ld.wait()
    rcopy(st_in.at[pl.ds(0, 3)], st_in.at[pl.ds(0, 3)], send_sem.at[0], st_sem, {"mx": partner}).wait()
    total = st_in[0] + st_in[1] + st_in[2] + st_in[3]
    scale = lax.rsqrt(total / hidden + NORM_EPS)
    gain = gain_ref[...].astype(jnp.float32).reshape(1, x_v.shape[1])
    for k in range(0, rows // 8, 2):
        col = jnp.concatenate([unpack_column(scale, k), unpack_column(scale, k + 1)], axis=0)
        nrm[8 * k:8 * k + 16, :] = (x_v[8 * k:8 * k + 16, :].astype(jnp.float32) * col * gain).astype(jnp.bfloat16)

    lhs = nrm[...]
    part = rows // 4
    off = 0
    for w in (wq_v, wk_v, wv_v):
        width = w.shape[1]
        for c0 in range(0, width, 256):
            cw = min(256, width - c0)
            r = jnp.dot(lhs, w[:, c0:c0 + cw], preferred_element_type=jnp.float32).astype(jnp.bfloat16)
            for m in range(4):
                pp[m % 2, m // 2, :, off + c0:off + c0 + cw] = r[m * part:(m + 1) * part]
        off += width
    rcopy(pp.at[1 - ci], dr, send_sem.at[1], d_sem, {"mx": partner}).start()
    rcopy(pp.at[1 - ci], dr, send_sem.at[1], d_sem, {"mx": partner}).wait_recv()
    xs[...] = (pp[ci, 1 - xi].astype(jnp.float32) + dr[1 - xi].astype(jnp.float32)).astype(jnp.bfloat16)
    out = rcopy(xs, xr, send_sem.at[2], x_sem, {"mx": xpeer})
    out.start()
    own[...] = pp[ci, xi].astype(jnp.float32) + dr[xi].astype(jnp.float32)
    out.wait_recv()
    out_ref[...] = own[...] + xr[...].astype(jnp.float32)
    out.wait_send()
    rcopy(pp.at[1 - ci], dr, send_sem.at[1], d_sem, {"mx": partner}).wait_send()


def qkv_call(x_in, gain, w_q, w_k, w_v, hidden):
    rows, cols = x_in.shape
    width = w_q.shape[1] + w_k.shape[1] + w_v.shape[1]
    bf, f32 = jnp.bfloat16, jnp.float32
    any_spec, vmem = pl.BlockSpec(memory_space=pl.ANY), pl.BlockSpec(memory_space=pltpu.VMEM)
    part = rows // 4
    return pl.pallas_call(
        functools.partial(qkv_kernel, hidden),
        name="qkv",
        out_shape=jax.ShapeDtypeStruct((part, width), f32),
        in_specs=[any_spec, vmem, any_spec, any_spec, any_spec],
        out_specs=vmem,
        scratch_shapes=[
            pltpu.VMEM((rows, cols), bf), pltpu.VMEM(w_q.shape, bf), pltpu.VMEM(w_k.shape, bf), pltpu.VMEM(w_v.shape, bf),
            pltpu.VMEM((8, 128), f32), pltpu.VMEM((4, 8, 128), f32), pltpu.VMEM((rows, cols), bf),
            pltpu.VMEM((2, 2, part, width), bf), pltpu.VMEM((2, part, width), bf), pltpu.VMEM((part, width), f32),
            pltpu.VMEM((part, width), bf), pltpu.VMEM((part, width), bf),
            pltpu.SemaphoreType.DMA((4,)), pltpu.SemaphoreType.DMA((3,)), pltpu.SemaphoreType.DMA, pltpu.SemaphoreType.DMA, pltpu.SemaphoreType.DMA,
        ],
        compiler_params=pltpu.CompilerParams(collective_id=0, has_side_effects=True, vmem_limit_bytes=VMEM_LIMIT),
    )(x_in, gain, w_q, w_k, w_v)


def mlp_kernel(hidden, x_hbm, gain_ref, attn_ref, wo_hbm, wg_hbm, wu_hbm, wd_hbm, out_ref,
               x_v, wo_v, wg_v, wu_v, wd_v, attn_v, p1, rs1, mp, ag1, st_own, st_in, h2,
               pp, dr, own, xs, xr, act, dacc, p2, rs2, mo, ag2,
               ld_sem, send_sem, at_sem, rs1_sem, ag1_sem, st_sem, rs2_sem, ag2_sem, d_sem, x_sem, ax_sem, ad_sem, af_sem):
    my, mx = lax.axis_index("my"), lax.axis_index("mx")
    n_my = 8
    xi, ci = mx // 2, mx % 2
    zi, yi = my // 2, my % 2
    partner, xpeer = 2 * xi + (1 - ci), 2 * (1 - xi) + ci
    core_dev, x_dev = {"mx": partner}, {"mx": xpeer}
    n_h = h2.shape[0]
    ff = wg_hbm.shape[0]
    n_j = pl.cdiv(ff, CHUNK)
    steps = n_h * n_j
    half = x_v.shape[1] // 2
    brows = attn_ref.shape[0]
    f32, bf = jnp.float32, jnp.bfloat16

    loads = [pltpu.make_async_copy(s, d, ld_sem.at[i]) for i, (s, d) in enumerate([
        (wo_hbm, wo_v), (x_hbm, x_v), (wg_hbm, wg_v.at[pl.ds(0, ff)]), (wu_hbm, wu_v.at[pl.ds(0, ff)]), (wd_hbm, wd_v.at[pl.ds(0, ff)])])]
    for ld in loads:
        ld.start()
    barrier = pltpu.get_barrier_semaphore()
    for d in range(1, 4):
        pl.semaphore_signal(barrier, inc=1, device_id={"mx": (mx + d) % 4}, device_id_type=MESH)
    for d in range(1, n_my):
        pl.semaphore_signal(barrier, inc=1, device_id={"my": (my + d) % n_my}, device_id_type=MESH)
    pl.semaphore_wait(barrier, 3 + n_my - 1)

    my_rows = pl.ds(pl.multiple_of(mx * brows, 16), brows)
    for d in range(1, 4):
        rcopy(attn_ref, attn_v.at[my_rows], send_sem.at[0], at_sem, {"mx": (mx + d) % 4}).start()
    attn_v[my_rows, :] = attn_ref[...]
    dacc[...] = jnp.zeros_like(dacc)
    for w in (wg_v, wu_v, wd_v):
        w[ff:, :] = jnp.zeros((w.shape[0] - ff, w.shape[1]), bf)
    loads[0].wait()
    gathered = attn_v.at[pl.ds(0, 3 * brows)]
    rcopy(gathered, gathered, send_sem.at[0], at_sem, core_dev).wait()

    for y in range(2):
        r = jnp.dot(attn_v[...], wo_v[:, y * half:(y + 1) * half], preferred_element_type=f32).astype(bf)
        for h in range(n_h):
            for z in range(4):
                r0 = h * ROWS + z * 16
                p1[h, 2 * z + y] = r[r0:r0 + 16]

    def send_rs(p, rs, h, ssem, rsem):
        for d in range(1, n_my):
            peer = (my + d) % n_my
            rcopy(p.at[h, peer], rs.at[h, d - 1], ssem, rsem.at[h], {"my": peer}).start()

    def finish_rs(p, rs, h, ssem, rsem, base):
        rcopy(rs.at[h], rs.at[h], ssem, rsem.at[h], {"my": my}).wait_recv()
        total = p[h, my].astype(f32)
        for i in range(n_my - 1):
            total += rs[h, i].astype(f32)
        return (base + total).astype(bf)

    def send_ag(piece, ag, h, ssem, rsem):
        for d in range(1, n_my):
            rcopy(piece.at[h], ag.at[h, my], ssem, rsem.at[h], {"my": (my + d) % n_my}).start()

    def wait_ag(ag, h, ssem, rsem):
        seven = ag.at[h, pl.ds(0, n_my - 1)]
        rcopy(seven, seven, ssem, rsem.at[h], {"my": my}).wait_recv()

    def rs1_send(h):
        send_rs(p1, rs1, h, send_sem.at[1], rs1_sem)

    def rs1_finish(h):
        r0 = pl.multiple_of(h * ROWS + zi * 16, 16)
        base = x_v[pl.ds(r0, 16), pl.ds(pl.multiple_of(yi * half, 128), half)].astype(f32)
        m = finish_rs(p1, rs1, h, send_sem.at[1], rs1_sem, base)
        mp[h] = m
        ag1[h, my] = m
        send_ag(mp, ag1, h, send_sem.at[2], ag1_sem)

    def stat_send(h):
        wait_ag(ag1, h, send_sem.at[2], ag1_sem)
        blocks = []
        for z in range(4):
            a, b = ag1[h, 2 * z].astype(f32), ag1[h, 2 * z + 1].astype(f32)
            ss = jnp.sum(a * a, axis=1, keepdims=True) + jnp.sum(b * b, axis=1, keepdims=True)
            blocks += [ss[:8], ss[8:]]
        tile = pack_column(blocks)
        st_own[h] = tile
        st_in[h, mx] = tile
        for d in range(1, 4):
            rcopy(st_own.at[h], st_in.at[h, mx], send_sem.at[3], st_sem.at[h], {"mx": (mx + d) % 4}).start()

    def norm(h):
        three = st_in.at[h, pl.ds(0, 3)]
        rcopy(three, three, send_sem.at[3], st_sem.at[h], core_dev).wait_recv()
        total = st_in[h, 0] + st_in[h, 1] + st_in[h, 2] + st_in[h, 3]
        scale = lax.rsqrt(total / hidden + NORM_EPS)
        for z in range(4):
            col = jnp.concatenate([unpack_column(scale, 2 * z), unpack_column(scale, 2 * z + 1)], axis=0)
            for y in range(2):
                gain = gain_ref[pl.ds(y * half, half)].astype(f32).reshape(1, half)
                h2[h, 16 * z:16 * z + 16, y * half:(y + 1) * half] = (ag1[h, 2 * z + y].astype(f32) * col * gain).astype(bf)

    def stage_a(s):
        h, j = s // n_j, s % n_j
        lhs = h2[h]
        part_rows = pl.ds(pl.multiple_of(j * CHUNK, CHUNK), CHUNK)
        for i, w in enumerate((wg_v, wu_v)):
            val = lax.dot_general(lhs, w[part_rows, :], (((1,), (1,)), ((), ())), preferred_element_type=f32).astype(bf)
            for m in range(4):
                pp[s, m % 2, m // 2, :, i * CHUNK:(i + 1) * CHUNK] = val[16 * m:16 * m + 16]
        rcopy(pp.at[s, 1 - ci], dr.at[s], send_sem.at[4], d_sem.at[s], core_dev).start()

    def stage_b(s):
        rcopy(pp.at[s, 1 - ci], dr.at[s], send_sem.at[4], d_sem.at[s], core_dev).wait_recv()
        xs[s] = (pp[s, ci, 1 - xi].astype(f32) + dr[s, 1 - xi].astype(f32)).astype(bf)
        rcopy(xs.at[s], xr.at[s], send_sem.at[5], x_sem.at[s], x_dev).start()
        own[s] = pp[s, ci, xi].astype(f32) + dr[s, xi].astype(f32)

    def stage_c(s):
        rcopy(xs.at[s], xr.at[s], send_sem.at[5], x_sem.at[s], x_dev).wait_recv()
        g = own[s, :, :CHUNK] + xr[s, :, :CHUNK].astype(f32)
        u = own[s, :, CHUNK:] + xr[s, :, CHUNK:].astype(f32)
        act[s, mx] = (jax.nn.silu(g) * u).astype(bf)
        rcopy(act.at[s, mx], act.at[s, mx], send_sem.at[6], ax_sem.at[s], x_dev).start()
        rcopy(act.at[s, mx], act.at[s, mx], send_sem.at[7], ad_sem.at[s], core_dev).start()

    def stage_d(s):
        rcopy(act.at[s, xpeer], act.at[s, xpeer], send_sem.at[6], ax_sem.at[s], x_dev).wait_recv()
        rcopy(act.at[s, xpeer], act.at[s, xpeer], send_sem.at[8], af_sem.at[s], core_dev).start()

    def stage_e(s):
        h, j = s // n_j, s % n_j
        rcopy(act.at[s, 0], act.at[s, 0], send_sem.at[7], ad_sem.at[s], core_dev).wait_recv()
        rcopy(act.at[s, 0], act.at[s, 0], send_sem.at[8], af_sem.at[s], core_dev).wait_recv()
        lhs = act[s].reshape(ROWS, CHUNK)
        dacc[h] += jnp.dot(lhs, wd_v[pl.ds(pl.multiple_of(j * CHUNK, CHUNK), CHUNK), :], preferred_element_type=f32)

    def rs2_send(h):
        for z in range(4):
            for y in range(2):
                p2[h, 2 * z + y] = dacc[h, 16 * z:16 * z + 16, y * half:(y + 1) * half].astype(bf)
        send_rs(p2, rs2, h, send_sem.at[9], rs2_sem)

    def rs2_finish(h):
        o = finish_rs(p2, rs2, h, send_sem.at[9], rs2_sem, mp[h].astype(f32))
        mo[h] = o
        ag2[h, my] = o
        send_ag(mo, ag2, h, send_sem.at[10], ag2_sem)

    rs1_send(0)
    loads[1].wait()
    rs1_finish(0)
    rs1_send(1)
    stat_send(0)
    for ld in loads[2:4]:
        ld.wait()
    norm(0)

    lag2 = 5

    def body(t, carry):
        h_now, j_now = t // n_j, t % n_j

        @pl.when((h_now + 1 < n_h) & (j_now == 1))
        def _():
            rs1_finish(h_now + 1)

        @pl.when((h_now + 2 < n_h) & (j_now == 2))
        def _():
            rs1_send(h_now + 2)

        @pl.when((h_now + 1 < n_h) & (j_now == 4))
        def _():
            stat_send(h_now + 1)

        @pl.when((t < steps) & (j_now == 0) & (t > 0))
        def _():
            norm(h_now)

        @pl.when(t < steps)
        def _():
            stage_a(t)

        @pl.when((t >= LAG_B) & (t < steps + LAG_B))
        def _():
            stage_b(t - LAG_B)

        @pl.when((t >= LAG_C) & (t < steps + LAG_C))
        def _():
            stage_c(t - LAG_C)

        @pl.when((t >= LAG_D) & (t < steps + LAG_D))
        def _():
            stage_d(t - LAG_D)

        @pl.when(t == LAG_E)
        def _():
            loads[4].wait()

        @pl.when(t >= LAG_E)
        def _():
            s = t - LAG_E
            stage_e(s)

            @pl.when(s % n_j == n_j - 1)
            def _():
                rs2_send(s // n_j)

        @pl.when((t >= LAG_E + n_j - 1 + lag2) & ((t - LAG_E - (n_j - 1) - lag2) % n_j == 0))
        def _():
            rs2_finish((t - LAG_E - (n_j - 1) - lag2) // n_j)

        return carry

    total_t = steps + LAG_E
    lax.fori_loop(0, total_t, body, 0)
    done = len([h for h in range(n_h) if LAG_E + n_j - 1 + lag2 + h * n_j < total_t])
    for h in range(done, n_h):
        rs2_finish(h)
    for h in range(n_h):
        wait_ag(ag2, h, send_sem.at[10], ag2_sem)
        for z in range(4):
            for y in range(2):
                r0 = h * ROWS + z * 16
                out_ref[r0:r0 + 16, y * half:(y + 1) * half] = ag2[h, 2 * z + y]
    for k, ref in ((1, rs1), (2, rs1), (3, st_in.at[:, pl.ds(0, 3)]), (4, dr), (5, xs), (6, act.at[:, 0]), (7, act.at[:, 0]), (8, act.at[:, 0]), (9, rs2), (10, rs2)):
        rcopy(ref, ref, send_sem.at[k], at_sem, core_dev).wait_send()


def mlp_call(x_in, gain, attn, w_o, w_gate, w_up, w_down, hidden):
    rows, cols = x_in.shape
    ff = w_gate.shape[0]
    n_j = pl.cdiv(ff, CHUNK)
    n_h = rows // ROWS
    steps = n_h * n_j
    half = cols // 2
    bf, f32 = jnp.bfloat16, jnp.float32
    any_spec, vmem = pl.BlockSpec(memory_space=pl.ANY), pl.BlockSpec(memory_space=pltpu.VMEM)
    dma = pltpu.SemaphoreType.DMA
    return pl.pallas_call(
        functools.partial(mlp_kernel, hidden),
        name="mlp",
        out_shape=jax.ShapeDtypeStruct((rows, cols), bf),
        in_specs=[any_spec, vmem, vmem, any_spec, any_spec, any_spec, any_spec],
        out_specs=vmem,
        scratch_shapes=[
            pltpu.VMEM((rows, cols), bf), pltpu.VMEM(w_o.shape, bf), pltpu.VMEM((n_j * CHUNK, cols), bf), pltpu.VMEM((n_j * CHUNK, cols), bf),
            pltpu.VMEM((n_j * CHUNK, cols), bf), pltpu.VMEM((rows, attn.shape[1]), bf),
            pltpu.VMEM((n_h, 8, 16, half), bf), pltpu.VMEM((n_h, 7, 16, half), bf), pltpu.VMEM((n_h, 16, half), bf), pltpu.VMEM((n_h, 8, 16, half), bf),
            pltpu.VMEM((n_h, 8, 128), f32), pltpu.VMEM((n_h, 4, 8, 128), f32), pltpu.VMEM((n_h, ROWS, cols), bf),
            pltpu.VMEM((steps, 2, 2, 16, 2 * CHUNK), bf), pltpu.VMEM((steps, 2, 16, 2 * CHUNK), bf), pltpu.VMEM((steps, 16, 2 * CHUNK), f32),
            pltpu.VMEM((steps, 16, 2 * CHUNK), bf), pltpu.VMEM((steps, 16, 2 * CHUNK), bf), pltpu.VMEM((steps, 4, 16, CHUNK), bf),
            pltpu.VMEM((n_h, ROWS, cols), f32),
            pltpu.VMEM((n_h, 8, 16, half), bf), pltpu.VMEM((n_h, 7, 16, half), bf), pltpu.VMEM((n_h, 16, half), bf), pltpu.VMEM((n_h, 8, 16, half), bf),
            dma((5,)), dma((11,)), dma, dma((n_h,)), dma((n_h,)), dma((n_h,)), dma((n_h,)), dma((n_h,)),
            dma((steps,)), dma((steps,)), dma((steps,)), dma((steps,)), dma((steps,)),
        ],
        compiler_params=pltpu.CompilerParams(collective_id=1, has_side_effects=True, vmem_limit_bytes=VMEM_LIMIT),
    )(x_in, gain, attn, w_o, w_gate, w_up, w_down)


GROUP_ROWS = 8


def attn_kernel(seq_ref, proj_ref, bq_ref, bk_ref, bv_ref, freq_ref, k_hbm, v_hbm, attn_ref, ko_hbm, vo_hbm, kc, vc, qs, kn, vn, os, pos, in_sem, out_sem):
    f32, bf = jnp.float32, jnp.bfloat16
    rows, seq = kc.shape[0], kc.shape[1]
    heads = attn_ref.shape[1] // HEAD
    groups = rows // GROUP_ROWS

    def moves(g, out):
        part = pl.ds(g * GROUP_ROWS, GROUP_ROWS)
        pairs, sem = (((kc, ko_hbm), (vc, vo_hbm)), out_sem) if out else (((k_hbm, kc), (v_hbm, vc)), in_sem)
        return [pltpu.make_async_copy(src.at[part], dst.at[part], sem.at[i, g]) for i, (src, dst) in enumerate(pairs)]

    for g in range(groups):
        for cp in moves(g, False):
            cp.start()
    for b in range(rows):
        pos[b:b + 1, :] = jnp.full((1, HEAD), seq_ref[b], jnp.int32).astype(f32)
    angles = pos[...] * freq_ref[...]
    lower = lax.broadcasted_iota(jnp.int32, (rows, HEAD), 1) < HEAD // 2
    cos_tab = jnp.cos(angles)
    sin_tab = jnp.sin(angles)
    sin_tab = jnp.where(lower, -sin_tab, sin_tab)

    def column(c, bias_ref, k):
        bias = bias_ref[pl.ds(k * HEAD, HEAD)].astype(f32).reshape(1, HEAD)
        return proj_ref[:, c * HEAD:(c + 1) * HEAD] + bias

    def rotate(v):
        return (v * cos_tab + pltpu.roll(v, HEAD // 2, 1) * sin_tab).astype(bf).astype(f32)

    qs[...] = jnp.zeros_like(qs)
    for h in range(heads):
        qs[:, h, :] = rotate(column(h, bq_ref, h))
    kn[...] = rotate(column(heads, bk_ref, 0))
    vn[...] = column(heads + 1, bv_ref, 0)

    def body(g, carry):
        for cp in moves(g, False):
            cp.wait()
        lens, scores = [], []
        times = lax.broadcasted_iota(jnp.int32, (8, seq), 1)
        slots = lax.broadcasted_iota(jnp.int32, (16, HEAD), 0)
        for r in range(GROUP_ROWS):
            b = g * GROUP_ROWS + r
            p = seq_ref[b]
            slab = pl.multiple_of((p // 16) * 16, 16)
            hit = slots == p - slab
            for cache, new in ((kc, kn), (vc, vn)):
                old = cache[b, pl.ds(slab, 16), :].astype(f32)
                cache[b, pl.ds(slab, 16), :] = jnp.where(hit, new[pl.ds(b, 1), :], old).astype(bf)
            s = lax.dot_general(qs[b].astype(bf), kc[b], (((1,), (1,)), ((), ())), preferred_element_type=f32) * HEAD ** -0.5
            scores.append(jnp.where(times <= p, s, -jnp.inf))
        s = jnp.concatenate(scores, axis=0)
        w = jnp.exp(s - jnp.max(s, axis=1, keepdims=True))
        total = jnp.sum(w, axis=1, keepdims=True)
        w = w.astype(bf)
        for r in range(GROUP_ROWS):
            b = g * GROUP_ROWS + r
            o = jnp.dot(w[8 * r:8 * r + 8], vc[b], preferred_element_type=f32)
            os[b] = o / total[8 * r:8 * r + 8]
        for cp in moves(g, True):
            cp.start()
        return carry

    lax.fori_loop(0, groups, body, 0)
    for h in range(heads):
        attn_ref[:, h * HEAD:(h + 1) * HEAD] = os[:, h, :].astype(bf)
    for g in range(groups):
        for cp in moves(g, True):
            cp.wait()


def attn_call(seq_lens, projected, b_q, b_k, b_v, k_cache, v_cache):
    rows, seq = k_cache.shape[0], k_cache.shape[1]
    f32, bf = jnp.float32, jnp.bfloat16
    freq = (ROPE_THETA ** (-2.0 * np.arange(HEAD // 2) / HEAD)).astype(np.float32)
    freq = jnp.asarray(np.concatenate([freq, freq])[None])
    any_spec, vmem, smem = pl.BlockSpec(memory_space=pl.ANY), pl.BlockSpec(memory_space=pltpu.VMEM), pl.BlockSpec(memory_space=pltpu.SMEM)
    dma = pltpu.SemaphoreType.DMA
    cache = jax.ShapeDtypeStruct((rows, seq, HEAD), bf)
    return pl.pallas_call(
        attn_kernel,
        name="attn",
        out_shape=(jax.ShapeDtypeStruct((rows, b_q.shape[0]), bf), cache, cache),
        in_specs=[smem, vmem, vmem, vmem, vmem, vmem, any_spec, any_spec],
        out_specs=(vmem, any_spec, any_spec),
        scratch_shapes=[
            pltpu.VMEM((rows, seq, HEAD), bf), pltpu.VMEM((rows, seq, HEAD), bf), pltpu.VMEM((rows, 8, HEAD), f32), pltpu.VMEM((rows, HEAD), f32),
            pltpu.VMEM((rows, HEAD), f32), pltpu.VMEM((rows, 8, HEAD), f32), pltpu.VMEM((rows, HEAD), f32),
            dma((2, rows // GROUP_ROWS)), dma((2, rows // GROUP_ROWS)),
        ],
        compiler_params=pltpu.CompilerParams(vmem_limit_bytes=VMEM_LIMIT),
    )(seq_lens, projected, b_q, b_k, b_v, freq, k_cache.reshape(rows, seq, HEAD), v_cache.reshape(rows, seq, HEAD))


def solution(mesh):
    mx_size = mesh.shape["mx"]
    act_spec = P(None, "mx")
    cache_spec = P("mx", None, "my", None)
    in_specs = (act_spec, P("mx"), P("mx"), P("mx"), P("mx", "my"), P("my"), P("mx", "my"), P("my"), P("mx", "my"), P("my"), P("my", "mx"), P("mx", "my"), P("mx", "my"), P("my", "mx"), cache_spec, cache_spec)
    out_specs = (act_spec, cache_spec, cache_spec)

    def local_layer(x_in, seq_lens, gain_attn, gain_mlp, w_q, b_q, w_k, b_k, w_v, b_v, w_o, w_gate, w_up, w_down, k_cache, v_cache):
        hidden = x_in.shape[1] * mx_size
        projected = qkv_call(x_in, gain_attn, w_q, w_k, w_v, hidden)
        attn_rows, k_out, v_out = attn_call(seq_lens, projected, b_q, b_k, b_v, k_cache, v_cache)
        x_out = mlp_call(x_in, gain_mlp, attn_rows, w_o, w_gate.T, w_up.T, w_down, hidden)
        k_cache_out, v_cache_out = k_out.reshape(k_cache.shape), v_out.reshape(v_cache.shape)
        return x_out, k_cache_out, v_cache_out

    return jax.shard_map(local_layer, mesh=mesh, in_specs=in_specs, out_specs=out_specs, check_vma=False)
```

```python
import functools

import jax
import jax.numpy as jnp
import numpy as np
from jax import lax
from jax.experimental import pallas as pl
from jax.experimental.pallas import tpu as pltpu
from jax.sharding import PartitionSpec as P

HEAD = 128
NORM_EPS = 1e-6
ROPE_THETA = 1000000.0
MESH = pl.DeviceIdType.MESH
CHUNK = 512
ROWS = 64
LAG_B, LAG_C, LAG_D, LAG_E, LAG_RS = 1, 4, 7, 8, 8
VMEM_LIMIT = 66 * 1024 * 1000


def rcopy(src, dst, send_sem, recv_sem, dev):
    return pltpu.make_async_remote_copy(src_ref=src, dst_ref=dst, send_sem=send_sem, recv_sem=recv_sem, device_id=dev, device_id_type=MESH)


def lane_ids():
    return lax.broadcasted_iota(jnp.int32, (8, 128), 1)


def pack_column(blocks):
    tile = jnp.zeros((8, 128), jnp.float32)
    lanes = lane_ids()
    for k, block in enumerate(blocks):
        tile = jnp.where(lanes == k, block, tile)
    return tile


def unpack_column(tile, k):
    return jnp.sum(jnp.where(lane_ids() == k, tile, 0.0), axis=1, keepdims=True)


def qkv_kernel(hidden, x_hbm, gain_ref, wq_hbm, wk_hbm, wv_hbm, out_ref, x_v, wq_v, wk_v, wv_v, st_own, st_in, nrm, pp, dr, own, xs, xr, ld_sem, send_sem, st_sem, d_sem, x_sem):
    mx = lax.axis_index("mx")
    xi, ci = mx // 2, mx % 2
    partner, xpeer = 2 * xi + (1 - ci), 2 * (1 - xi) + ci
    loads = [pltpu.make_async_copy(s, d, ld_sem.at[i]) for i, (s, d) in enumerate([(x_hbm, x_v), (wq_hbm, wq_v), (wk_hbm, wk_v), (wv_hbm, wv_v)])]
    for ld in loads:
        ld.start()
    barrier = pltpu.get_barrier_semaphore()
    for d in range(1, 4):
        pl.semaphore_signal(barrier, inc=1, device_id={"mx": (mx + d) % 4}, device_id_type=MESH)
    pl.semaphore_wait(barrier, 3)

    rows = x_v.shape[0]
    loads[0].wait()
    blocks = []
    for k in range(rows // 8):
        v = x_v[8 * k:8 * k + 8, :].astype(jnp.float32)
        blocks.append(jnp.sum(v * v, axis=1, keepdims=True))
    tile = pack_column(blocks)
    st_own[...] = tile
    st_in[mx] = tile
    for d in range(1, 4):
        rcopy(st_own, st_in.at[mx], send_sem.at[0], st_sem, {"mx": (mx + d) % 4}).start()
    for ld in loads[1:]:
        ld.wait()
    rcopy(st_in.at[pl.ds(0, 3)], st_in.at[pl.ds(0, 3)], send_sem.at[0], st_sem, {"mx": partner}).wait()
    total = st_in[0] + st_in[1] + st_in[2] + st_in[3]
    scale = lax.rsqrt(total / hidden + NORM_EPS)
    gain = gain_ref[...].astype(jnp.float32).reshape(1, x_v.shape[1])
    for k in range(0, rows // 8, 2):
        col = jnp.concatenate([unpack_column(scale, k), unpack_column(scale, k + 1)], axis=0)
        nrm[8 * k:8 * k + 16, :] = (x_v[8 * k:8 * k + 16, :].astype(jnp.float32) * col * gain).astype(jnp.bfloat16)

    lhs = nrm[...]
    part = rows // 4
    off = 0
    for w in (wq_v, wk_v, wv_v):
        width = w.shape[1]
        for c0 in range(0, width, 256):
            cw = min(256, width - c0)
            r = jnp.dot(lhs, w[:, c0:c0 + cw], preferred_element_type=jnp.float32).astype(jnp.bfloat16)
            for m in range(4):
                pp[m % 2, m // 2, :, off + c0:off + c0 + cw] = r[m * part:(m + 1) * part]
        off += width
    rcopy(pp.at[1 - ci], dr, send_sem.at[1], d_sem, {"mx": partner}).start()
    rcopy(pp.at[1 - ci], dr, send_sem.at[1], d_sem, {"mx": partner}).wait_recv()
    xs[...] = (pp[ci, 1 - xi].astype(jnp.float32) + dr[1 - xi].astype(jnp.float32)).astype(jnp.bfloat16)
    out = rcopy(xs, xr, send_sem.at[2], x_sem, {"mx": xpeer})
    out.start()
    own[...] = pp[ci, xi].astype(jnp.float32) + dr[xi].astype(jnp.float32)
    out.wait_recv()
    out_ref[...] = own[...] + xr[...].astype(jnp.float32)
    out.wait_send()
    rcopy(pp.at[1 - ci], dr, send_sem.at[1], d_sem, {"mx": partner}).wait_send()


def qkv_call(x_in, gain, w_q, w_k, w_v, hidden):
    rows, cols = x_in.shape
    width = w_q.shape[1] + w_k.shape[1] + w_v.shape[1]
    bf, f32 = jnp.bfloat16, jnp.float32
    any_spec, vmem = pl.BlockSpec(memory_space=pl.ANY), pl.BlockSpec(memory_space=pltpu.VMEM)
    part = rows // 4
    return pl.pallas_call(
        functools.partial(qkv_kernel, hidden),
        name="qkv",
        out_shape=jax.ShapeDtypeStruct((part, width), f32),
        in_specs=[any_spec, vmem, any_spec, any_spec, any_spec],
        out_specs=vmem,
        scratch_shapes=[
            pltpu.VMEM((rows, cols), bf), pltpu.VMEM(w_q.shape, bf), pltpu.VMEM(w_k.shape, bf), pltpu.VMEM(w_v.shape, bf),
            pltpu.VMEM((8, 128), f32), pltpu.VMEM((4, 8, 128), f32), pltpu.VMEM((rows, cols), bf),
            pltpu.VMEM((2, 2, part, width), bf), pltpu.VMEM((2, part, width), bf), pltpu.VMEM((part, width), f32),
            pltpu.VMEM((part, width), bf), pltpu.VMEM((part, width), bf),
            pltpu.SemaphoreType.DMA((4,)), pltpu.SemaphoreType.DMA((3,)), pltpu.SemaphoreType.DMA, pltpu.SemaphoreType.DMA, pltpu.SemaphoreType.DMA,
        ],
        compiler_params=pltpu.CompilerParams(collective_id=0, has_side_effects=True, vmem_limit_bytes=VMEM_LIMIT),
    )(x_in, gain, w_q, w_k, w_v)


def mlp_kernel(hidden, x_hbm, gain_ref, attn_ref, wo_hbm, wg_hbm, wu_hbm, wd_hbm, out_ref,
               x_v, wo_v, wg_v, wu_v, wd_v, attn_v, p1, rs1, mp, ag1, st_own, st_in, st_sum, st_all, h2,
               pp, dr, own, xs, xr, act, dacc, p2, rs2, mo, ag2,
               ld_sem, send_sem, at_sem, rs1_sem, ag1_sem, st_sem, sg_sem, rs2_sem, ag2_sem, d_sem, x_sem, ax_sem, ad_sem, af_sem):
    my, mx = lax.axis_index("my"), lax.axis_index("mx")
    n_my = 8
    xi, ci = mx // 2, mx % 2
    zi, yi = my // 2, my % 2
    partner, xpeer = 2 * xi + (1 - ci), 2 * (1 - xi) + ci
    core_dev, x_dev = {"mx": partner}, {"mx": xpeer}
    n_h = h2.shape[0]
    ff = wg_hbm.shape[0]
    n_j = pl.cdiv(ff, CHUNK)
    steps = n_h * n_j
    half = x_v.shape[1] // 2
    brows = attn_ref.shape[0]
    f32, bf = jnp.float32, jnp.bfloat16

    loads = [pltpu.make_async_copy(s, d, ld_sem.at[i]) for i, (s, d) in enumerate([
        (wo_hbm, wo_v), (x_hbm, x_v), (wg_hbm, wg_v.at[pl.ds(0, ff)]), (wu_hbm, wu_v.at[pl.ds(0, ff)]), (wd_hbm, wd_v.at[pl.ds(0, ff)])])]
    for ld in loads:
        ld.start()
    barrier = pltpu.get_barrier_semaphore()
    for d in range(1, 4):
        pl.semaphore_signal(barrier, inc=1, device_id={"mx": (mx + d) % 4}, device_id_type=MESH)
    for d in range(1, n_my):
        pl.semaphore_signal(barrier, inc=1, device_id={"my": (my + d) % n_my}, device_id_type=MESH)
    pl.semaphore_wait(barrier, 3 + n_my - 1)

    mine = pl.ds(pl.multiple_of(mx * 16, 16), 16)
    for h in range(n_h):
        for d in range(1, 4):
            rcopy(attn_ref.at[pl.ds(16 * h, 16)], attn_v.at[h, mine], send_sem.at[0], at_sem.at[h], {"mx": (mx + d) % 4}).start()
    for h in range(n_h):
        attn_v[h, mine, :] = attn_ref[16 * h:16 * h + 16, :]
    dacc[...] = jnp.zeros_like(dacc)
    for w in (wg_v, wu_v, wd_v):
        w[ff:, :] = jnp.zeros((w.shape[0] - ff, w.shape[1]), bf)
    loads[0].wait()

    zs = (3 - zi, (zi + 2) % 4, zi + 1 - 2 * (zi % 2), zi)
    peers = [2 * z + y for z in zs for y in (1 - yi, yi)][:-1]

    def project(h):
        gathered = attn_v.at[h, pl.ds(0, 48)]
        rcopy(gathered, gathered, send_sem.at[0], at_sem.at[h], core_dev).wait_recv()
        for y in range(2):
            r = jnp.dot(attn_v[h], wo_v[:, y * half:(y + 1) * half], preferred_element_type=f32).astype(bf)
            for z in range(4):
                p1[h, 2 * z + y] = r[16 * z:16 * z + 16]

    def send_rs(p, rs, h, ssem, rsem):
        for k, peer in enumerate(peers):
            rcopy(p.at[h, peer], rs.at[h, k], ssem, rsem.at[h], {"my": peer}).start()

    def finish_rs(p, rs, h, ssem, rsem, base):
        rcopy(rs.at[h], rs.at[h], ssem, rsem.at[h], {"my": my}).wait_recv()
        total = p[h, my].astype(f32)
        for i in range(n_my - 1):
            total += rs[h, i].astype(f32)
        return (base + total).astype(bf)

    def send_ag(piece, ag, h, ssem, rsem):
        for peer in peers:
            rcopy(piece.at[h], ag.at[h, my], ssem, rsem.at[h], {"my": peer}).start()

    def wait_ag(ag, h, ssem, rsem):
        seven = ag.at[h, pl.ds(0, n_my - 1)]
        rcopy(seven, seven, ssem, rsem.at[h], {"my": my}).wait_recv()

    def rs1_send(h):
        send_rs(p1, rs1, h, send_sem.at[1], rs1_sem)

    def rs1_finish(h):
        r0 = pl.multiple_of(zi * brows + h * 16, 16)
        base = x_v[pl.ds(r0, 16), pl.ds(pl.multiple_of(yi * half, 128), half)].astype(f32)
        m = finish_rs(p1, rs1, h, send_sem.at[1], rs1_sem, base)
        mp[h] = m
        ag1[h, my] = m
        send_ag(mp, ag1, h, send_sem.at[2], ag1_sem)
        m = m.astype(f32)
        ss = jnp.sum(m * m, axis=1, keepdims=True)
        tile = pack_column([ss[:8], ss[8:]])
        st_own[h] = tile
        st_in[h, mx] = tile
        for d in range(1, 4):
            rcopy(st_own.at[h], st_in.at[h, mx], send_sem.at[3], st_sem.at[h], {"mx": (mx + d) % 4}).start()

    def stat_gather(h):
        three = st_in.at[h, pl.ds(0, 3)]
        rcopy(three, three, send_sem.at[3], st_sem.at[h], core_dev).wait_recv()
        total = st_in[h, 0] + st_in[h, 1] + st_in[h, 2] + st_in[h, 3]
        st_sum[h] = total
        st_all[h, my] = total
        send_ag(st_sum, st_all, h, send_sem.at[11], sg_sem)

    def norm(h):
        wait_ag(st_all, h, send_sem.at[11], sg_sem)
        wait_ag(ag1, h, send_sem.at[2], ag1_sem)
        for z in range(4):
            scale = lax.rsqrt((st_all[h, 2 * z] + st_all[h, 2 * z + 1]) / hidden + NORM_EPS)
            col = jnp.concatenate([unpack_column(scale, 0), unpack_column(scale, 1)], axis=0)
            for y in range(2):
                gain = gain_ref[pl.ds(y * half, half)].astype(f32).reshape(1, half)
                h2[h, 16 * z:16 * z + 16, y * half:(y + 1) * half] = (ag1[h, 2 * z + y].astype(f32) * col * gain).astype(bf)

    def stage_a(s):
        h, j = s // n_j, s % n_j
        lhs = h2[h]
        part_rows = pl.ds(pl.multiple_of(j * CHUNK, CHUNK), CHUNK)
        for i, w in enumerate((wg_v, wu_v)):
            val = lax.dot_general(lhs, w[part_rows, :], (((1,), (1,)), ((), ())), preferred_element_type=f32).astype(bf)
            for m in range(4):
                pp[s, m % 2, m // 2, :, i * CHUNK:(i + 1) * CHUNK] = val[16 * m:16 * m + 16]
        rcopy(pp.at[s, 1 - ci], dr.at[s], send_sem.at[4], d_sem.at[s], core_dev).start()

    def stage_b(s):
        rcopy(pp.at[s, 1 - ci], dr.at[s], send_sem.at[4], d_sem.at[s], core_dev).wait_recv()
        xs[s] = (pp[s, ci, 1 - xi].astype(f32) + dr[s, 1 - xi].astype(f32)).astype(bf)
        rcopy(xs.at[s], xr.at[s], send_sem.at[5], x_sem.at[s], x_dev).start()
        own[s] = pp[s, ci, xi].astype(f32) + dr[s, xi].astype(f32)

    def stage_c(s):
        rcopy(xs.at[s], xr.at[s], send_sem.at[5], x_sem.at[s], x_dev).wait_recv()
        g = own[s, :, :CHUNK] + xr[s, :, :CHUNK].astype(f32)
        u = own[s, :, CHUNK:] + xr[s, :, CHUNK:].astype(f32)
        act[s, mx] = (jax.nn.silu(g) * u).astype(bf)
        rcopy(act.at[s, mx], act.at[s, mx], send_sem.at[6], ax_sem.at[s], x_dev).start()
        rcopy(act.at[s, mx], act.at[s, mx], send_sem.at[7], ad_sem.at[s], core_dev).start()

    def stage_d(s):
        rcopy(act.at[s, xpeer], act.at[s, xpeer], send_sem.at[6], ax_sem.at[s], x_dev).wait_recv()
        rcopy(act.at[s, xpeer], act.at[s, xpeer], send_sem.at[8], af_sem.at[s], core_dev).start()

    def stage_e(s):
        h, j = s // n_j, s % n_j
        rcopy(act.at[s, 0], act.at[s, 0], send_sem.at[7], ad_sem.at[s], core_dev).wait_recv()
        rcopy(act.at[s, 0], act.at[s, 0], send_sem.at[8], af_sem.at[s], core_dev).wait_recv()
        lhs = act[s].reshape(ROWS, CHUNK)
        dacc[h] += jnp.dot(lhs, wd_v[pl.ds(pl.multiple_of(j * CHUNK, CHUNK), CHUNK), :], preferred_element_type=f32)

    def rs2_send(h):
        for z in range(4):
            for y in range(2):
                p2[h, 2 * z + y] = dacc[h, 16 * z:16 * z + 16, y * half:(y + 1) * half].astype(bf)
        send_rs(p2, rs2, h, send_sem.at[9], rs2_sem)

    def rs2_finish(h):
        o = finish_rs(p2, rs2, h, send_sem.at[9], rs2_sem, mp[h].astype(f32))
        mo[h] = o
        ag2[h, my] = o
        send_ag(mo, ag2, h, send_sem.at[10], ag2_sem)

    project(0)
    rs1_send(0)
    project(1)
    rs1_send(1)
    project(2)
    loads[1].wait()
    rs1_finish(0)
    stat_gather(0)
    rs1_finish(1)
    rs1_send(2)
    stat_gather(1)
    for ld in loads[2:4]:
        ld.wait()
    norm(0)

    def body(t, carry):
        @pl.when(t == n_j)
        def _():
            norm(1)

        @pl.when(t == 2 * n_j)
        def _():
            norm(2)

        @pl.when(t == n_j + 1)
        def _():
            rs1_finish(2)

        @pl.when(t == n_j + 4)
        def _():
            stat_gather(2)

        @pl.when(t < steps)
        def _():
            stage_a(t)

        @pl.when((t >= LAG_B) & (t < steps + LAG_B))
        def _():
            stage_b(t - LAG_B)

        @pl.when((t >= LAG_C) & (t < steps + LAG_C))
        def _():
            stage_c(t - LAG_C)

        @pl.when((t >= LAG_D) & (t < steps + LAG_D))
        def _():
            stage_d(t - LAG_D)

        @pl.when(t == LAG_E)
        def _():
            loads[4].wait()

        @pl.when(t >= LAG_E)
        def _():
            s = t - LAG_E
            stage_e(s)

            @pl.when(s % n_j == n_j - 1)
            def _():
                rs2_send(s // n_j)

        lag2 = LAG_RS

        @pl.when((t >= LAG_E + n_j - 1 + lag2) & ((t - LAG_E - (n_j - 1) - lag2) % n_j == 0))
        def _():
            rs2_finish((t - LAG_E - (n_j - 1) - lag2) // n_j)

        return carry

    total_t = steps + LAG_E
    lax.fori_loop(0, total_t, body, 0)
    done = len([h for h in range(n_h) if LAG_E + n_j - 1 + LAG_RS + h * n_j < total_t])
    for h in range(done, n_h):
        rs2_finish(h)
    for h in range(n_h):
        wait_ag(ag2, h, send_sem.at[10], ag2_sem)
        for z in range(4):
            for y in range(2):
                r0 = z * brows + h * 16
                out_ref[r0:r0 + 16, y * half:(y + 1) * half] = ag2[h, 2 * z + y]
    for k, ref in ((0, attn_v.at[:, pl.ds(0, 48)]), (11, st_all.at[:, pl.ds(0, 7)]), (1, rs1), (2, rs1), (3, st_in.at[:, pl.ds(0, 3)]), (4, dr), (5, xs), (6, act.at[:, 0]), (7, act.at[:, 0]), (8, act.at[:, 0]), (9, rs2), (10, rs2)):
        rcopy(ref, ref, send_sem.at[k], at_sem.at[0], core_dev).wait_send()


def mlp_call(x_in, gain, attn, w_o, w_gate, w_up, w_down, hidden):
    rows, cols = x_in.shape
    ff = w_gate.shape[0]
    n_j = pl.cdiv(ff, CHUNK)
    n_h = rows // ROWS
    steps = n_h * n_j
    half = cols // 2
    bf, f32 = jnp.bfloat16, jnp.float32
    any_spec, vmem = pl.BlockSpec(memory_space=pl.ANY), pl.BlockSpec(memory_space=pltpu.VMEM)
    dma = pltpu.SemaphoreType.DMA
    return pl.pallas_call(
        functools.partial(mlp_kernel, hidden),
        name="mlp",
        out_shape=jax.ShapeDtypeStruct((rows, cols), bf),
        in_specs=[any_spec, vmem, vmem, any_spec, any_spec, any_spec, any_spec],
        out_specs=vmem,
        scratch_shapes=[
            pltpu.VMEM((rows, cols), bf), pltpu.VMEM(w_o.shape, bf), pltpu.VMEM((n_j * CHUNK, cols), bf), pltpu.VMEM((n_j * CHUNK, cols), bf),
            pltpu.VMEM((n_j * CHUNK, cols), bf), pltpu.VMEM((n_h, 64, attn.shape[1]), bf),
            pltpu.VMEM((n_h, 8, 16, half), bf), pltpu.VMEM((n_h, 7, 16, half), bf), pltpu.VMEM((n_h, 16, half), bf), pltpu.VMEM((n_h, 8, 16, half), bf),
            pltpu.VMEM((n_h, 8, 128), f32), pltpu.VMEM((n_h, 4, 8, 128), f32), pltpu.VMEM((n_h, 8, 128), f32), pltpu.VMEM((n_h, 8, 8, 128), f32), pltpu.VMEM((n_h, ROWS, cols), bf),
            pltpu.VMEM((steps, 2, 2, 16, 2 * CHUNK), bf), pltpu.VMEM((steps, 2, 16, 2 * CHUNK), bf), pltpu.VMEM((steps, 16, 2 * CHUNK), f32),
            pltpu.VMEM((steps, 16, 2 * CHUNK), bf), pltpu.VMEM((steps, 16, 2 * CHUNK), bf), pltpu.VMEM((steps, 4, 16, CHUNK), bf),
            pltpu.VMEM((n_h, ROWS, cols), f32),
            pltpu.VMEM((n_h, 8, 16, half), bf), pltpu.VMEM((n_h, 7, 16, half), bf), pltpu.VMEM((n_h, 16, half), bf), pltpu.VMEM((n_h, 8, 16, half), bf),
            dma((5,)), dma((12,)), dma((n_h,)), dma((n_h,)), dma((n_h,)), dma((n_h,)), dma((n_h,)), dma((n_h,)), dma((n_h,)),
            dma((steps,)), dma((steps,)), dma((steps,)), dma((steps,)), dma((steps,)),
        ],
        compiler_params=pltpu.CompilerParams(collective_id=1, has_side_effects=True, vmem_limit_bytes=VMEM_LIMIT),
    )(x_in, gain, attn, w_o, w_gate, w_up, w_down)


GROUP_ROWS = 16


def attn_kernel(seq_ref, proj_ref, bq_ref, bk_ref, bv_ref, freq_ref, k_hbm, v_hbm, attn_ref, ko_hbm, vo_hbm, kc, vc, qs, kn, vn, os, pos, in_sem, out_sem):
    f32, bf = jnp.float32, jnp.bfloat16
    rows, seq = kc.shape[0], kc.shape[1]
    heads = attn_ref.shape[1] // HEAD
    groups = rows // GROUP_ROWS

    def moves(g, out):
        part = pl.ds(g * GROUP_ROWS, GROUP_ROWS)
        pairs, sem = (((kc, ko_hbm), (vc, vo_hbm)), out_sem) if out else (((k_hbm, kc), (v_hbm, vc)), in_sem)
        return [pltpu.make_async_copy(src.at[part], dst.at[part], sem.at[i, g]) for i, (src, dst) in enumerate(pairs)]

    for g in range(groups):
        for cp in moves(g, False):
            cp.start()
    for b in range(rows):
        pos[b:b + 1, :] = jnp.full((1, HEAD), seq_ref[b], jnp.int32).astype(f32)
    angles = pos[...] * freq_ref[...]
    lower = lax.broadcasted_iota(jnp.int32, (rows, HEAD), 1) < HEAD // 2
    cos_tab = jnp.cos(angles)
    sin_tab = jnp.sin(angles)
    sin_tab = jnp.where(lower, -sin_tab, sin_tab)

    def column(c, bias_ref, k):
        bias = bias_ref[pl.ds(k * HEAD, HEAD)].astype(f32).reshape(1, HEAD)
        return proj_ref[:, c * HEAD:(c + 1) * HEAD] + bias

    def rotate(v):
        return (v * cos_tab + pltpu.roll(v, HEAD // 2, 1) * sin_tab).astype(bf).astype(f32)

    qs[...] = jnp.zeros_like(qs)
    for h in range(heads):
        qs[:, h, :] = rotate(column(h, bq_ref, h))
    kn[...] = rotate(column(heads, bk_ref, 0))
    vn[...] = column(heads + 1, bv_ref, 0)

    def body(g, carry):
        for cp in moves(g, False):
            cp.wait()
        lens, scores = [], []
        times = lax.broadcasted_iota(jnp.int32, (8, seq), 1)
        slots = lax.broadcasted_iota(jnp.int32, (16, HEAD), 0)
        for r in range(GROUP_ROWS):
            b = g * GROUP_ROWS + r
            p = seq_ref[b]
            slab = pl.multiple_of((p // 16) * 16, 16)
            hit = slots == p - slab
            for cache, new in ((kc, kn), (vc, vn)):
                old = cache[b, pl.ds(slab, 16), :].astype(f32)
                cache[b, pl.ds(slab, 16), :] = jnp.where(hit, new[pl.ds(b, 1), :], old).astype(bf)
            s = lax.dot_general(qs[b].astype(bf), kc[b], (((1,), (1,)), ((), ())), preferred_element_type=f32) * HEAD ** -0.5
            scores.append(jnp.where(times <= p, s, -jnp.inf))
        s = jnp.concatenate(scores, axis=0)
        w = jnp.exp(s - jnp.max(s, axis=1, keepdims=True))
        total = jnp.sum(w, axis=1, keepdims=True)
        w = w.astype(bf)
        for r in range(GROUP_ROWS):
            b = g * GROUP_ROWS + r
            o = jnp.dot(w[8 * r:8 * r + 8], vc[b], preferred_element_type=f32)
            os[b] = o / total[8 * r:8 * r + 8]
        for cp in moves(g, True):
            cp.start()
        return carry

    lax.fori_loop(0, groups, body, 0)
    for h in range(heads):
        attn_ref[:, h * HEAD:(h + 1) * HEAD] = os[:, h, :].astype(bf)
    for g in range(groups):
        for cp in moves(g, True):
            cp.wait()


def attn_call(seq_lens, projected, b_q, b_k, b_v, k_cache, v_cache):
    rows, seq = k_cache.shape[0], k_cache.shape[1]
    f32, bf = jnp.float32, jnp.bfloat16
    freq = (ROPE_THETA ** (-2.0 * np.arange(HEAD // 2) / HEAD)).astype(np.float32)
    freq = jnp.asarray(np.concatenate([freq, freq])[None])
    any_spec, vmem, smem = pl.BlockSpec(memory_space=pl.ANY), pl.BlockSpec(memory_space=pltpu.VMEM), pl.BlockSpec(memory_space=pltpu.SMEM)
    dma = pltpu.SemaphoreType.DMA
    cache = jax.ShapeDtypeStruct((rows, seq, HEAD), bf)
    return pl.pallas_call(
        attn_kernel,
        name="attn",
        out_shape=(jax.ShapeDtypeStruct((rows, b_q.shape[0]), bf), cache, cache),
        in_specs=[smem, vmem, vmem, vmem, vmem, vmem, any_spec, any_spec],
        out_specs=(vmem, any_spec, any_spec),
        scratch_shapes=[
            pltpu.VMEM((rows, seq, HEAD), bf), pltpu.VMEM((rows, seq, HEAD), bf), pltpu.VMEM((rows, 8, HEAD), f32), pltpu.VMEM((rows, HEAD), f32),
            pltpu.VMEM((rows, HEAD), f32), pltpu.VMEM((rows, 8, HEAD), f32), pltpu.VMEM((rows, HEAD), f32),
            dma((2, rows // GROUP_ROWS)), dma((2, rows // GROUP_ROWS)),
        ],
        compiler_params=pltpu.CompilerParams(vmem_limit_bytes=VMEM_LIMIT),
    )(seq_lens, projected, b_q, b_k, b_v, freq, k_cache.reshape(rows, seq, HEAD), v_cache.reshape(rows, seq, HEAD))


def solution(mesh):
    mx_size = mesh.shape["mx"]
    act_spec = P(None, "mx")
    cache_spec = P("mx", None, "my", None)
    in_specs = (act_spec, P("mx"), P("mx"), P("mx"), P("mx", "my"), P("my"), P("mx", "my"), P("my"), P("mx", "my"), P("my"), P("my", "mx"), P("mx", "my"), P("mx", "my"), P("my", "mx"), cache_spec, cache_spec)
    out_specs = (act_spec, cache_spec, cache_spec)

    def local_layer(x_in, seq_lens, gain_attn, gain_mlp, w_q, b_q, w_k, b_k, w_v, b_v, w_o, w_gate, w_up, w_down, k_cache, v_cache):
        hidden = x_in.shape[1] * mx_size
        projected = qkv_call(x_in, gain_attn, w_q, w_k, w_v, hidden)
        attn_rows, k_out, v_out = attn_call(seq_lens, projected, b_q, b_k, b_v, k_cache, v_cache)
        x_out = mlp_call(x_in, gain_mlp, attn_rows, w_o, w_gate.T, w_up.T, w_down, hidden)
        k_cache_out, v_cache_out = k_out.reshape(k_cache.shape), v_out.reshape(v_cache.shape)
        return x_out, k_cache_out, v_cache_out

    return jax.shard_map(local_layer, mesh=mesh, in_specs=in_specs, out_specs=out_specs, check_vma=False)
```

```python
import functools

import jax
import jax.numpy as jnp
import numpy as np
from jax import lax
from jax.experimental import pallas as pl
from jax.experimental.pallas import tpu as pltpu
from jax.sharding import PartitionSpec as P

HEAD = 128
NORM_EPS = 1e-6
ROPE_THETA = 1000000.0
MESH = pl.DeviceIdType.MESH
CHUNK = 512
TILE = 256
ROWS = 64
LAG_B, LAG_C, LAG_D, LAG_E, LAG_RS = 1, 4, 7, 8, 8
VMEM_LIMIT = 67043328
MLP_LIMIT = VMEM_LIMIT


def rcopy(src, dst, send_sem, recv_sem, dev):
    return pltpu.make_async_remote_copy(src_ref=src, dst_ref=dst, send_sem=send_sem, recv_sem=recv_sem, device_id=dev, device_id_type=MESH)


def lane_ids():
    return lax.broadcasted_iota(jnp.int32, (8, 128), 1)


def pack_column(blocks):
    tile = jnp.zeros((8, 128), jnp.float32)
    lanes = lane_ids()
    for k, block in enumerate(blocks):
        tile = jnp.where(lanes == k, block, tile)
    return tile


def unpack_column(tile, k):
    return jnp.sum(jnp.where(lane_ids() == k, tile, 0.0), axis=1, keepdims=True)


def qkv_kernel(hidden, x_hbm, gain_ref, wq_hbm, wk_hbm, wv_hbm, out_ref, x_v, wq_v, wk_v, wv_v, st_own, st_in, nrm, pp, dr, own, xs, xr, ld_sem, send_sem, st_sem, d_sem, x_sem):
    mx = lax.axis_index("mx")
    xi, ci = mx // 2, mx % 2
    partner, xpeer = 2 * xi + (1 - ci), 2 * (1 - xi) + ci
    loads = [pltpu.make_async_copy(s, d, ld_sem.at[i]) for i, (s, d) in enumerate([(x_hbm, x_v), (wq_hbm, wq_v), (wk_hbm, wk_v), (wv_hbm, wv_v)])]
    for ld in loads:
        ld.start()
    barrier = pltpu.get_barrier_semaphore()
    for d in range(1, 4):
        pl.semaphore_signal(barrier, inc=1, device_id={"mx": (mx + d) % 4}, device_id_type=MESH)
    pl.semaphore_wait(barrier, 3)

    rows = x_v.shape[0]
    loads[0].wait()
    blocks = []
    for k in range(rows // 8):
        v = x_v[8 * k:8 * k + 8, :].astype(jnp.float32)
        blocks.append(jnp.sum(v * v, axis=1, keepdims=True))
    tile = pack_column(blocks)
    st_own[...] = tile
    st_in[mx] = tile
    for d in range(1, 4):
        rcopy(st_own, st_in.at[mx], send_sem.at[0], st_sem, {"mx": (mx + d) % 4}).start()
    for ld in loads[1:]:
        ld.wait()
    rcopy(st_in.at[pl.ds(0, 3)], st_in.at[pl.ds(0, 3)], send_sem.at[0], st_sem, {"mx": partner}).wait()
    total = st_in[0] + st_in[1] + st_in[2] + st_in[3]
    scale = lax.rsqrt(total / hidden + NORM_EPS)
    gain = gain_ref[...].astype(jnp.float32).reshape(1, x_v.shape[1])
    for k in range(0, rows // 8, 2):
        col = jnp.concatenate([unpack_column(scale, k), unpack_column(scale, k + 1)], axis=0)
        nrm[8 * k:8 * k + 16, :] = (x_v[8 * k:8 * k + 16, :].astype(jnp.float32) * col * gain).astype(jnp.bfloat16)

    lhs = nrm[...]
    part = rows // 4
    off = 0
    for w in (wq_v, wk_v, wv_v):
        width = w.shape[1]
        for c0 in range(0, width, 256):
            cw = min(256, width - c0)
            r = jnp.dot(lhs, w[:, c0:c0 + cw], preferred_element_type=jnp.float32).astype(jnp.bfloat16)
            for m in range(4):
                pp[m % 2, m // 2, :, off + c0:off + c0 + cw] = r[m * part:(m + 1) * part]
        off += width
    rcopy(pp.at[1 - ci], dr, send_sem.at[1], d_sem, {"mx": partner}).start()
    rcopy(pp.at[1 - ci], dr, send_sem.at[1], d_sem, {"mx": partner}).wait_recv()
    xs[...] = (pp[ci, 1 - xi].astype(jnp.float32) + dr[1 - xi].astype(jnp.float32)).astype(jnp.bfloat16)
    out = rcopy(xs, xr, send_sem.at[2], x_sem, {"mx": xpeer})
    out.start()
    own[...] = pp[ci, xi].astype(jnp.float32) + dr[xi].astype(jnp.float32)
    out.wait_recv()
    out_ref[...] = own[...] + xr[...].astype(jnp.float32)
    out.wait_send()
    rcopy(pp.at[1 - ci], dr, send_sem.at[1], d_sem, {"mx": partner}).wait_send()


def qkv_call(x_in, gain, w_q, w_k, w_v, hidden):
    rows, cols = x_in.shape
    width = w_q.shape[1] + w_k.shape[1] + w_v.shape[1]
    bf, f32 = jnp.bfloat16, jnp.float32
    any_spec, vmem = pl.BlockSpec(memory_space=pl.ANY), pl.BlockSpec(memory_space=pltpu.VMEM)
    part = rows // 4
    return pl.pallas_call(
        functools.partial(qkv_kernel, hidden),
        name="qkv",
        out_shape=jax.ShapeDtypeStruct((part, width), f32),
        in_specs=[any_spec, vmem, any_spec, any_spec, any_spec],
        out_specs=vmem,
        scratch_shapes=[
            pltpu.VMEM((rows, cols), bf), pltpu.VMEM(w_q.shape, bf), pltpu.VMEM(w_k.shape, bf), pltpu.VMEM(w_v.shape, bf),
            pltpu.VMEM((8, 128), f32), pltpu.VMEM((4, 8, 128), f32), pltpu.VMEM((rows, cols), bf),
            pltpu.VMEM((2, 2, part, width), bf), pltpu.VMEM((2, part, width), bf), pltpu.VMEM((part, width), f32),
            pltpu.VMEM((part, width), bf), pltpu.VMEM((part, width), bf),
            pltpu.SemaphoreType.DMA((4,)), pltpu.SemaphoreType.DMA((3,)), pltpu.SemaphoreType.DMA, pltpu.SemaphoreType.DMA, pltpu.SemaphoreType.DMA,
        ],
        compiler_params=pltpu.CompilerParams(collective_id=0, has_side_effects=True, vmem_limit_bytes=VMEM_LIMIT),
    )(x_in, gain, w_q, w_k, w_v)


def mlp_kernel(hidden, x_hbm, gain_ref, attn_ref, wo_hbm, wg_hbm, wu_hbm, wd_hbm, ag2,
               x_v, wo_v, wg_v, wu_v, wd_v, attn_v, p1, rs1, mp, ag1, st_own, st_in, st_sum, st_all, h2,
               pp, dr, own, xs, xr, act, dacc, p2, rs2, mo, eye,
               ld_sem, send_sem, at_sem, rs1_sem, ag1_sem, st_sem, sg_sem, rs2_sem, ag2_sem, d_sem, x_sem, ax_sem, ad_sem, af_sem):
    my, mx = lax.axis_index("my"), lax.axis_index("mx")
    n_my = 8
    xi, ci = mx // 2, mx % 2
    zi, yi = my // 2, my % 2
    partner, xpeer = 2 * xi + (1 - ci), 2 * (1 - xi) + ci
    core_dev, x_dev = {"mx": partner}, {"mx": xpeer}
    n_h = h2.shape[0]
    ff = wg_hbm.shape[0]
    n_j = pl.cdiv(ff, CHUNK)
    steps = n_h * n_j
    half = x_v.shape[1] // 2
    brows = attn_ref.shape[0]
    f32, bf = jnp.float32, jnp.bfloat16

    n_k = wg_v.shape[0]
    tiles = [(src.at[:, pl.ds(TILE * k, TILE)], dst.at[k, pl.ds(0, ff)]) for src, dst in ((wg_hbm, wg_v), (wu_hbm, wu_v)) for k in range(n_k)]
    loads = [pltpu.make_async_copy(s, d, ld_sem.at[i]) for i, (s, d) in enumerate([
        (wo_hbm, wo_v), (x_hbm, x_v)] + tiles + [(wd_hbm, wd_v.at[pl.ds(0, ff)])])]
    for ld in loads:
        ld.start()
    barrier = pltpu.get_barrier_semaphore()
    for d in range(1, 4):
        pl.semaphore_signal(barrier, inc=1, device_id={"mx": (mx + d) % 4}, device_id_type=MESH)
    for d in range(1, n_my):
        pl.semaphore_signal(barrier, inc=1, device_id={"my": (my + d) % n_my}, device_id_type=MESH)
    pl.semaphore_wait(barrier, 3 + n_my - 1)

    mine = pl.ds(pl.multiple_of(mx * 16, 16), 16)
    for h in range(n_h):
        for d in range(1, 4):
            rcopy(attn_ref.at[pl.ds(16 * h, 16)], attn_v.at[h, mine], send_sem.at[0], at_sem.at[h], {"mx": (mx + d) % 4}).start()
    for h in range(n_h):
        attn_v[h, mine, :] = attn_ref[16 * h:16 * h + 16, :]
    dacc[...] = jnp.zeros_like(dacc)
    wd_v[ff:, :] = jnp.zeros((wd_v.shape[0] - ff, wd_v.shape[1]), bf)
    for w in (wg_v, wu_v):
        for k in range(n_k):
            w[k, ff:, :] = jnp.zeros((w.shape[1] - ff, TILE), bf)
    eye[...] = (lax.broadcasted_iota(jnp.int32, (TILE, TILE), 0) == lax.broadcasted_iota(jnp.int32, (TILE, TILE), 1)).astype(f32).astype(bf)
    loads[0].wait()

    zs = (3 - zi, (zi + 2) % 4, zi + 1 - 2 * (zi % 2), zi)
    peers = [2 * z + y for z in zs for y in (1 - yi, yi)][:-1]

    def project(h):
        gathered = attn_v.at[h, pl.ds(0, 48)]
        rcopy(gathered, gathered, send_sem.at[0], at_sem.at[h], core_dev).wait_recv()
        for y in range(2):
            r = jnp.dot(attn_v[h], wo_v[:, y * half:(y + 1) * half], preferred_element_type=f32).astype(bf)
            for z in range(4):
                p1[h, 2 * z + y] = r[16 * z:16 * z + 16]

    parts = ((0, TILE), (TILE, half))

    def send_rs(p, rs, h, ssem, rsem):
        for i, (lo, hi) in enumerate(parts):
            cols = pl.ds(lo, hi - lo)
            for k, peer in enumerate(peers):
                rcopy(p.at[h, peer, :, cols], rs.at[h, k, :, cols], ssem, rsem.at[h, i], {"my": peer}).start()

    def finish_rs(p, rs, h, i, ssem, rsem, base):
        lo, hi = parts[i]
        seven = rs.at[h, :, :, pl.ds(lo, hi - lo)]
        rcopy(seven, seven, ssem, rsem.at[h, i], {"my": my}).wait_recv()
        total = p[h, my, :, lo:hi].astype(f32)
        for k in range(n_my - 1):
            total += rs[h, k, :, lo:hi].astype(f32)
        return (base + total).astype(bf)

    def send_ag(piece, ag, h, ssem, rsem, i=None):
        src, dst, sem = piece.at[h], ag.at[h, my], rsem.at[h]
        if i is not None:
            cols = pl.ds(parts[i][0], parts[i][1] - parts[i][0])
            src, dst, sem = piece.at[h, :, cols], ag.at[h, my, :, cols], rsem.at[h, i]
        for peer in peers:
            rcopy(src, dst, ssem, sem, {"my": peer}).start()

    def wait_ag(ag, h, ssem, rsem, i=None):
        seven, sem = ag.at[h, pl.ds(0, n_my - 1)], rsem.at[h] if i is None else rsem.at[h, i]
        if i is not None:
            seven = ag.at[h, pl.ds(0, n_my - 1), :, pl.ds(parts[i][0], parts[i][1] - parts[i][0])]
        rcopy(seven, seven, ssem, sem, {"my": my}).wait_recv()

    def rs1_send(h):
        send_rs(p1, rs1, h, send_sem.at[1], rs1_sem)

    def rs1_finish(h):
        ss = jnp.zeros((16, 1), f32)
        for i, (lo, hi) in enumerate(parts):
            r0 = pl.multiple_of(zi * brows + h * 16, 16)
            base = x_v[pl.ds(r0, 16), pl.ds(pl.multiple_of(yi * half + lo, 128), hi - lo)].astype(f32)
            m = finish_rs(p1, rs1, h, i, send_sem.at[1], rs1_sem, base)
            mp[h, :, lo:hi] = m
            ag1[h, my, :, lo:hi] = m
            send_ag(mp, ag1, h, send_sem.at[2], ag1_sem, i)
            m = m.astype(f32)
            ss += jnp.sum(m * m, axis=1, keepdims=True)
        tile = pack_column([ss[:8], ss[8:]])
        st_own[h] = tile
        st_in[h, mx] = tile
        for d in range(1, 4):
            rcopy(st_own.at[h], st_in.at[h, mx], send_sem.at[3], st_sem.at[h], {"mx": (mx + d) % 4}).start()

    def stat_gather(h):
        three = st_in.at[h, pl.ds(0, 3)]
        rcopy(three, three, send_sem.at[3], st_sem.at[h], core_dev).wait_recv()
        total = st_in[h, 0] + st_in[h, 1] + st_in[h, 2] + st_in[h, 3]
        st_sum[h] = total
        st_all[h, my] = total
        send_ag(st_sum, st_all, h, send_sem.at[11], sg_sem)

    def norm(h):
        wait_ag(st_all, h, send_sem.at[11], sg_sem)
        for i in range(2):
            wait_ag(ag1, h, send_sem.at[2], ag1_sem, i)
        for z in range(4):
            scale = lax.rsqrt((st_all[h, 2 * z] + st_all[h, 2 * z + 1]) / hidden + NORM_EPS)
            col = jnp.concatenate([unpack_column(scale, 0), unpack_column(scale, 1)], axis=0)
            for y in range(2):
                gain = gain_ref[pl.ds(y * half, half)].astype(f32).reshape(1, half)
                h2[h, 16 * z:16 * z + 16, y * half:(y + 1) * half] = (ag1[h, 2 * z + y].astype(f32) * col * gain).astype(bf)

    def transpose(i, carry):
        rows = pl.ds(pl.multiple_of(i * TILE, TILE), TILE)
        for k in range(n_k):
            flipped = [lax.dot_general(eye[...], w[k, rows, :], (((1,), (1,)), ((), ())), preferred_element_type=f32).astype(bf) for w in (wg_v, wu_v)]
            for w, val in zip((wg_v, wu_v), flipped):
                w[k, rows, :] = val
        return carry

    def stage_a(s):
        h, j = s // n_j, s % n_j
        lhs = h2[h]
        for i, w in enumerate((wg_v, wu_v)):
            cols = []
            for n in range(CHUNK // TILE):
                rows = pl.ds(pl.multiple_of(j * CHUNK + n * TILE, TILE), TILE)
                acc = jnp.dot(lhs[:, :TILE], w[0, rows, :], preferred_element_type=f32)
                for k in range(1, n_k):
                    acc += jnp.dot(lhs[:, TILE * k:TILE * (k + 1)], w[k, rows, :], preferred_element_type=f32)
                cols.append(acc.astype(bf))
            val = jnp.concatenate(cols, axis=1)
            for m in range(4):
                pp[s, m % 2, m // 2, :, i * CHUNK:(i + 1) * CHUNK] = val[16 * m:16 * m + 16]
        rcopy(pp.at[s, 1 - ci], dr.at[s], send_sem.at[4], d_sem.at[s], core_dev).start()

    def stage_b(s):
        rcopy(pp.at[s, 1 - ci], dr.at[s], send_sem.at[4], d_sem.at[s], core_dev).wait_recv()
        xs[s] = (pp[s, ci, 1 - xi].astype(f32) + dr[s, 1 - xi].astype(f32)).astype(bf)
        rcopy(xs.at[s], xr.at[s], send_sem.at[5], x_sem.at[s], x_dev).start()
        own[s] = pp[s, ci, xi].astype(f32) + dr[s, xi].astype(f32)

    def stage_c(s):
        rcopy(xs.at[s], xr.at[s], send_sem.at[5], x_sem.at[s], x_dev).wait_recv()
        g = own[s, :, :CHUNK] + xr[s, :, :CHUNK].astype(f32)
        u = own[s, :, CHUNK:] + xr[s, :, CHUNK:].astype(f32)
        act[s, mx] = (jax.nn.silu(g) * u).astype(bf)
        rcopy(act.at[s, mx], act.at[s, mx], send_sem.at[6], ax_sem.at[s], x_dev).start()
        rcopy(act.at[s, mx], act.at[s, mx], send_sem.at[7], ad_sem.at[s], core_dev).start()

    def stage_d(s):
        rcopy(act.at[s, xpeer], act.at[s, xpeer], send_sem.at[6], ax_sem.at[s], x_dev).wait_recv()
        rcopy(act.at[s, xpeer], act.at[s, xpeer], send_sem.at[8], af_sem.at[s], core_dev).start()

    def stage_e(s):
        h, j = s // n_j, s % n_j
        rcopy(act.at[s, 0], act.at[s, 0], send_sem.at[7], ad_sem.at[s], core_dev).wait_recv()
        rcopy(act.at[s, 0], act.at[s, 0], send_sem.at[8], af_sem.at[s], core_dev).wait_recv()
        lhs = act[s].reshape(ROWS, CHUNK)
        dacc[h] += jnp.dot(lhs, wd_v[pl.ds(pl.multiple_of(j * CHUNK, CHUNK), CHUNK), :], preferred_element_type=f32)

    def rs2_send(h):
        for z in range(4):
            for y in range(2):
                p2[h, 2 * z + y] = dacc[h, 16 * z:16 * z + 16, y * half:(y + 1) * half].astype(bf)
        send_rs(p2, rs2, h, send_sem.at[9], rs2_sem)

    def rs2_finish(h):
        for i, (lo, hi) in enumerate(parts):
            o = finish_rs(p2, rs2, h, i, send_sem.at[9], rs2_sem, mp[h, :, lo:hi].astype(f32))
            mo[h, :, lo:hi] = o
            ag2[h, my, :, lo:hi] = o
            send_ag(mo, ag2, h, send_sem.at[10], ag2_sem, i)

    n_t = n_j * (CHUNK // TILE)
    project(0)
    rs1_send(0)
    project(1)
    rs1_send(1)
    project(2)
    loads[1].wait()
    for ld in loads[2:2 + 2 * n_k]:
        ld.wait()
    lax.fori_loop(0, n_t // 2, transpose, 0)
    rs1_finish(0)
    lax.fori_loop(n_t // 2, n_t // 2 + 3, transpose, 0)
    stat_gather(0)
    rs1_finish(1)
    rs1_send(2)
    lax.fori_loop(n_t // 2 + 3, n_t, transpose, 0)
    stat_gather(1)
    norm(0)

    def body(t, carry):
        @pl.when(t == n_j)
        def _():
            norm(1)

        @pl.when(t == 2 * n_j)
        def _():
            norm(2)

        @pl.when(t == n_j + 1)
        def _():
            rs1_finish(2)

        @pl.when(t == n_j + 4)
        def _():
            stat_gather(2)

        @pl.when(t < steps)
        def _():
            stage_a(t)

        @pl.when((t >= LAG_B) & (t < steps + LAG_B))
        def _():
            stage_b(t - LAG_B)

        @pl.when((t >= LAG_C) & (t < steps + LAG_C))
        def _():
            stage_c(t - LAG_C)

        @pl.when((t >= LAG_D) & (t < steps + LAG_D))
        def _():
            stage_d(t - LAG_D)

        @pl.when(t == LAG_E)
        def _():
            loads[-1].wait()

        @pl.when(t >= LAG_E)
        def _():
            s = t - LAG_E
            stage_e(s)

            @pl.when(s % n_j == n_j - 1)
            def _():
                rs2_send(s // n_j)

        lag2 = LAG_RS

        @pl.when((t >= LAG_E + n_j - 1 + lag2) & ((t - LAG_E - (n_j - 1) - lag2) % n_j == 0))
        def _():
            rs2_finish((t - LAG_E - (n_j - 1) - lag2) // n_j)

        return carry

    total_t = steps + LAG_E
    lax.fori_loop(0, total_t, body, 0)
    done = len([h for h in range(n_h) if LAG_E + n_j - 1 + LAG_RS + h * n_j < total_t])
    for h in range(done, n_h):
        rs2_finish(h)
    for h in range(n_h):
        for i in range(2):
            wait_ag(ag2, h, send_sem.at[10], ag2_sem, i)
    for k, ref in ((0, attn_v.at[:, pl.ds(0, 48)]), (11, st_all.at[:, pl.ds(0, 7)]), (1, rs1), (2, rs1), (3, st_in.at[:, pl.ds(0, 3)]), (4, dr), (5, xs), (6, act.at[:, 0]), (7, act.at[:, 0]), (8, act.at[:, 0]), (9, rs2), (10, rs2)):
        rcopy(ref, ref, send_sem.at[k], at_sem.at[0], core_dev).wait_send()


def mlp_call(x_in, gain, attn, w_o, w_gate, w_up, w_down, hidden):
    rows, cols = x_in.shape
    ff = w_gate.shape[0]
    n_j = pl.cdiv(ff, CHUNK)
    n_h = rows // ROWS
    steps = n_h * n_j
    half = cols // 2
    bf, f32 = jnp.bfloat16, jnp.float32
    hbm, vmem = pl.BlockSpec(memory_space=pltpu.HBM), pl.BlockSpec(memory_space=pltpu.VMEM)
    dma = pltpu.SemaphoreType.DMA
    return pl.pallas_call(
        functools.partial(mlp_kernel, hidden),
        name="mlp",
        out_shape=jax.ShapeDtypeStruct((n_h, 8, 16, half), bf),
        in_specs=[hbm, vmem, vmem, hbm, hbm, hbm, hbm],
        out_specs=vmem,
        scratch_shapes=[
            pltpu.VMEM((rows, cols), bf), pltpu.VMEM(w_o.shape, bf), pltpu.VMEM((cols // TILE, n_j * CHUNK, TILE), bf), pltpu.VMEM((cols // TILE, n_j * CHUNK, TILE), bf),
            pltpu.VMEM((n_j * CHUNK, cols), bf), pltpu.VMEM((n_h, 64, attn.shape[1]), bf),
            pltpu.VMEM((n_h, 8, 16, half), bf), pltpu.VMEM((n_h, 7, 16, half), bf), pltpu.VMEM((n_h, 16, half), bf), pltpu.VMEM((n_h, 8, 16, half), bf),
            pltpu.VMEM((n_h, 8, 128), f32), pltpu.VMEM((n_h, 4, 8, 128), f32), pltpu.VMEM((n_h, 8, 128), f32), pltpu.VMEM((n_h, 8, 8, 128), f32), pltpu.VMEM((n_h, ROWS, cols), bf),
            pltpu.VMEM((steps, 2, 2, 16, 2 * CHUNK), bf), pltpu.VMEM((steps, 2, 16, 2 * CHUNK), bf), pltpu.VMEM((steps, 16, 2 * CHUNK), f32),
            pltpu.VMEM((steps, 16, 2 * CHUNK), bf), pltpu.VMEM((steps, 16, 2 * CHUNK), bf), pltpu.VMEM((steps, 4, 16, CHUNK), bf),
            pltpu.VMEM((n_h, ROWS, cols), f32),
            pltpu.VMEM((n_h, 8, 16, half), bf), pltpu.VMEM((n_h, 7, 16, half), bf), pltpu.VMEM((n_h, 16, half), bf), pltpu.VMEM((TILE, TILE), bf),
            dma((3 + 2 * (cols // TILE),)), dma((12,)), dma((n_h,)), dma((n_h, 2)), dma((n_h, 2)), dma((n_h,)), dma((n_h,)), dma((n_h, 2)), dma((n_h, 2)),
            dma((steps,)), dma((steps,)), dma((steps,)), dma((steps,)), dma((steps,)),
        ],
        compiler_params=pltpu.CompilerParams(collective_id=1, has_side_effects=True, vmem_limit_bytes=MLP_LIMIT),
    )(x_in, gain, attn, w_o, w_gate, w_up, w_down)


def place_kernel(pieces_ref, out_ref):
    n_h, _, _, half = pieces_ref.shape
    for h in range(n_h):
        for z in range(4):
            for y in range(2):
                r0 = z * 16 * n_h + h * 16
                out_ref[r0:r0 + 16, y * half:(y + 1) * half] = pieces_ref[h, 2 * z + y]


def place_call(pieces, shape):
    vmem = pl.BlockSpec(memory_space=pltpu.VMEM)
    return pl.pallas_call(place_kernel, name="place", out_shape=jax.ShapeDtypeStruct(shape, pieces.dtype), in_specs=[vmem], out_specs=vmem, compiler_params=pltpu.CompilerParams(vmem_limit_bytes=4 * 1024 * 1024))(pieces)


GROUP_ROWS = 16


def attn_kernel(seq_ref, proj_ref, bq_ref, bk_ref, bv_ref, freq_ref, k_hbm, v_hbm, attn_ref, ko_hbm, vo_hbm, kc, vc, qs, kn, vn, os, pos, in_sem, out_sem):
    f32, bf = jnp.float32, jnp.bfloat16
    rows, seq = kc.shape[0], kc.shape[1]
    heads = attn_ref.shape[1] // HEAD
    groups = rows // GROUP_ROWS

    def moves(g, out):
        part = pl.ds(g * GROUP_ROWS, GROUP_ROWS)
        pairs, sem = (((kc, ko_hbm), (vc, vo_hbm)), out_sem) if out else (((k_hbm, kc), (v_hbm, vc)), in_sem)
        return [pltpu.make_async_copy(src.at[part], dst.at[part], sem.at[i, g]) for i, (src, dst) in enumerate(pairs)]

    for g in range(groups):
        for cp in moves(g, False):
            cp.start()
    for b in range(rows):
        pos[b:b + 1, :] = jnp.full((1, HEAD), seq_ref[b], jnp.int32).astype(f32)
    angles = pos[...] * freq_ref[...]
    lower = lax.broadcasted_iota(jnp.int32, (rows, HEAD), 1) < HEAD // 2
    cos_tab = jnp.cos(angles)
    sin_tab = jnp.sin(angles)
    sin_tab = jnp.where(lower, -sin_tab, sin_tab)

    def column(c, bias_ref, k):
        bias = bias_ref[pl.ds(k * HEAD, HEAD)].astype(f32).reshape(1, HEAD)
        return proj_ref[:, c * HEAD:(c + 1) * HEAD] + bias

    def rotate(v):
        return (v * cos_tab + pltpu.roll(v, HEAD // 2, 1) * sin_tab).astype(bf).astype(f32)

    qs[...] = jnp.zeros_like(qs)
    for h in range(heads):
        qs[:, h, :] = rotate(column(h, bq_ref, h))
    kn[...] = rotate(column(heads, bk_ref, 0))
    vn[...] = column(heads + 1, bv_ref, 0)

    def body(g, carry):
        for cp in moves(g, False):
            cp.wait()
        lens, scores = [], []
        times = lax.broadcasted_iota(jnp.int32, (8, seq), 1)
        slots = lax.broadcasted_iota(jnp.int32, (16, HEAD), 0)
        for r in range(GROUP_ROWS):
            b = g * GROUP_ROWS + r
            p = seq_ref[b]
            slab = pl.multiple_of((p // 16) * 16, 16)
            hit = slots == p - slab
            for cache, new in ((kc, kn), (vc, vn)):
                old = cache[b, pl.ds(slab, 16), :].astype(f32)
                cache[b, pl.ds(slab, 16), :] = jnp.where(hit, new[pl.ds(b, 1), :], old).astype(bf)
            s = lax.dot_general(qs[b].astype(bf), kc[b], (((1,), (1,)), ((), ())), preferred_element_type=f32) * HEAD ** -0.5
            scores.append(jnp.where(times <= p, s, -jnp.inf))
        s = jnp.concatenate(scores, axis=0)
        w = jnp.exp(s - jnp.max(s, axis=1, keepdims=True))
        total = jnp.sum(w, axis=1, keepdims=True)
        w = w.astype(bf)
        for r in range(GROUP_ROWS):
            b = g * GROUP_ROWS + r
            o = jnp.dot(w[8 * r:8 * r + 8], vc[b], preferred_element_type=f32)
            os[b] = o / total[8 * r:8 * r + 8]
        for cp in moves(g, True):
            cp.start()
        return carry

    lax.fori_loop(0, groups, body, 0)
    for h in range(heads):
        attn_ref[:, h * HEAD:(h + 1) * HEAD] = os[:, h, :].astype(bf)
    for g in range(groups):
        for cp in moves(g, True):
            cp.wait()


def attn_call(seq_lens, projected, b_q, b_k, b_v, k_cache, v_cache):
    rows, seq = k_cache.shape[0], k_cache.shape[1]
    f32, bf = jnp.float32, jnp.bfloat16
    freq = (ROPE_THETA ** (-2.0 * np.arange(HEAD // 2) / HEAD)).astype(np.float32)
    freq = jnp.asarray(np.concatenate([freq, freq])[None])
    any_spec, vmem, smem = pl.BlockSpec(memory_space=pl.ANY), pl.BlockSpec(memory_space=pltpu.VMEM), pl.BlockSpec(memory_space=pltpu.SMEM)
    dma = pltpu.SemaphoreType.DMA
    cache = jax.ShapeDtypeStruct((rows, seq, HEAD), bf)
    return pl.pallas_call(
        attn_kernel,
        name="attn",
        out_shape=(jax.ShapeDtypeStruct((rows, b_q.shape[0]), bf), cache, cache),
        in_specs=[smem, vmem, vmem, vmem, vmem, vmem, any_spec, any_spec],
        out_specs=(vmem, any_spec, any_spec),
        scratch_shapes=[
            pltpu.VMEM((rows, seq, HEAD), bf), pltpu.VMEM((rows, seq, HEAD), bf), pltpu.VMEM((rows, 8, HEAD), f32), pltpu.VMEM((rows, HEAD), f32),
            pltpu.VMEM((rows, HEAD), f32), pltpu.VMEM((rows, 8, HEAD), f32), pltpu.VMEM((rows, HEAD), f32),
            dma((2, rows // GROUP_ROWS)), dma((2, rows // GROUP_ROWS)),
        ],
        compiler_params=pltpu.CompilerParams(vmem_limit_bytes=VMEM_LIMIT),
    )(seq_lens, projected, b_q, b_k, b_v, freq, k_cache.reshape(rows, seq, HEAD), v_cache.reshape(rows, seq, HEAD))


def solution(mesh):
    mx_size = mesh.shape["mx"]
    act_spec = P(None, "mx")
    cache_spec = P("mx", None, "my", None)
    in_specs = (act_spec, P("mx"), P("mx"), P("mx"), P("mx", "my"), P("my"), P("mx", "my"), P("my"), P("mx", "my"), P("my"), P("my", "mx"), P("mx", "my"), P("mx", "my"), P("my", "mx"), cache_spec, cache_spec)
    out_specs = (act_spec, cache_spec, cache_spec)

    def local_layer(x_in, seq_lens, gain_attn, gain_mlp, w_q, b_q, w_k, b_k, w_v, b_v, w_o, w_gate, w_up, w_down, k_cache, v_cache):
        hidden = x_in.shape[1] * mx_size
        projected = qkv_call(x_in, gain_attn, w_q, w_k, w_v, hidden)
        attn_rows, k_out, v_out = attn_call(seq_lens, projected, b_q, b_k, b_v, k_cache, v_cache)
        pieces = mlp_call(x_in, gain_mlp, attn_rows, w_o, w_gate.T, w_up.T, w_down, hidden)
        x_out = place_call(pieces, x_in.shape)
        k_cache_out, v_cache_out = k_out.reshape(k_cache.shape), v_out.reshape(v_cache.shape)
        return x_out, k_cache_out, v_cache_out

    return jax.shard_map(local_layer, mesh=mesh, in_specs=in_specs, out_specs=out_specs, check_vma=False)
```

```python
import functools

import jax
import jax.numpy as jnp
import numpy as np
from jax import lax
from jax.experimental import pallas as pl
from jax.experimental.pallas import tpu as pltpu
from jax.sharding import PartitionSpec as P

HEAD = 128
NORM_EPS = 1e-6
ROPE_THETA = 1000000.0
MESH = pl.DeviceIdType.MESH
CHUNK = 512
TILE = 256
ROWS = 64
LAG_B, LAG_C, LAG_D, LAG_E, LAG_RS = 1, 4, 7, 8, 8
VMEM_LIMIT = 67043328
MLP_LIMIT = 48 * 1024 * 1024
ATTN_LIMIT = 14 * 1024 * 1024
QKV_LIMIT = 8 * 1024 * 1024


def rcopy(src, dst, send_sem, recv_sem, dev):
    return pltpu.make_async_remote_copy(src_ref=src, dst_ref=dst, send_sem=send_sem, recv_sem=recv_sem, device_id=dev, device_id_type=MESH)


def pinned(x):
    return pltpu.with_memory_space_constraint(x, pltpu.HBM)


def lane_ids():
    return lax.broadcasted_iota(jnp.int32, (8, 128), 1)


def pack_column(blocks):
    tile = jnp.zeros((8, 128), jnp.float32)
    lanes = lane_ids()
    for k, block in enumerate(blocks):
        tile = jnp.where(lanes == k, block, tile)
    return tile


def unpack_column(tile, k):
    return jnp.sum(jnp.where(lane_ids() == k, tile, 0.0), axis=1, keepdims=True)


def qkv_kernel(hidden, x_hbm, gain_hbm, wq_hbm, wk_hbm, wv_hbm, out_ref, gain_ref, x_v, wq_v, wk_v, wv_v, st_own, st_in, nrm, pp, dr, own, xs, xr, ld_sem, send_sem, st_sem, d_sem, x_sem):
    mx = lax.axis_index("mx")
    xi, ci = mx // 2, mx % 2
    partner, xpeer = 2 * xi + (1 - ci), 2 * (1 - xi) + ci
    loads = [pltpu.make_async_copy(s, d, ld_sem.at[i]) for i, (s, d) in enumerate([(x_hbm, x_v), (gain_hbm, gain_ref), (wq_hbm, wq_v), (wk_hbm, wk_v), (wv_hbm, wv_v)])]
    for ld in loads:
        ld.start()
    barrier = pltpu.get_barrier_semaphore()
    for d in range(1, 4):
        pl.semaphore_signal(barrier, inc=1, device_id={"mx": (mx + d) % 4}, device_id_type=MESH)
    with jax.named_scope('q_barrier'):
        pl.semaphore_wait(barrier, 3)

    rows = x_v.shape[0]
    with jax.named_scope('q_xload'):
        loads[0].wait()
    blocks = []
    for k in range(rows // 8):
        v = x_v[8 * k:8 * k + 8, :].astype(jnp.float32)
        blocks.append(jnp.sum(v * v, axis=1, keepdims=True))
    tile = pack_column(blocks)
    st_own[...] = tile
    st_in[mx] = tile
    for d in range(1, 4):
        rcopy(st_own, st_in.at[mx], send_sem.at[0], st_sem, {"mx": (mx + d) % 4}).start()
    with jax.named_scope('q_wload'):
        for ld in loads[1:]:
            ld.wait()
    with jax.named_scope('q_stat'):
        rcopy(st_in.at[pl.ds(0, 3)], st_in.at[pl.ds(0, 3)], send_sem.at[0], st_sem, {"mx": partner}).wait()
    total = st_in[0] + st_in[1] + st_in[2] + st_in[3]
    scale = lax.rsqrt(total / hidden + NORM_EPS)
    gain = gain_ref[...].astype(jnp.float32).reshape(1, x_v.shape[1])
    for k in range(0, rows // 8, 2):
        col = jnp.concatenate([unpack_column(scale, k), unpack_column(scale, k + 1)], axis=0)
        nrm[8 * k:8 * k + 16, :] = (x_v[8 * k:8 * k + 16, :].astype(jnp.float32) * col * gain).astype(jnp.bfloat16)

    lhs = nrm[...]
    part = rows // 4
    off = 0
    for w in (wq_v, wk_v, wv_v):
        width = w.shape[1]
        for c0 in range(0, width, 256):
            cw = min(256, width - c0)
            r = jnp.dot(lhs, w[:, c0:c0 + cw], preferred_element_type=jnp.float32).astype(jnp.bfloat16)
            for m in range(4):
                pp[m % 2, m // 2, :, off + c0:off + c0 + cw] = r[m * part:(m + 1) * part]
        off += width
    rcopy(pp.at[1 - ci], dr, send_sem.at[1], d_sem, {"mx": partner}).start()
    with jax.named_scope('q_d2d'):
        rcopy(pp.at[1 - ci], dr, send_sem.at[1], d_sem, {"mx": partner}).wait_recv()
    xs[...] = (pp[ci, 1 - xi].astype(jnp.float32) + dr[1 - xi].astype(jnp.float32)).astype(jnp.bfloat16)
    out = rcopy(xs, xr, send_sem.at[2], x_sem, {"mx": xpeer})
    out.start()
    own[...] = pp[ci, xi].astype(jnp.float32) + dr[xi].astype(jnp.float32)
    with jax.named_scope('q_x'):
        out.wait_recv()
    out_ref[...] = own[...] + xr[...].astype(jnp.float32)
    out.wait_send()
    rcopy(pp.at[1 - ci], dr, send_sem.at[1], d_sem, {"mx": partner}).wait_send()


def qkv_call(x_in, gain, w_q, w_k, w_v, hidden):
    rows, cols = x_in.shape
    width = w_q.shape[1] + w_k.shape[1] + w_v.shape[1]
    bf, f32 = jnp.bfloat16, jnp.float32
    any_spec, vmem = pl.BlockSpec(memory_space=pl.ANY), pl.BlockSpec(memory_space=pltpu.VMEM)
    part = rows // 4
    return pl.pallas_call(
        functools.partial(qkv_kernel, hidden),
        name="qkv",
        out_shape=jax.ShapeDtypeStruct((part, width), f32),
        in_specs=[any_spec] * 5,
        out_specs=vmem,
        scratch_shapes=[
            pltpu.VMEM(gain.shape, bf),
            pltpu.VMEM((rows, cols), bf), pltpu.VMEM(w_q.shape, bf), pltpu.VMEM(w_k.shape, bf), pltpu.VMEM(w_v.shape, bf),
            pltpu.VMEM((8, 128), f32), pltpu.VMEM((4, 8, 128), f32), pltpu.VMEM((rows, cols), bf),
            pltpu.VMEM((2, 2, part, width), bf), pltpu.VMEM((2, part, width), bf), pltpu.VMEM((part, width), f32),
            pltpu.VMEM((part, width), bf), pltpu.VMEM((part, width), bf),
            pltpu.SemaphoreType.DMA((5,)), pltpu.SemaphoreType.DMA((3,)), pltpu.SemaphoreType.DMA, pltpu.SemaphoreType.DMA, pltpu.SemaphoreType.DMA,
        ],
        compiler_params=pltpu.CompilerParams(collective_id=0, has_side_effects=True, vmem_limit_bytes=QKV_LIMIT),
        cost_estimate=pl.CostEstimate(flops=10 ** 10, bytes_accessed=3 * 10 ** 6, transcendentals=0),
    )(pinned(x_in), pinned(gain), pinned(w_q), pinned(w_k), pinned(w_v))


def mlp_kernel(hidden, x_v, gain_ref, attn_ref, wo_v, wg_hbm, wu_hbm, wd_hbm, ag2,
               wg_v, wu_v, wd_v, attn_v, p1, rs1, mp, ag1, st_own, st_in, st_sum, st_all, h2,
               pp, dr, own, xs, xr, act, dacc, p2, rs2, mo, eye,
               ld_sem, send_sem, at_sem, rs1_sem, ag1_sem, st_sem, sg_sem, rs2_sem, ag2_sem, d_sem, x_sem, ax_sem, ad_sem, af_sem):
    my, mx = lax.axis_index("my"), lax.axis_index("mx")
    n_my = 8
    xi, ci = mx // 2, mx % 2
    zi, yi = my // 2, my % 2
    partner, xpeer = 2 * xi + (1 - ci), 2 * (1 - xi) + ci
    core_dev, x_dev = {"mx": partner}, {"mx": xpeer}
    n_h = h2.shape[0]
    ff = wg_hbm.shape[0]
    n_j = pl.cdiv(ff, CHUNK)
    steps = n_h * n_j
    half = x_v.shape[1] // 2
    brows = attn_ref.shape[0]
    f32, bf = jnp.float32, jnp.bfloat16

    n_k = wg_v.shape[0]
    tiles = [(src.at[:, pl.ds(TILE * k, TILE)], dst.at[k, pl.ds(0, ff)]) for src, dst in ((wg_hbm, wg_v), (wu_hbm, wu_v)) for k in range(n_k)]
    loads = [pltpu.make_async_copy(s, d, ld_sem.at[i]) for i, (s, d) in enumerate(tiles + [(wd_hbm, wd_v.at[pl.ds(0, ff)])])]
    for ld in loads:
        ld.start()
    barrier = pltpu.get_barrier_semaphore()
    for d in range(1, 4):
        pl.semaphore_signal(barrier, inc=1, device_id={"mx": (mx + d) % 4}, device_id_type=MESH)
    for d in range(1, n_my):
        pl.semaphore_signal(barrier, inc=1, device_id={"my": (my + d) % n_my}, device_id_type=MESH)
    with jax.named_scope('m_barrier'):
        pl.semaphore_wait(barrier, 3 + n_my - 1)

    mine = pl.ds(pl.multiple_of(mx * 16, 16), 16)
    for h in range(n_h):
        for d in range(1, 4):
            rcopy(attn_ref.at[pl.ds(16 * h, 16)], attn_v.at[h, mine], send_sem.at[0], at_sem.at[h], {"mx": (mx + d) % 4}).start()
    for h in range(n_h):
        attn_v[h, mine, :] = attn_ref[16 * h:16 * h + 16, :]
    dacc[...] = jnp.zeros_like(dacc)
    wd_v[ff:, :] = jnp.zeros((wd_v.shape[0] - ff, wd_v.shape[1]), bf)
    for w in (wg_v, wu_v):
        for k in range(n_k):
            w[k, ff:, :] = jnp.zeros((w.shape[1] - ff, TILE), bf)
    eye[...] = (lax.broadcasted_iota(jnp.int32, (TILE, TILE), 0) == lax.broadcasted_iota(jnp.int32, (TILE, TILE), 1)).astype(f32).astype(bf)

    zs = (3 - zi, (zi + 2) % 4, zi + 1 - 2 * (zi % 2), zi)
    peers = [2 * z + y for z in zs for y in (1 - yi, yi)][:-1]

    def project(h):
        with jax.named_scope("m_project"):
            gathered = attn_v.at[h, pl.ds(0, 48)]
            rcopy(gathered, gathered, send_sem.at[0], at_sem.at[h], core_dev).wait_recv()
            for y in range(2):
                r = jnp.dot(attn_v[h], wo_v[:, y * half:(y + 1) * half], preferred_element_type=f32).astype(bf)
                for z in range(4):
                    p1[h, 2 * z + y] = r[16 * z:16 * z + 16]

    parts = ((0, TILE), (TILE, half))

    def send_rs(p, rs, h, ssem, rsem):
        for i, (lo, hi) in enumerate(parts):
            cols = pl.ds(lo, hi - lo)
            for k, peer in enumerate(peers):
                rcopy(p.at[h, peer, :, cols], rs.at[h, k, :, cols], ssem, rsem.at[h, i], {"my": peer}).start()

    def finish_rs(p, rs, h, i, ssem, rsem, base):
        lo, hi = parts[i]
        seven = rs.at[h, :, :, pl.ds(lo, hi - lo)]
        rcopy(seven, seven, ssem, rsem.at[h, i], {"my": my}).wait_recv()
        total = p[h, my, :, lo:hi].astype(f32)
        for k in range(n_my - 1):
            total += rs[h, k, :, lo:hi].astype(f32)
        return (base + total).astype(bf)

    def send_ag(piece, ag, h, ssem, rsem, i=None):
        src, dst, sem = piece.at[h], ag.at[h, my], rsem.at[h]
        if i is not None:
            cols = pl.ds(parts[i][0], parts[i][1] - parts[i][0])
            src, dst, sem = piece.at[h, :, cols], ag.at[h, my, :, cols], rsem.at[h, i]
        for peer in peers:
            rcopy(src, dst, ssem, sem, {"my": peer}).start()

    def wait_ag(ag, h, ssem, rsem, i=None):
        seven, sem = ag.at[h, pl.ds(0, n_my - 1)], rsem.at[h] if i is None else rsem.at[h, i]
        if i is not None:
            seven = ag.at[h, pl.ds(0, n_my - 1), :, pl.ds(parts[i][0], parts[i][1] - parts[i][0])]
        rcopy(seven, seven, ssem, sem, {"my": my}).wait_recv()

    def rs1_send(h):
        with jax.named_scope("m_rs1_send"):
            send_rs(p1, rs1, h, send_sem.at[1], rs1_sem)

    def rs1_finish(h):
        with jax.named_scope("m_rs1_finish"):
            ss = jnp.zeros((16, 1), f32)
            for i, (lo, hi) in enumerate(parts):
                r0 = pl.multiple_of(zi * brows + h * 16, 16)
                base = x_v[pl.ds(r0, 16), pl.ds(pl.multiple_of(yi * half + lo, 128), hi - lo)].astype(f32)
                m = finish_rs(p1, rs1, h, i, send_sem.at[1], rs1_sem, base)
                mp[h, :, lo:hi] = m
                ag1[h, my, :, lo:hi] = m
                send_ag(mp, ag1, h, send_sem.at[2], ag1_sem, i)
                m = m.astype(f32)
                ss += jnp.sum(m * m, axis=1, keepdims=True)
            tile = pack_column([ss[:8], ss[8:]])
            st_own[h] = tile
            st_in[h, mx] = tile
            for d in range(1, 4):
                rcopy(st_own.at[h], st_in.at[h, mx], send_sem.at[3], st_sem.at[h], {"mx": (mx + d) % 4}).start()

    def stat_gather(h):
        with jax.named_scope("m_stat_gather"):
            three = st_in.at[h, pl.ds(0, 3)]
            rcopy(three, three, send_sem.at[3], st_sem.at[h], core_dev).wait_recv()
            total = st_in[h, 0] + st_in[h, 1] + st_in[h, 2] + st_in[h, 3]
            st_sum[h] = total
            st_all[h, my] = total
            send_ag(st_sum, st_all, h, send_sem.at[11], sg_sem)

    def norm(h):
        with jax.named_scope("m_norm"):
            wait_ag(st_all, h, send_sem.at[11], sg_sem)
            for i in range(2):
                wait_ag(ag1, h, send_sem.at[2], ag1_sem, i)
            for z in range(4):
                scale = lax.rsqrt((st_all[h, 2 * z] + st_all[h, 2 * z + 1]) / hidden + NORM_EPS)
                col = jnp.concatenate([unpack_column(scale, 0), unpack_column(scale, 1)], axis=0)
                for y in range(2):
                    gain = gain_ref[pl.ds(y * half, half)].astype(f32).reshape(1, half)
                    h2[h, 16 * z:16 * z + 16, y * half:(y + 1) * half] = (ag1[h, 2 * z + y].astype(f32) * col * gain).astype(bf)

    def transpose(i, carry):
        with jax.named_scope("m_transpose"):
            rows = pl.ds(pl.multiple_of(i * TILE, TILE), TILE)
            for k in range(n_k):
                flipped = [lax.dot_general(eye[...], w[k, rows, :], (((1,), (1,)), ((), ())), preferred_element_type=f32).astype(bf) for w in (wg_v, wu_v)]
                for w, val in zip((wg_v, wu_v), flipped):
                    w[k, rows, :] = val
            return carry

    def stage_a(s):
        with jax.named_scope("m_stage_a"):
            h, j = s // n_j, s % n_j
            lhs = h2[h]
            for i, w in enumerate((wg_v, wu_v)):
                cols = []
                for n in range(CHUNK // TILE):
                    rows = pl.ds(pl.multiple_of(j * CHUNK + n * TILE, TILE), TILE)
                    acc = jnp.dot(lhs[:, :TILE], w[0, rows, :], preferred_element_type=f32)
                    for k in range(1, n_k):
                        acc += jnp.dot(lhs[:, TILE * k:TILE * (k + 1)], w[k, rows, :], preferred_element_type=f32)
                    cols.append(acc.astype(bf))
                val = jnp.concatenate(cols, axis=1)
                for m in range(4):
                    pp[s, m % 2, m // 2, :, i * CHUNK:(i + 1) * CHUNK] = val[16 * m:16 * m + 16]
            rcopy(pp.at[s, 1 - ci], dr.at[s], send_sem.at[4], d_sem.at[s], core_dev).start()

    def stage_b(s):
        with jax.named_scope("m_stage_b"):
            rcopy(pp.at[s, 1 - ci], dr.at[s], send_sem.at[4], d_sem.at[s], core_dev).wait_recv()
            xs[s] = (pp[s, ci, 1 - xi].astype(f32) + dr[s, 1 - xi].astype(f32)).astype(bf)
            rcopy(xs.at[s], xr.at[s], send_sem.at[5], x_sem.at[s], x_dev).start()
            own[s] = pp[s, ci, xi].astype(f32) + dr[s, xi].astype(f32)

    def stage_c(s):
        with jax.named_scope("m_stage_c"):
            rcopy(xs.at[s], xr.at[s], send_sem.at[5], x_sem.at[s], x_dev).wait_recv()
            g = own[s, :, :CHUNK] + xr[s, :, :CHUNK].astype(f32)
            u = own[s, :, CHUNK:] + xr[s, :, CHUNK:].astype(f32)
            act[s, mx] = (jax.nn.silu(g) * u).astype(bf)
            rcopy(act.at[s, mx], act.at[s, mx], send_sem.at[6], ax_sem.at[s], x_dev).start()
            rcopy(act.at[s, mx], act.at[s, mx], send_sem.at[7], ad_sem.at[s], core_dev).start()

    def stage_d(s):
        with jax.named_scope("m_stage_d"):
            rcopy(act.at[s, xpeer], act.at[s, xpeer], send_sem.at[6], ax_sem.at[s], x_dev).wait_recv()
            rcopy(act.at[s, xpeer], act.at[s, xpeer], send_sem.at[8], af_sem.at[s], core_dev).start()

    def stage_e(s):
        with jax.named_scope("m_stage_e"):
            h, j = s // n_j, s % n_j
            rcopy(act.at[s, 0], act.at[s, 0], send_sem.at[7], ad_sem.at[s], core_dev).wait_recv()
            rcopy(act.at[s, 0], act.at[s, 0], send_sem.at[8], af_sem.at[s], core_dev).wait_recv()
            lhs = act[s].reshape(ROWS, CHUNK)
            dacc[h] += jnp.dot(lhs, wd_v[pl.ds(pl.multiple_of(j * CHUNK, CHUNK), CHUNK), :], preferred_element_type=f32)

    def rs2_send(h):
        with jax.named_scope("m_rs2_send"):
            for z in range(4):
                for y in range(2):
                    p2[h, 2 * z + y] = dacc[h, 16 * z:16 * z + 16, y * half:(y + 1) * half].astype(bf)
            send_rs(p2, rs2, h, send_sem.at[9], rs2_sem)

    def rs2_finish(h):
        with jax.named_scope("m_rs2_finish"):
            for i, (lo, hi) in enumerate(parts):
                o = finish_rs(p2, rs2, h, i, send_sem.at[9], rs2_sem, mp[h, :, lo:hi].astype(f32))
                mo[h, :, lo:hi] = o
                ag2[h, my, :, lo:hi] = o
                send_ag(mo, ag2, h, send_sem.at[10], ag2_sem, i)

    n_t = n_j * (CHUNK // TILE)
    project(0)
    rs1_send(0)
    project(1)
    rs1_send(1)
    project(2)
    for ld in loads[:-1]:
        ld.wait()
    lax.fori_loop(0, n_t // 2, transpose, 0)
    rs1_finish(0)
    lax.fori_loop(n_t // 2, n_t // 2 + 3, transpose, 0)
    stat_gather(0)
    rs1_finish(1)
    rs1_send(2)
    lax.fori_loop(n_t // 2 + 3, n_t, transpose, 0)
    stat_gather(1)
    norm(0)

    def body(t, carry):
        @pl.when(t == n_j)
        def _():
            norm(1)

        @pl.when(t == 2 * n_j)
        def _():
            norm(2)

        @pl.when(t == n_j + 1)
        def _():
            rs1_finish(2)

        @pl.when(t == n_j + 4)
        def _():
            stat_gather(2)

        @pl.when(t < steps)
        def _():
            stage_a(t)

        @pl.when((t >= LAG_B) & (t < steps + LAG_B))
        def _():
            stage_b(t - LAG_B)

        @pl.when((t >= LAG_C) & (t < steps + LAG_C))
        def _():
            stage_c(t - LAG_C)

        @pl.when((t >= LAG_D) & (t < steps + LAG_D))
        def _():
            stage_d(t - LAG_D)

        @pl.when(t == LAG_E)
        def _():
            loads[-1].wait()

        @pl.when(t >= LAG_E)
        def _():
            s = t - LAG_E
            stage_e(s)

            @pl.when(s % n_j == n_j - 1)
            def _():
                rs2_send(s // n_j)

        lag2 = LAG_RS

        @pl.when((t >= LAG_E + n_j - 1 + lag2) & ((t - LAG_E - (n_j - 1) - lag2) % n_j == 0))
        def _():
            rs2_finish((t - LAG_E - (n_j - 1) - lag2) // n_j)

        return carry

    total_t = steps + LAG_E
    lax.fori_loop(0, total_t, body, 0)
    done = len([h for h in range(n_h) if LAG_E + n_j - 1 + LAG_RS + h * n_j < total_t])
    for h in range(done, n_h):
        rs2_finish(h)
    for h in range(n_h):
        for i in range(2):
            wait_ag(ag2, h, send_sem.at[10], ag2_sem, i)
    for k, ref in ((0, attn_v.at[:, pl.ds(0, 48)]), (11, st_all.at[:, pl.ds(0, 7)]), (1, rs1), (2, rs1), (3, st_in.at[:, pl.ds(0, 3)]), (4, dr), (5, xs), (6, act.at[:, 0]), (7, act.at[:, 0]), (8, act.at[:, 0]), (9, rs2), (10, rs2)):
        rcopy(ref, ref, send_sem.at[k], at_sem.at[0], core_dev).wait_send()


def mlp_call(x_in, gain, attn, w_o, w_gate, w_up, w_down, hidden):
    rows, cols = x_in.shape
    ff = w_gate.shape[0]
    n_j = pl.cdiv(ff, CHUNK)
    n_h = rows // ROWS
    steps = n_h * n_j
    half = cols // 2
    bf, f32 = jnp.bfloat16, jnp.float32
    hbm, vmem = pl.BlockSpec(memory_space=pltpu.HBM), pl.BlockSpec(memory_space=pltpu.VMEM)
    dma = pltpu.SemaphoreType.DMA
    return pl.pallas_call(
        functools.partial(mlp_kernel, hidden),
        name="mlp",
        out_shape=jax.ShapeDtypeStruct((n_h, 8, 16, half), bf),
        in_specs=[vmem, vmem, vmem, vmem, hbm, hbm, hbm],
        out_specs=vmem,
        scratch_shapes=[
            pltpu.VMEM((cols // TILE, n_j * CHUNK, TILE), bf), pltpu.VMEM((cols // TILE, n_j * CHUNK, TILE), bf),
            pltpu.VMEM((n_j * CHUNK, cols), bf), pltpu.VMEM((n_h, 64, attn.shape[1]), bf),
            pltpu.VMEM((n_h, 8, 16, half), bf), pltpu.VMEM((n_h, 7, 16, half), bf), pltpu.VMEM((n_h, 16, half), bf), pltpu.VMEM((n_h, 8, 16, half), bf),
            pltpu.VMEM((n_h, 8, 128), f32), pltpu.VMEM((n_h, 4, 8, 128), f32), pltpu.VMEM((n_h, 8, 128), f32), pltpu.VMEM((n_h, 8, 8, 128), f32), pltpu.VMEM((n_h, ROWS, cols), bf),
            pltpu.VMEM((steps, 2, 2, 16, 2 * CHUNK), bf), pltpu.VMEM((steps, 2, 16, 2 * CHUNK), bf), pltpu.VMEM((steps, 16, 2 * CHUNK), f32),
            pltpu.VMEM((steps, 16, 2 * CHUNK), bf), pltpu.VMEM((steps, 16, 2 * CHUNK), bf), pltpu.VMEM((steps, 4, 16, CHUNK), bf),
            pltpu.VMEM((n_h, ROWS, cols), f32),
            pltpu.VMEM((n_h, 8, 16, half), bf), pltpu.VMEM((n_h, 7, 16, half), bf), pltpu.VMEM((n_h, 16, half), bf), pltpu.VMEM((TILE, TILE), bf),
            dma((1 + 2 * (cols // TILE),)), dma((12,)), dma((n_h,)), dma((n_h, 2)), dma((n_h, 2)), dma((n_h,)), dma((n_h,)), dma((n_h, 2)), dma((n_h, 2)),
            dma((steps,)), dma((steps,)), dma((steps,)), dma((steps,)), dma((steps,)),
        ],
        compiler_params=pltpu.CompilerParams(collective_id=1, has_side_effects=True, vmem_limit_bytes=MLP_LIMIT),
    )(x_in, gain, attn, w_o, pinned(w_gate), pinned(w_up), pinned(w_down))


def place_kernel(pieces_ref, out_ref):
    n_h, _, _, half = pieces_ref.shape
    for h in range(n_h):
        for z in range(4):
            for y in range(2):
                r0 = z * 16 * n_h + h * 16
                out_ref[r0:r0 + 16, y * half:(y + 1) * half] = pieces_ref[h, 2 * z + y]


def place_call(pieces, shape):
    vmem = pl.BlockSpec(memory_space=pltpu.VMEM)
    return pl.pallas_call(place_kernel, name="place", out_shape=jax.ShapeDtypeStruct(shape, pieces.dtype), in_specs=[vmem], out_specs=vmem, compiler_params=pltpu.CompilerParams(vmem_limit_bytes=4 * 1024 * 1024))(pieces)


GROUP_ROWS = 16


def attn_kernel(seq_ref, proj_ref, bq_ref, bk_ref, bv_ref, freq_ref, k_ref, v_ref, attn_ref, ko_hbm, vo_hbm, qs, kn, vn, os, pos, patch, out_sem, patch_sem):
    f32, bf = jnp.float32, jnp.bfloat16
    rows, seq = k_ref.shape[0], k_ref.shape[1]
    heads = attn_ref.shape[1] // HEAD
    groups = rows // GROUP_ROWS
    outs = [ko_hbm, vo_hbm]

    def bulk(g):
        part = pl.ds(g * GROUP_ROWS, GROUP_ROWS)
        return [pltpu.make_async_copy(src.at[part], dst.at[part], out_sem.at[i, g]) for i, (src, dst) in enumerate(zip((k_ref, v_ref), outs))]

    for g in range(groups):
        for cp in bulk(g):
            cp.start()
    for b in range(rows):
        pos[b:b + 1, :] = jnp.full((1, HEAD), seq_ref[b], jnp.int32).astype(f32)
    angles = pos[...] * freq_ref[...]
    lower = lax.broadcasted_iota(jnp.int32, (rows, HEAD), 1) < HEAD // 2
    cos_tab = jnp.cos(angles)
    sin_tab = jnp.sin(angles)
    sin_tab = jnp.where(lower, -sin_tab, sin_tab)

    def column(c, bias_ref, k):
        bias = bias_ref[pl.ds(k * HEAD, HEAD)].astype(f32).reshape(1, HEAD)
        return proj_ref[:, c * HEAD:(c + 1) * HEAD] + bias

    def rotate(v):
        return (v * cos_tab + pltpu.roll(v, HEAD // 2, 1) * sin_tab).astype(bf).astype(f32)

    with jax.named_scope('a_pre'):
        qs[...] = jnp.zeros_like(qs)
    for h in range(heads):
        qs[:, h, :] = rotate(column(h, bq_ref, h))
    kn[...] = rotate(column(heads, bk_ref, 0))
    vn[...] = column(heads + 1, bv_ref, 0).astype(bf).astype(f32)

    def slab_of(b):
        p = seq_ref[b]
        return p, pl.multiple_of((p // 16) * 16, 16)

    def body(g, carry):
        times = lax.broadcasted_iota(jnp.int32, (8, seq), 1)
        slots = lax.broadcasted_iota(jnp.int32, (16, HEAD), 0)
        scores, news, hits = [], [], []
        for r in range(GROUP_ROWS):
            b = g * GROUP_ROWS + r
            p, slab = slab_of(b)
            hit = slots == p - slab
            for i, (cache, new) in enumerate(((k_ref, kn), (v_ref, vn))):
                old = cache[b, pl.ds(slab, 16), :].astype(f32)
                patch[i, b] = jnp.where(hit, new[pl.ds(b, 1), :], old).astype(bf)
            q = qs[b]
            s = lax.dot_general(q.astype(bf), k_ref[b], (((1,), (1,)), ((), ())), preferred_element_type=f32) * HEAD ** -0.5
            s_new = jnp.sum(q * kn[pl.ds(b, 1), :], axis=1, keepdims=True) * HEAD ** -0.5
            hits.append(times == p)
            news.append(s_new)
            scores.append(jnp.where(hits[r], s_new, jnp.where(times < p, s, -jnp.inf)))
        s = jnp.concatenate(scores, axis=0)
        top = jnp.max(s, axis=1, keepdims=True)
        w = jnp.exp(s - top)
        total = jnp.sum(w, axis=1, keepdims=True)
        w_new = jnp.exp(jnp.concatenate(news, axis=0) - top).astype(bf).astype(f32)
        w = jnp.where(jnp.concatenate(hits, axis=0), 0.0, w).astype(bf)
        for r in range(GROUP_ROWS):
            b = g * GROUP_ROWS + r
            part = slice(8 * r, 8 * r + 8)
            o = jnp.dot(w[part], v_ref[b], preferred_element_type=f32) + w_new[part] * vn[pl.ds(b, 1), :]
            os[b] = o / total[part]
        return carry

    with jax.named_scope('a_main'):
        lax.fori_loop(0, groups, body, 0)
    for h in range(heads):
        attn_ref[:, h * HEAD:(h + 1) * HEAD] = os[:, h, :].astype(bf)

    def patches(b):
        slab = slab_of(b)[1]
        return [pltpu.make_async_copy(patch.at[i, b], dst.at[b, pl.ds(slab, 16)], patch_sem.at[i]) for i, dst in enumerate(outs)]

    for g in range(groups):
        with jax.named_scope('a_bulk'):
            for cp in bulk(g):
                cp.wait()
        for b in range(g * GROUP_ROWS, (g + 1) * GROUP_ROWS):
            for cp in patches(b):
                cp.start()
    with jax.named_scope('a_patch'):
        for b in range(rows):
            for cp in patches(b):
                cp.wait()


def attn_call(seq_lens, projected, b_q, b_k, b_v, k_cache, v_cache):
    rows, seq = k_cache.shape[0], k_cache.shape[1]
    f32, bf = jnp.float32, jnp.bfloat16
    freq = (ROPE_THETA ** (-2.0 * np.arange(HEAD // 2) / HEAD)).astype(np.float32)
    freq = jnp.asarray(np.concatenate([freq, freq])[None])
    any_spec, vmem, smem = pl.BlockSpec(memory_space=pl.ANY), pl.BlockSpec(memory_space=pltpu.VMEM), pl.BlockSpec(memory_space=pltpu.SMEM)
    dma = pltpu.SemaphoreType.DMA
    cache = jax.ShapeDtypeStruct((rows, seq, HEAD), bf)
    return pl.pallas_call(
        attn_kernel,
        name="attn",
        out_shape=(jax.ShapeDtypeStruct((rows, b_q.shape[0]), bf), cache, cache),
        in_specs=[smem, vmem, vmem, vmem, vmem, vmem, vmem, vmem],
        out_specs=(vmem, any_spec, any_spec),
        scratch_shapes=[
            pltpu.VMEM((rows, 8, HEAD), f32), pltpu.VMEM((rows, HEAD), f32),
            pltpu.VMEM((rows, HEAD), f32), pltpu.VMEM((rows, 8, HEAD), f32), pltpu.VMEM((rows, HEAD), f32), pltpu.VMEM((2, rows, 16, HEAD), bf),
            dma((2, rows // GROUP_ROWS)), dma((2,)),
        ],
        compiler_params=pltpu.CompilerParams(vmem_limit_bytes=ATTN_LIMIT),
    )(seq_lens, projected, b_q, b_k, b_v, freq, k_cache.reshape(rows, seq, HEAD), v_cache.reshape(rows, seq, HEAD))


def solution(mesh):
    mx_size = mesh.shape["mx"]
    act_spec = P(None, "mx")
    cache_spec = P("mx", None, "my", None)
    in_specs = (act_spec, P("mx"), P("mx"), P("mx"), P("mx", "my"), P("my"), P("mx", "my"), P("my"), P("mx", "my"), P("my"), P("my", "mx"), P("mx", "my"), P("mx", "my"), P("my", "mx"), cache_spec, cache_spec)
    out_specs = (act_spec, cache_spec, cache_spec)

    def local_layer(x_in, seq_lens, gain_attn, gain_mlp, w_q, b_q, w_k, b_k, w_v, b_v, w_o, w_gate, w_up, w_down, k_cache, v_cache):
        hidden = x_in.shape[1] * mx_size
        projected = qkv_call(x_in, gain_attn, w_q, w_k, w_v, hidden)
        attn_rows, k_out, v_out = attn_call(seq_lens, projected, b_q, b_k, b_v, k_cache, v_cache)
        pieces = mlp_call(x_in, gain_mlp, attn_rows, w_o, w_gate.T, w_up.T, w_down, hidden)
        x_out = place_call(pieces, x_in.shape)
        k_cache_out, v_cache_out = k_out.reshape(k_cache.shape), v_out.reshape(v_cache.shape)
        return x_out, k_cache_out, v_cache_out

    return jax.shard_map(local_layer, mesh=mesh, in_specs=in_specs, out_specs=out_specs, check_vma=False)
```

```python
import functools

import jax
import jax.numpy as jnp
import numpy as np
from jax import lax
from jax.experimental import pallas as pl
from jax.experimental.pallas import tpu as pltpu
from jax.sharding import PartitionSpec as P

HEAD = 128
NORM_EPS = 1e-6
ROPE_THETA = 1000000.0
MESH = pl.DeviceIdType.MESH
CHUNK = 512
TILE = 256
DIRECT = 2
HOLD = 6000
ROWS = 64
LAG_B, LAG_C, LAG_D, LAG_E, LAG_RS = 1, 4, 7, 8, 8
VMEM_LIMIT = 67043328
MLP_LIMIT = 48 * 1024 * 1024
ATTN_LIMIT = 14 * 1024 * 1024
QKV_LIMIT = 8 * 1024 * 1024


def rcopy(src, dst, send_sem, recv_sem, dev):
    return pltpu.make_async_remote_copy(src_ref=src, dst_ref=dst, send_sem=send_sem, recv_sem=recv_sem, device_id=dev, device_id_type=MESH)


def pinned(x):
    return pltpu.with_memory_space_constraint(x, pltpu.HBM)


def lane_ids():
    return lax.broadcasted_iota(jnp.int32, (8, 128), 1)


def pack_column(blocks):
    tile = jnp.zeros((8, 128), jnp.float32)
    lanes = lane_ids()
    for k, block in enumerate(blocks):
        tile = jnp.where(lanes == k, block, tile)
    return tile


def unpack_column(tile, k):
    return jnp.sum(jnp.where(lane_ids() == k, tile, 0.0), axis=1, keepdims=True)


def qkv_kernel(hidden, x_hbm, gain_hbm, wq_hbm, wk_hbm, wv_hbm, out_ref, gain_ref, x_v, wq_v, wk_v, wv_v, st_own, st_in, nrm, pp, dr, own, xs, xr, ld_sem, send_sem, st_sem, d_sem, x_sem):
    mx = lax.axis_index("mx")
    xi, ci = mx // 2, mx % 2
    partner, xpeer = 2 * xi + (1 - ci), 2 * (1 - xi) + ci
    loads = [pltpu.make_async_copy(s, d, ld_sem.at[i]) for i, (s, d) in enumerate([(x_hbm, x_v), (gain_hbm, gain_ref), (wq_hbm, wq_v), (wk_hbm, wk_v), (wv_hbm, wv_v)])]
    for ld in loads:
        ld.start()
    barrier = pltpu.get_barrier_semaphore()
    for d in range(1, 4):
        pl.semaphore_signal(barrier, inc=1, device_id={"mx": (mx + d) % 4}, device_id_type=MESH)
    with jax.named_scope('q_barrier'):
        pl.semaphore_wait(barrier, 3)

    rows = x_v.shape[0]
    with jax.named_scope('q_xload'):
        loads[0].wait()
    blocks = []
    for k in range(rows // 8):
        v = x_v[8 * k:8 * k + 8, :].astype(jnp.float32)
        blocks.append(jnp.sum(v * v, axis=1, keepdims=True))
    tile = pack_column(blocks)
    st_own[...] = tile
    st_in[mx] = tile
    for d in range(1, 4):
        rcopy(st_own, st_in.at[mx], send_sem.at[0], st_sem, {"mx": (mx + d) % 4}).start()
    with jax.named_scope('q_wload'):
        for ld in loads[1:]:
            ld.wait()
    with jax.named_scope('q_stat'):
        rcopy(st_in.at[pl.ds(0, 3)], st_in.at[pl.ds(0, 3)], send_sem.at[0], st_sem, {"mx": partner}).wait()
    total = st_in[0] + st_in[1] + st_in[2] + st_in[3]
    scale = lax.rsqrt(total / hidden + NORM_EPS)
    gain = gain_ref[...].astype(jnp.float32).reshape(1, x_v.shape[1])
    for k in range(0, rows // 8, 2):
        col = jnp.concatenate([unpack_column(scale, k), unpack_column(scale, k + 1)], axis=0)
        nrm[8 * k:8 * k + 16, :] = (x_v[8 * k:8 * k + 16, :].astype(jnp.float32) * col * gain).astype(jnp.bfloat16)

    lhs = nrm[...]
    part = rows // 4
    width = out_ref.shape[1]
    offs = [0, wq_v.shape[1], wq_v.shape[1] + wk_v.shape[1]]
    pieces = [(w, c0, min(c0 + TILE, w.shape[1]), off) for w, off in zip((wq_v, wk_v, wv_v), offs) for c0 in range(0, w.shape[1], TILE)]
    cut = 2 * TILE
    parts = ((0, cut), (cut, width))

    def swap(i):
        cols = pl.ds(parts[i][0], parts[i][1] - parts[i][0])
        return rcopy(pp.at[1 - ci, :, :, cols], dr.at[:, :, cols], send_sem.at[1], d_sem.at[i], {"mx": partner})

    def cross(i):
        cols = pl.ds(parts[i][0], parts[i][1] - parts[i][0])
        return rcopy(xs.at[:, cols], xr.at[:, cols], send_sem.at[2], x_sem.at[i], {"mx": xpeer})

    for i, (lo, hi) in enumerate(parts):
        for w, c0, c1, off in pieces:
            if lo <= off + c0 < hi:
                r = jnp.dot(lhs, w[:, c0:c1], preferred_element_type=jnp.float32).astype(jnp.bfloat16)
                for m in range(4):
                    pp[m % 2, m // 2, :, off + c0:off + c1] = r[m * part:(m + 1) * part]
        swap(i).start()
    for i, (lo, hi) in enumerate(parts):
        with jax.named_scope('q_d2d'):
            swap(i).wait_recv()
        xs[:, lo:hi] = (pp[ci, 1 - xi, :, lo:hi].astype(jnp.float32) + dr[1 - xi, :, lo:hi].astype(jnp.float32)).astype(jnp.bfloat16)
        cross(i).start()
        own[:, lo:hi] = pp[ci, xi, :, lo:hi].astype(jnp.float32) + dr[xi, :, lo:hi].astype(jnp.float32)
    for i, (lo, hi) in enumerate(parts):
        with jax.named_scope('q_x'):
            cross(i).wait_recv()
        out_ref[:, lo:hi] = own[:, lo:hi] + xr[:, lo:hi].astype(jnp.float32)
    for i in range(2):
        swap(i).wait_send()
        cross(i).wait_send()


def qkv_call(x_in, gain, w_q, w_k, w_v, hidden):
    rows, cols = x_in.shape
    width = w_q.shape[1] + w_k.shape[1] + w_v.shape[1]
    bf, f32 = jnp.bfloat16, jnp.float32
    any_spec, vmem = pl.BlockSpec(memory_space=pl.ANY), pl.BlockSpec(memory_space=pltpu.VMEM)
    part = rows // 4
    return pl.pallas_call(
        functools.partial(qkv_kernel, hidden),
        name="qkv",
        out_shape=jax.ShapeDtypeStruct((part, width), f32),
        in_specs=[any_spec] * 5,
        out_specs=vmem,
        scratch_shapes=[
            pltpu.VMEM(gain.shape, bf),
            pltpu.VMEM((rows, cols), bf), pltpu.VMEM(w_q.shape, bf), pltpu.VMEM(w_k.shape, bf), pltpu.VMEM(w_v.shape, bf),
            pltpu.VMEM((8, 128), f32), pltpu.VMEM((4, 8, 128), f32), pltpu.VMEM((rows, cols), bf),
            pltpu.VMEM((2, 2, part, width), bf), pltpu.VMEM((2, part, width), bf), pltpu.VMEM((part, width), f32),
            pltpu.VMEM((part, width), bf), pltpu.VMEM((part, width), bf),
            pltpu.SemaphoreType.DMA((5,)), pltpu.SemaphoreType.DMA((3,)), pltpu.SemaphoreType.DMA, pltpu.SemaphoreType.DMA((2,)), pltpu.SemaphoreType.DMA((2,)),
        ],
        compiler_params=pltpu.CompilerParams(collective_id=0, has_side_effects=True, vmem_limit_bytes=QKV_LIMIT),
        cost_estimate=pl.CostEstimate(flops=10 ** 10, bytes_accessed=3 * 10 ** 6, transcendentals=0),
    )(pinned(x_in), pinned(gain), pinned(w_q), pinned(w_k), pinned(w_v))


def mlp_kernel(hidden, x_v, gain_ref, attn_ref, wo_v, wg_hbm, wu_hbm, wd_hbm, ag2,
               wg_v, wu_v, wd_v, attn_v, p1, rs1, mp, ag1, st_own, st_in, st_sum, st_all, h2,
               pp, dr, own, xs, xr, act, dacc, p2, rs2, mo, eye,
               ld_sem, send_sem, at_sem, rs1_sem, ag1_sem, st_sem, sg_sem, rs2_sem, ag2_sem, d_sem, x_sem, ax_sem, ad_sem, af_sem):
    my, mx = lax.axis_index("my"), lax.axis_index("mx")
    n_my = 8
    xi, ci = mx // 2, mx % 2
    zi, yi = my // 2, my % 2
    partner, xpeer = 2 * xi + (1 - ci), 2 * (1 - xi) + ci
    core_dev, x_dev = {"mx": partner}, {"mx": xpeer}
    n_h = h2.shape[0]
    ff = wg_hbm.shape[0]
    n_j = pl.cdiv(ff, CHUNK)
    steps = n_h * n_j
    half = x_v.shape[1] // 2
    brows = attn_ref.shape[0]
    f32, bf = jnp.float32, jnp.bfloat16

    n_k = wg_v.shape[0]
    tiles = [(src.at[:, pl.ds(TILE * k, TILE)], dst.at[k, pl.ds(0, ff)]) for src, dst in ((wg_hbm, wg_v), (wu_hbm, wu_v)) for k in range(n_k)]
    loads = [pltpu.make_async_copy(s, d, ld_sem.at[i]) for i, (s, d) in enumerate(tiles + [(wd_hbm, wd_v.at[pl.ds(0, ff)])])]
    for ld in loads:
        ld.start()
    barrier = pltpu.get_barrier_semaphore()
    for d in range(1, 4):
        pl.semaphore_signal(barrier, inc=1, device_id={"mx": (mx + d) % 4}, device_id_type=MESH)
    for d in range(1, n_my):
        pl.semaphore_signal(barrier, inc=1, device_id={"my": (my + d) % n_my}, device_id_type=MESH)
    with jax.named_scope('m_barrier'):
        pl.semaphore_wait(barrier, 3 + n_my - 1)

    mine = pl.ds(pl.multiple_of(mx * 16, 16), 16)
    for h in range(n_h):
        for d in range(1, 4):
            rcopy(attn_ref.at[pl.ds(16 * h, 16)], attn_v.at[h, mine], send_sem.at[0], at_sem.at[h], {"mx": (mx + d) % 4}).start()
    for h in range(n_h):
        attn_v[h, mine, :] = attn_ref[16 * h:16 * h + 16, :]
    dacc[...] = jnp.zeros_like(dacc)
    wd_v[ff:, :] = jnp.zeros((wd_v.shape[0] - ff, wd_v.shape[1]), bf)
    for w in (wg_v, wu_v):
        for k in range(n_k):
            w[k, ff:, :] = jnp.zeros((w.shape[1] - ff, TILE), bf)
    eye[...] = (lax.broadcasted_iota(jnp.int32, (TILE, TILE), 0) == lax.broadcasted_iota(jnp.int32, (TILE, TILE), 1)).astype(f32).astype(bf)

    zs = (3 - zi, (zi + 2) % 4, zi + 1 - 2 * (zi % 2), zi)
    peers = [2 * z + y for z in zs for y in (1 - yi, yi)][:-1]

    def project(h):
        with jax.named_scope("m_project"):
            gathered = attn_v.at[h, pl.ds(0, 48)]
            rcopy(gathered, gathered, send_sem.at[0], at_sem.at[h], core_dev).wait_recv()
            for y in range(2):
                r = jnp.dot(attn_v[h], wo_v[:, y * half:(y + 1) * half], preferred_element_type=f32).astype(bf)
                for z in range(4):
                    p1[h, 2 * z + y] = r[16 * z:16 * z + 16]

    parts = ((0, TILE), (TILE, half))

    def send_rs(p, rs, h, ssem, rsem):
        for i, (lo, hi) in enumerate(parts):
            cols = pl.ds(lo, hi - lo)
            for k, peer in enumerate(peers):
                rcopy(p.at[h, peer, :, cols], rs.at[h, k, :, cols], ssem, rsem.at[h, i], {"my": peer}).start()

    def finish_rs(p, rs, h, i, ssem, rsem, base):
        lo, hi = parts[i]
        seven = rs.at[h, :, :, pl.ds(lo, hi - lo)]
        rcopy(seven, seven, ssem, rsem.at[h, i], {"my": my}).wait_recv()
        total = p[h, my, :, lo:hi].astype(f32)
        for k in range(n_my - 1):
            total += rs[h, k, :, lo:hi].astype(f32)
        return (base + total).astype(bf)

    def send_ag(piece, ag, h, ssem, rsem, i=None):
        src, dst, sem = piece.at[h], ag.at[h, my], rsem.at[h]
        if i is not None:
            cols = pl.ds(parts[i][0], parts[i][1] - parts[i][0])
            src, dst, sem = piece.at[h, :, cols], ag.at[h, my, :, cols], rsem.at[h, i]
        for peer in peers:
            rcopy(src, dst, ssem, sem, {"my": peer}).start()

    def wait_ag(ag, h, ssem, rsem, i=None):
        seven, sem = ag.at[h, pl.ds(0, n_my - 1)], rsem.at[h] if i is None else rsem.at[h, i]
        if i is not None:
            seven = ag.at[h, pl.ds(0, n_my - 1), :, pl.ds(parts[i][0], parts[i][1] - parts[i][0])]
        rcopy(seven, seven, ssem, sem, {"my": my}).wait_recv()

    def rs1_send(h):
        with jax.named_scope("m_rs1_send"):
            send_rs(p1, rs1, h, send_sem.at[1], rs1_sem)

    def rs1_finish(h):
        with jax.named_scope("m_rs1_finish"):
            ss = jnp.zeros((16, 1), f32)
            for i, (lo, hi) in enumerate(parts):
                r0 = pl.multiple_of(zi * brows + h * 16, 16)
                base = x_v[pl.ds(r0, 16), pl.ds(pl.multiple_of(yi * half + lo, 128), hi - lo)].astype(f32)
                m = finish_rs(p1, rs1, h, i, send_sem.at[1], rs1_sem, base)
                mp[h, :, lo:hi] = m
                ag1[h, my, :, lo:hi] = m
                send_ag(mp, ag1, h, send_sem.at[2], ag1_sem, i)
                m = m.astype(f32)
                ss += jnp.sum(m * m, axis=1, keepdims=True)
            tile = pack_column([ss[:8], ss[8:]])
            st_own[h] = tile
            st_in[h, mx] = tile
            for d in range(1, 4):
                rcopy(st_own.at[h], st_in.at[h, mx], send_sem.at[3], st_sem.at[h], {"mx": (mx + d) % 4}).start()

    def stat_gather(h):
        with jax.named_scope("m_stat_gather"):
            three = st_in.at[h, pl.ds(0, 3)]
            rcopy(three, three, send_sem.at[3], st_sem.at[h], core_dev).wait_recv()
            total = st_in[h, 0] + st_in[h, 1] + st_in[h, 2] + st_in[h, 3]
            st_sum[h] = total
            st_all[h, my] = total
            send_ag(st_sum, st_all, h, send_sem.at[11], sg_sem)

    def norm(h):
        with jax.named_scope("m_norm"):
            wait_ag(st_all, h, send_sem.at[11], sg_sem)
            for i in range(2):
                wait_ag(ag1, h, send_sem.at[2], ag1_sem, i)
            for z in range(4):
                scale = lax.rsqrt((st_all[h, 2 * z] + st_all[h, 2 * z + 1]) / hidden + NORM_EPS)
                col = jnp.concatenate([unpack_column(scale, 0), unpack_column(scale, 1)], axis=0)
                for y in range(2):
                    gain = gain_ref[pl.ds(y * half, half)].astype(f32).reshape(1, half)
                    h2[h, 16 * z:16 * z + 16, y * half:(y + 1) * half] = (ag1[h, 2 * z + y].astype(f32) * col * gain).astype(bf)

    def transpose(i, carry):
        with jax.named_scope("m_transpose"):
            rows = pl.ds(pl.multiple_of(i * TILE, TILE), TILE)
            for k in range(n_k):
                flipped = [lax.dot_general(eye[...], w[k, rows, :], (((1,), (1,)), ((), ())), preferred_element_type=f32).astype(bf) for w in (wg_v, wu_v)]
                for w, val in zip((wg_v, wu_v), flipped):
                    w[k, rows, :] = val
            return carry

    def stage_a(s):
        with jax.named_scope("m_stage_a"):
            h, j = s // n_j, s % n_j
            lhs = h2[h]
            for i, w in enumerate((wg_v, wu_v)):
                cols = []
                for n in range(CHUNK // TILE):
                    rows = pl.ds(pl.multiple_of(j * CHUNK + n * TILE, TILE), TILE)
                    acc = jnp.dot(lhs[:, :TILE], w[0, rows, :], preferred_element_type=f32)
                    for k in range(1, n_k):
                        acc += jnp.dot(lhs[:, TILE * k:TILE * (k + 1)], w[k, rows, :], preferred_element_type=f32)
                    cols.append(acc.astype(bf))
                val = jnp.concatenate(cols, axis=1)
                for m in range(4):
                    pp[s, m % 2, m // 2, :, i * CHUNK:(i + 1) * CHUNK] = val[16 * m:16 * m + 16]
            rcopy(pp.at[s, 1 - ci], dr.at[s], send_sem.at[4], d_sem.at[s], core_dev).start()

    def stage_b(s):
        with jax.named_scope("m_stage_b"):
            rcopy(pp.at[s, 1 - ci], dr.at[s], send_sem.at[4], d_sem.at[s], core_dev).wait_recv()
            xs[s] = (pp[s, ci, 1 - xi].astype(f32) + dr[s, 1 - xi].astype(f32)).astype(bf)
            rcopy(xs.at[s], xr.at[s], send_sem.at[5], x_sem.at[s], x_dev).start()
            own[s] = pp[s, ci, xi].astype(f32) + dr[s, xi].astype(f32)

    def stage_c(s):
        with jax.named_scope("m_stage_c"):
            rcopy(xs.at[s], xr.at[s], send_sem.at[5], x_sem.at[s], x_dev).wait_recv()
            g = own[s, :, :CHUNK] + xr[s, :, :CHUNK].astype(f32)
            u = own[s, :, CHUNK:] + xr[s, :, CHUNK:].astype(f32)
            act[s, mx] = (jax.nn.silu(g) * u).astype(bf)
            rcopy(act.at[s, mx], act.at[s, mx], send_sem.at[6], ax_sem.at[s], x_dev).start()
            rcopy(act.at[s, mx], act.at[s, mx], send_sem.at[7], ad_sem.at[s], core_dev).start()

            @pl.when(s >= steps - DIRECT)
            def _():
                rcopy(act.at[s, mx], act.at[s, mx], send_sem.at[8], af_sem.at[s], {"mx": 2 * (1 - xi) + (1 - ci)}).start()

    def stage_d(s):
        with jax.named_scope("m_stage_d"):
            rcopy(act.at[s, xpeer], act.at[s, xpeer], send_sem.at[6], ax_sem.at[s], x_dev).wait_recv()

            @pl.when(s < steps - DIRECT)
            def _():
                rcopy(act.at[s, xpeer], act.at[s, xpeer], send_sem.at[8], af_sem.at[s], core_dev).start()

    def stage_e(s):
        with jax.named_scope("m_stage_e"):
            h, j = s // n_j, s % n_j
            rcopy(act.at[s, 0], act.at[s, 0], send_sem.at[7], ad_sem.at[s], core_dev).wait_recv()
            rcopy(act.at[s, 0], act.at[s, 0], send_sem.at[8], af_sem.at[s], core_dev).wait_recv()
            lhs = act[s].reshape(ROWS, CHUNK)
            dacc[h] += jnp.dot(lhs, wd_v[pl.ds(pl.multiple_of(j * CHUNK, CHUNK), CHUNK), :], preferred_element_type=f32)

    def rs2_send(h):
        with jax.named_scope("m_rs2_send"):
            for z in range(4):
                for y in range(2):
                    p2[h, 2 * z + y] = dacc[h, 16 * z:16 * z + 16, y * half:(y + 1) * half].astype(bf)
            send_rs(p2, rs2, h, send_sem.at[9], rs2_sem)

    def rs2_finish(h):
        with jax.named_scope("m_rs2_finish"):
            for i, (lo, hi) in enumerate(parts):
                o = finish_rs(p2, rs2, h, i, send_sem.at[9], rs2_sem, mp[h, :, lo:hi].astype(f32))
                mo[h, :, lo:hi] = o
                ag2[h, my, :, lo:hi] = o
                send_ag(mo, ag2, h, send_sem.at[10], ag2_sem, i)

    n_t = n_j * (CHUNK // TILE)
    project(0)
    rs1_send(0)
    project(1)
    project(2)
    for ld in loads[:-1]:
        ld.wait()
    lax.fori_loop(0, n_t // 2, transpose, 0)
    rs1_send(1)
    rs1_finish(0)
    lax.fori_loop(n_t // 2, n_t // 2 + 3, transpose, 0)
    stat_gather(0)
    rs1_finish(1)
    rs1_send(2)
    lax.fori_loop(n_t // 2 + 3, n_t, transpose, 0)
    stat_gather(1)
    norm(0)

    def body(t, carry):
        @pl.when(t == n_j)
        def _():
            norm(1)

        @pl.when(t == 2 * n_j)
        def _():
            norm(2)

        @pl.when(t == n_j + 1)
        def _():
            rs1_finish(2)

        @pl.when(t == n_j + 4)
        def _():
            stat_gather(2)

        @pl.when(t < steps)
        def _():
            stage_a(t)

        @pl.when((t >= LAG_B) & (t < steps + LAG_B))
        def _():
            stage_b(t - LAG_B)

        @pl.when((t >= LAG_C) & (t < steps + LAG_C))
        def _():
            stage_c(t - LAG_C)

        @pl.when((t >= LAG_D) & (t < steps + LAG_D))
        def _():
            stage_d(t - LAG_D)

        @pl.when(t == LAG_E)
        def _():
            loads[-1].wait()

        @pl.when(t >= LAG_E)
        def _():
            s = t - LAG_E
            stage_e(s)

            @pl.when(s % n_j == n_j - 1)
            def _():
                rs2_send(s // n_j)

        lag2 = LAG_RS

        @pl.when((t >= LAG_E + n_j - 1 + lag2) & ((t - LAG_E - (n_j - 1) - lag2) % n_j == 0))
        def _():
            rs2_finish((t - LAG_E - (n_j - 1) - lag2) // n_j)

        return carry

    total_t = steps + LAG_E
    lax.fori_loop(0, total_t, body, 0)
    done = len([h for h in range(n_h) if LAG_E + n_j - 1 + LAG_RS + h * n_j < total_t])
    pl.delay(HOLD)
    for h in range(done, n_h):
        rs2_finish(h)
    for h in range(n_h):
        for i in range(2):
            wait_ag(ag2, h, send_sem.at[10], ag2_sem, i)
    for k, ref in ((0, attn_v.at[:, pl.ds(0, 48)]), (11, st_all.at[:, pl.ds(0, 7)]), (1, rs1), (2, rs1), (3, st_in.at[:, pl.ds(0, 3)]), (4, dr), (5, xs), (6, act.at[:, 0]), (7, act.at[:, 0]), (8, act.at[:, 0]), (9, rs2), (10, rs2)):
        rcopy(ref, ref, send_sem.at[k], at_sem.at[0], core_dev).wait_send()


def mlp_call(x_in, gain, attn, w_o, w_gate, w_up, w_down, hidden):
    rows, cols = x_in.shape
    ff = w_gate.shape[0]
    n_j = pl.cdiv(ff, CHUNK)
    n_h = rows // ROWS
    steps = n_h * n_j
    half = cols // 2
    bf, f32 = jnp.bfloat16, jnp.float32
    hbm, vmem = pl.BlockSpec(memory_space=pltpu.HBM), pl.BlockSpec(memory_space=pltpu.VMEM)
    dma = pltpu.SemaphoreType.DMA
    return pl.pallas_call(
        functools.partial(mlp_kernel, hidden),
        name="mlp",
        out_shape=jax.ShapeDtypeStruct((n_h, 8, 16, half), bf),
        in_specs=[vmem, vmem, vmem, vmem, hbm, hbm, hbm],
        out_specs=vmem,
        scratch_shapes=[
            pltpu.VMEM((cols // TILE, n_j * CHUNK, TILE), bf), pltpu.VMEM((cols // TILE, n_j * CHUNK, TILE), bf),
            pltpu.VMEM((n_j * CHUNK, cols), bf), pltpu.VMEM((n_h, 64, attn.shape[1]), bf),
            pltpu.VMEM((n_h, 8, 16, half), bf), pltpu.VMEM((n_h, 7, 16, half), bf), pltpu.VMEM((n_h, 16, half), bf), pltpu.VMEM((n_h, 8, 16, half), bf),
            pltpu.VMEM((n_h, 8, 128), f32), pltpu.VMEM((n_h, 4, 8, 128), f32), pltpu.VMEM((n_h, 8, 128), f32), pltpu.VMEM((n_h, 8, 8, 128), f32), pltpu.VMEM((n_h, ROWS, cols), bf),
            pltpu.VMEM((steps, 2, 2, 16, 2 * CHUNK), bf), pltpu.VMEM((steps, 2, 16, 2 * CHUNK), bf), pltpu.VMEM((steps, 16, 2 * CHUNK), f32),
            pltpu.VMEM((steps, 16, 2 * CHUNK), bf), pltpu.VMEM((steps, 16, 2 * CHUNK), bf), pltpu.VMEM((steps, 4, 16, CHUNK), bf),
            pltpu.VMEM((n_h, ROWS, cols), f32),
            pltpu.VMEM((n_h, 8, 16, half), bf), pltpu.VMEM((n_h, 7, 16, half), bf), pltpu.VMEM((n_h, 16, half), bf), pltpu.VMEM((TILE, TILE), bf),
            dma((1 + 2 * (cols // TILE),)), dma((12,)), dma((n_h,)), dma((n_h, 2)), dma((n_h, 2)), dma((n_h,)), dma((n_h,)), dma((n_h, 2)), dma((n_h, 2)),
            dma((steps,)), dma((steps,)), dma((steps,)), dma((steps,)), dma((steps,)),
        ],
        compiler_params=pltpu.CompilerParams(collective_id=1, has_side_effects=True, vmem_limit_bytes=MLP_LIMIT),
    )(x_in, gain, attn, w_o, pinned(w_gate), pinned(w_up), pinned(w_down))


def place_kernel(pieces_ref, out_ref):
    n_h, _, _, half = pieces_ref.shape
    for h in range(n_h):
        for z in range(4):
            for y in range(2):
                r0 = z * 16 * n_h + h * 16
                out_ref[r0:r0 + 16, y * half:(y + 1) * half] = pieces_ref[h, 2 * z + y]


def place_call(pieces, shape):
    vmem = pl.BlockSpec(memory_space=pltpu.VMEM)
    return pl.pallas_call(place_kernel, name="place", out_shape=jax.ShapeDtypeStruct(shape, pieces.dtype), in_specs=[vmem], out_specs=vmem, compiler_params=pltpu.CompilerParams(vmem_limit_bytes=4 * 1024 * 1024))(pieces)


GROUP_ROWS = 16


def attn_kernel(seq_ref, proj_ref, bq_ref, bk_ref, bv_ref, freq_ref, k_ref, v_ref, attn_ref, ko_hbm, vo_hbm, qs, kn, vn, os, pos, patch, out_sem, patch_sem):
    f32, bf = jnp.float32, jnp.bfloat16
    rows, seq = k_ref.shape[0], k_ref.shape[1]
    heads = attn_ref.shape[1] // HEAD
    groups = rows // GROUP_ROWS
    outs = [ko_hbm, vo_hbm]

    def bulk(g):
        part = pl.ds(g * GROUP_ROWS, GROUP_ROWS)
        return [pltpu.make_async_copy(src.at[part], dst.at[part], out_sem.at[i, g]) for i, (src, dst) in enumerate(zip((k_ref, v_ref), outs))]

    for g in range(groups):
        for cp in bulk(g):
            cp.start()
    for b in range(rows):
        pos[b:b + 1, :] = jnp.full((1, HEAD), seq_ref[b], jnp.int32).astype(f32)
    angles = pos[...] * freq_ref[...]
    lower = lax.broadcasted_iota(jnp.int32, (rows, HEAD), 1) < HEAD // 2
    cos_tab = jnp.cos(angles)
    sin_tab = jnp.sin(angles)
    sin_tab = jnp.where(lower, -sin_tab, sin_tab)

    def column(c, bias_ref, k):
        bias = bias_ref[pl.ds(k * HEAD, HEAD)].astype(f32).reshape(1, HEAD)
        return proj_ref[:, c * HEAD:(c + 1) * HEAD] + bias

    def rotate(v):
        return (v * cos_tab + pltpu.roll(v, HEAD // 2, 1) * sin_tab).astype(bf).astype(f32)

    with jax.named_scope('a_pre'):
        qs[...] = jnp.zeros_like(qs)
    for h in range(heads):
        qs[:, h, :] = rotate(column(h, bq_ref, h))
    kn[...] = rotate(column(heads, bk_ref, 0))
    vn[...] = column(heads + 1, bv_ref, 0).astype(bf).astype(f32)

    def slab_of(b):
        p = seq_ref[b]
        return p, pl.multiple_of((p // 16) * 16, 16)

    def body(g, carry):
        times = lax.broadcasted_iota(jnp.int32, (8, seq), 1)
        slots = lax.broadcasted_iota(jnp.int32, (16, HEAD), 0)
        scores, news, hits = [], [], []
        for r in range(GROUP_ROWS):
            b = g * GROUP_ROWS + r
            p, slab = slab_of(b)
            hit = slots == p - slab
            for i, (cache, new) in enumerate(((k_ref, kn), (v_ref, vn))):
                old = cache[b, pl.ds(slab, 16), :].astype(f32)
                patch[i, b] = jnp.where(hit, new[pl.ds(b, 1), :], old).astype(bf)
            q = qs[b]
            s = lax.dot_general(q.astype(bf), k_ref[b], (((1,), (1,)), ((), ())), preferred_element_type=f32) * HEAD ** -0.5
            s_new = jnp.sum(q * kn[pl.ds(b, 1), :], axis=1, keepdims=True) * HEAD ** -0.5
            hits.append(times == p)
            news.append(s_new)
            scores.append(jnp.where(hits[r], s_new, jnp.where(times < p, s, -jnp.inf)))
        s = jnp.concatenate(scores, axis=0)
        top = jnp.max(s, axis=1, keepdims=True)
        w = jnp.exp(s - top)
        total = jnp.sum(w, axis=1, keepdims=True)
        w_new = jnp.exp(jnp.concatenate(news, axis=0) - top).astype(bf).astype(f32)
        w = jnp.where(jnp.concatenate(hits, axis=0), 0.0, w).astype(bf)
        for r in range(GROUP_ROWS):
            b = g * GROUP_ROWS + r
            part = slice(8 * r, 8 * r + 8)
            o = jnp.dot(w[part], v_ref[b], preferred_element_type=f32) + w_new[part] * vn[pl.ds(b, 1), :]
            os[b] = o / total[part]
        return carry

    with jax.named_scope('a_main'):
        lax.fori_loop(0, groups, body, 0)
    for h in range(heads):
        attn_ref[:, h * HEAD:(h + 1) * HEAD] = os[:, h, :].astype(bf)

    def patches(b):
        slab = slab_of(b)[1]
        return [pltpu.make_async_copy(patch.at[i, b], dst.at[b, pl.ds(slab, 16)], patch_sem.at[i]) for i, dst in enumerate(outs)]

    for g in range(groups):
        with jax.named_scope('a_bulk'):
            for cp in bulk(g):
                cp.wait()
        for b in range(g * GROUP_ROWS, (g + 1) * GROUP_ROWS):
            for cp in patches(b):
                cp.start()
    with jax.named_scope('a_patch'):
        for b in range(rows):
            for cp in patches(b):
                cp.wait()


def attn_call(seq_lens, projected, b_q, b_k, b_v, k_cache, v_cache):
    rows, seq = k_cache.shape[0], k_cache.shape[1]
    f32, bf = jnp.float32, jnp.bfloat16
    freq = (ROPE_THETA ** (-2.0 * np.arange(HEAD // 2) / HEAD)).astype(np.float32)
    freq = jnp.asarray(np.concatenate([freq, freq])[None])
    any_spec, vmem, smem = pl.BlockSpec(memory_space=pl.ANY), pl.BlockSpec(memory_space=pltpu.VMEM), pl.BlockSpec(memory_space=pltpu.SMEM)
    dma = pltpu.SemaphoreType.DMA
    cache = jax.ShapeDtypeStruct((rows, seq, HEAD), bf)
    return pl.pallas_call(
        attn_kernel,
        name="attn",
        out_shape=(jax.ShapeDtypeStruct((rows, b_q.shape[0]), bf), cache, cache),
        in_specs=[smem, vmem, vmem, vmem, vmem, vmem, vmem, vmem],
        out_specs=(vmem, any_spec, any_spec),
        scratch_shapes=[
            pltpu.VMEM((rows, 8, HEAD), f32), pltpu.VMEM((rows, HEAD), f32),
            pltpu.VMEM((rows, HEAD), f32), pltpu.VMEM((rows, 8, HEAD), f32), pltpu.VMEM((rows, HEAD), f32), pltpu.VMEM((2, rows, 16, HEAD), bf),
            dma((2, rows // GROUP_ROWS)), dma((2,)),
        ],
        compiler_params=pltpu.CompilerParams(vmem_limit_bytes=ATTN_LIMIT),
    )(seq_lens, projected, b_q, b_k, b_v, freq, k_cache.reshape(rows, seq, HEAD), v_cache.reshape(rows, seq, HEAD))


def solution(mesh):
    mx_size = mesh.shape["mx"]
    act_spec = P(None, "mx")
    cache_spec = P("mx", None, "my", None)
    in_specs = (act_spec, P("mx"), P("mx"), P("mx"), P("mx", "my"), P("my"), P("mx", "my"), P("my"), P("mx", "my"), P("my"), P("my", "mx"), P("mx", "my"), P("mx", "my"), P("my", "mx"), cache_spec, cache_spec)
    out_specs = (act_spec, cache_spec, cache_spec)

    def local_layer(x_in, seq_lens, gain_attn, gain_mlp, w_q, b_q, w_k, b_k, w_v, b_v, w_o, w_gate, w_up, w_down, k_cache, v_cache):
        hidden = x_in.shape[1] * mx_size
        projected = qkv_call(x_in, gain_attn, w_q, w_k, w_v, hidden)
        attn_rows, k_out, v_out = attn_call(seq_lens, projected, b_q, b_k, b_v, k_cache, v_cache)
        pieces = mlp_call(x_in, gain_mlp, attn_rows, w_o, w_gate.T, w_up.T, w_down, hidden)
        x_out = place_call(pieces, x_in.shape)
        k_cache_out, v_cache_out = k_out.reshape(k_cache.shape), v_out.reshape(v_cache.shape)
        return x_out, k_cache_out, v_cache_out

    return jax.shard_map(local_layer, mesh=mesh, in_specs=in_specs, out_specs=out_specs, check_vma=False)
```

```python
import functools
import types

import jax
import jax.numpy as jnp
import numpy as np
from jax import lax
from jax.experimental import pallas as pl
from jax.experimental.pallas import tpu as pltpu
from jax.sharding import PartitionSpec as P

HEAD = 128
NORM_EPS = 1e-6
ROPE_THETA = 1000000.0
MESH = pl.DeviceIdType.MESH
CHUNK = 512
TILE = 256
DIRECT = 2
ROWS = 64
LAG_B, LAG_C, LAG_D, LAG_E, LAG_M, LAG_F = 1, 4, 7, 8, 4, 9
VMEM_LIMIT = 67043328
MLP_LIMIT = 48 * 1024 * 1024
ATTN_LIMIT = 14 * 1024 * 1024
QKV_LIMIT = 8 * 1024 * 1024


def rcopy(src, dst, send_sem, recv_sem, dev):
    return pltpu.make_async_remote_copy(src_ref=src, dst_ref=dst, send_sem=send_sem, recv_sem=recv_sem, device_id=dev, device_id_type=MESH)


def pinned(x):
    return pltpu.with_memory_space_constraint(x, pltpu.HBM)


def lane_ids():
    return lax.broadcasted_iota(jnp.int32, (8, 128), 1)


def pack_column(blocks):
    tile = jnp.zeros((8, 128), jnp.float32)
    lanes = lane_ids()
    for k, block in enumerate(blocks):
        tile = jnp.where(lanes == k, block, tile)
    return tile


def unpack_column(tile, k):
    return jnp.sum(jnp.where(lane_ids() == k, tile, 0.0), axis=1, keepdims=True)


def qkv_kernel(hidden, x_hbm, gain_hbm, wq_hbm, wk_hbm, wv_hbm, out_ref, gain_ref, x_v, wq_v, wk_v, wv_v, st_own, st_in, nrm, pp, dr, own, xs, xr, ld_sem, send_sem, st_sem, d_sem, x_sem):
    mx = lax.axis_index("mx")
    xi, ci = mx // 2, mx % 2
    partner, xpeer = 2 * xi + (1 - ci), 2 * (1 - xi) + ci
    loads = [pltpu.make_async_copy(s, d, ld_sem.at[i]) for i, (s, d) in enumerate([(x_hbm, x_v), (gain_hbm, gain_ref), (wq_hbm, wq_v), (wk_hbm, wk_v), (wv_hbm, wv_v)])]
    for ld in loads:
        ld.start()
    barrier = pltpu.get_barrier_semaphore()
    for d in range(1, 4):
        pl.semaphore_signal(barrier, inc=1, device_id={"mx": (mx + d) % 4}, device_id_type=MESH)
    with jax.named_scope('q_barrier'):
        pl.semaphore_wait(barrier, 3)

    rows = x_v.shape[0]
    with jax.named_scope('q_xload'):
        loads[0].wait()
    blocks = []
    for k in range(rows // 8):
        v = x_v[8 * k:8 * k + 8, :].astype(jnp.float32)
        blocks.append(jnp.sum(v * v, axis=1, keepdims=True))
    tile = pack_column(blocks)
    st_own[...] = tile
    st_in[mx] = tile
    for d in range(1, 4):
        rcopy(st_own, st_in.at[mx], send_sem.at[0], st_sem, {"mx": (mx + d) % 4}).start()
    with jax.named_scope('q_wload'):
        for ld in loads[1:]:
            ld.wait()
    with jax.named_scope('q_stat'):
        rcopy(st_in.at[pl.ds(0, 3)], st_in.at[pl.ds(0, 3)], send_sem.at[0], st_sem, {"mx": partner}).wait()
    total = st_in[0] + st_in[1] + st_in[2] + st_in[3]
    scale = lax.rsqrt(total / hidden + NORM_EPS)
    gain = gain_ref[...].astype(jnp.float32).reshape(1, x_v.shape[1])
    for k in range(0, rows // 8, 2):
        col = jnp.concatenate([unpack_column(scale, k), unpack_column(scale, k + 1)], axis=0)
        nrm[8 * k:8 * k + 16, :] = (x_v[8 * k:8 * k + 16, :].astype(jnp.float32) * col * gain).astype(jnp.bfloat16)

    lhs = nrm[...]
    part = rows // 4
    width = out_ref.shape[1]
    offs = [0, wq_v.shape[1], wq_v.shape[1] + wk_v.shape[1]]
    pieces = [(w, c0, min(c0 + TILE, w.shape[1]), off) for w, off in zip((wq_v, wk_v, wv_v), offs) for c0 in range(0, w.shape[1], TILE)]
    cut = 2 * TILE
    parts = ((0, cut), (cut, width))

    def swap(i):
        cols = pl.ds(parts[i][0], parts[i][1] - parts[i][0])
        return rcopy(pp.at[1 - ci, :, :, cols], dr.at[:, :, cols], send_sem.at[1], d_sem.at[i], {"mx": partner})

    def cross(i):
        cols = pl.ds(parts[i][0], parts[i][1] - parts[i][0])
        return rcopy(xs.at[:, cols], xr.at[:, cols], send_sem.at[2], x_sem.at[i], {"mx": xpeer})

    for i, (lo, hi) in enumerate(parts):
        for w, c0, c1, off in pieces:
            if lo <= off + c0 < hi:
                r = jnp.dot(lhs, w[:, c0:c1], preferred_element_type=jnp.float32).astype(jnp.bfloat16)
                for m in range(4):
                    pp[m % 2, m // 2, :, off + c0:off + c1] = r[m * part:(m + 1) * part]
        swap(i).start()
    for i, (lo, hi) in enumerate(parts):
        with jax.named_scope('q_d2d'):
            swap(i).wait_recv()
        xs[:, lo:hi] = (pp[ci, 1 - xi, :, lo:hi].astype(jnp.float32) + dr[1 - xi, :, lo:hi].astype(jnp.float32)).astype(jnp.bfloat16)
        cross(i).start()
        own[:, lo:hi] = pp[ci, xi, :, lo:hi].astype(jnp.float32) + dr[xi, :, lo:hi].astype(jnp.float32)
    for i, (lo, hi) in enumerate(parts):
        with jax.named_scope('q_x'):
            cross(i).wait_recv()
        out_ref[:, lo:hi] = own[:, lo:hi] + xr[:, lo:hi].astype(jnp.float32)
    for i in range(2):
        swap(i).wait_send()
        cross(i).wait_send()


def qkv_call(x_in, gain, w_q, w_k, w_v, hidden):
    rows, cols = x_in.shape
    width = w_q.shape[1] + w_k.shape[1] + w_v.shape[1]
    bf, f32 = jnp.bfloat16, jnp.float32
    any_spec, vmem = pl.BlockSpec(memory_space=pl.ANY), pl.BlockSpec(memory_space=pltpu.VMEM)
    part = rows // 4
    return pl.pallas_call(
        functools.partial(qkv_kernel, hidden),
        name="qkv",
        out_shape=jax.ShapeDtypeStruct((part, width), f32),
        in_specs=[any_spec] * 5,
        out_specs=vmem,
        scratch_shapes=[
            pltpu.VMEM(gain.shape, bf),
            pltpu.VMEM((rows, cols), bf), pltpu.VMEM(w_q.shape, bf), pltpu.VMEM(w_k.shape, bf), pltpu.VMEM(w_v.shape, bf),
            pltpu.VMEM((8, 128), f32), pltpu.VMEM((4, 8, 128), f32), pltpu.VMEM((rows, cols), bf),
            pltpu.VMEM((2, 2, part, width), bf), pltpu.VMEM((2, part, width), bf), pltpu.VMEM((part, width), f32),
            pltpu.VMEM((part, width), bf), pltpu.VMEM((part, width), bf),
            pltpu.SemaphoreType.DMA((5,)), pltpu.SemaphoreType.DMA((3,)), pltpu.SemaphoreType.DMA, pltpu.SemaphoreType.DMA((2,)), pltpu.SemaphoreType.DMA((2,)),
        ],
        compiler_params=pltpu.CompilerParams(collective_id=0, has_side_effects=True, vmem_limit_bytes=QKV_LIMIT),
        cost_estimate=pl.CostEstimate(flops=10 ** 10, bytes_accessed=3 * 10 ** 6, transcendentals=0),
    )(pinned(x_in), pinned(gain), pinned(w_q), pinned(w_k), pinned(w_v))


def mlp_kernel(hidden, x_v, gain_ref, attn_ref, wo_v, wg_hbm, wu_hbm, wd_hbm, ag2,
               wg_v, wu_v, wd_v, attn_v, p1, yb1, zs1, zb1, mp, ag1, st_own, st_in, st_sum, st_all, h2,
               pp, dr, own, xs, xr, act, dacc, p2, yb2, zs2, zb2, mo, eye,
               ld_sem, send_sem, at_sem, st_sem, sg_sem, ysem1, zsem1, agz1, agy1, ysem2, zsem2, agz2, agy2, d_sem, x_sem, ax_sem, ad_sem, af_sem):
    my, mx = lax.axis_index("my"), lax.axis_index("mx")
    n_my = 8
    xi, ci = mx // 2, mx % 2
    zi, yi = my // 2, my % 2
    partner, xpeer = 2 * xi + (1 - ci), 2 * (1 - xi) + ci
    core_dev, x_dev = {"mx": partner}, {"mx": xpeer}
    n_h = h2.shape[0]
    ff = wg_hbm.shape[0]
    n_j = pl.cdiv(ff, CHUNK)
    steps = n_h * n_j
    half = x_v.shape[1] // 2
    brows = attn_ref.shape[0]
    f32, bf = jnp.float32, jnp.bfloat16

    n_k = wg_v.shape[0]
    tiles = [(src.at[:, pl.ds(TILE * k, TILE)], dst.at[k, pl.ds(0, ff)]) for src, dst in ((wg_hbm, wg_v), (wu_hbm, wu_v)) for k in range(n_k)]
    loads = [pltpu.make_async_copy(s, d, ld_sem.at[i]) for i, (s, d) in enumerate(tiles + [(wd_hbm, wd_v.at[pl.ds(0, ff)])])]
    for ld in loads:
        ld.start()
    barrier = pltpu.get_barrier_semaphore()
    for d in range(1, 4):
        pl.semaphore_signal(barrier, inc=1, device_id={"mx": (mx + d) % 4}, device_id_type=MESH)
    for d in range(1, n_my):
        pl.semaphore_signal(barrier, inc=1, device_id={"my": (my + d) % n_my}, device_id_type=MESH)
    with jax.named_scope('m_barrier'):
        pl.semaphore_wait(barrier, 3 + n_my - 1)

    mine = pl.ds(pl.multiple_of(mx * 16, 16), 16)
    for h in range(n_h):
        for d in range(1, 4):
            rcopy(attn_ref.at[pl.ds(16 * h, 16)], attn_v.at[h, mine], send_sem.at[0], at_sem.at[h], {"mx": (mx + d) % 4}).start()
    for h in range(n_h):
        attn_v[h, mine, :] = attn_ref[16 * h:16 * h + 16, :]
    dacc[...] = jnp.zeros_like(dacc)
    wd_v[ff:, :] = jnp.zeros((wd_v.shape[0] - ff, wd_v.shape[1]), bf)
    for w in (wg_v, wu_v):
        for k in range(n_k):
            w[k, ff:, :] = jnp.zeros((w.shape[1] - ff, TILE), bf)
    eye[...] = (lax.broadcasted_iota(jnp.int32, (TILE, TILE), 0) == lax.broadcasted_iota(jnp.int32, (TILE, TILE), 1)).astype(f32).astype(bf)

    zs = (3 - zi, (zi + 2) % 4, zi + 1 - 2 * (zi % 2), zi)
    peers = [2 * z + y for z in zs for y in (1 - yi, yi)][:-1]
    y_peer = 2 * zi + 1 - yi
    y_dev = {"my": y_peer}
    z_devs = [{"my": 2 * z + yi} for z in zs[:3]]

    def project(h):
        with jax.named_scope("m_project"):
            gathered = attn_v.at[h, pl.ds(0, 48)]
            rcopy(gathered, gathered, send_sem.at[0], at_sem.at[h], core_dev).wait_recv()
            for y in range(2):
                r = jnp.dot(attn_v[h], wo_v[:, y * half:(y + 1) * half], preferred_element_type=f32).astype(bf)
                for z in range(4):
                    p1[h, 2 * z + y] = r[16 * z:16 * z + 16]

    def rs_start(r, h):
        with jax.named_scope("m_rs_start"):
            for k, z in enumerate(zs):
                rcopy(r.part.at[h, 2 * z + 1 - yi], r.ybuf.at[h, k], send_sem.at[r.sem], r.ysem.at[h, k], y_dev).start()

    def wait_y(r, h, k):
        rcopy(r.ybuf.at[h, k], r.ybuf.at[h, k], send_sem.at[r.sem], r.ysem.at[h, k], y_dev).wait_recv()

    def rs_mid(r, h):
        with jax.named_scope("m_rs_mid"):
            for k in range(3):
                wait_y(r, h, k)
                r.zsend[h, k] = (r.part[h, 2 * zs[k] + yi].astype(f32) + r.ybuf[h, k].astype(f32)).astype(bf)
                rcopy(r.zsend.at[h, k], r.zbuf.at[h, k], send_sem.at[r.sem + 1], r.zsem.at[h], z_devs[k]).start()

    def rs_fin(r, h, base):
        wait_y(r, h, 3)
        rcopy(r.zbuf.at[h], r.zbuf.at[h], send_sem.at[r.sem + 1], r.zsem.at[h], y_dev).wait_recv()
        total = r.part[h, my].astype(f32) + r.ybuf[h, 3].astype(f32)
        for k in range(3):
            total += r.zbuf[h, k].astype(f32)
        return (base + total).astype(bf)

    def ag_start(r, h, val):
        r.piece[h] = val
        r.all[h, my] = val
        for k in range(3):
            rcopy(r.piece.at[h], r.all.at[h, my], send_sem.at[r.sem + 2], r.agz.at[h, k], z_devs[k]).start()
        rcopy(r.piece.at[h], r.all.at[h, my], send_sem.at[r.sem + 2], r.agy.at[h], y_dev).start()

    def ag_mid(r, h):
        with jax.named_scope("m_ag_mid"):
            for k in (2, 1, 0):
                got = r.all.at[h, 2 * zs[k] + yi]
                rcopy(got, got, send_sem.at[r.sem + 2], r.agz.at[h, k], y_dev).wait_recv()
                rcopy(got, got, send_sem.at[r.sem + 2], r.agy.at[h], y_dev).start()

    def ag_fin(r, h):
        with jax.named_scope("m_ag_fin"):
            four = r.all.at[h, pl.ds(0, 4)]
            rcopy(four, four, send_sem.at[r.sem + 2], r.agy.at[h], y_dev).wait_recv()

    one = types.SimpleNamespace(part=p1, ybuf=yb1, zsend=zs1, zbuf=zb1, piece=mp, all=ag1, ysem=ysem1, zsem=zsem1, agz=agz1, agy=agy1, sem=9)
    two = types.SimpleNamespace(part=p2, ybuf=yb2, zsend=zs2, zbuf=zb2, piece=mo, all=ag2, ysem=ysem2, zsem=zsem2, agz=agz2, agy=agy2, sem=12)

    def rs1_finish(h):
        with jax.named_scope("m_rs1_finish"):
            r0 = pl.multiple_of(zi * brows + h * 16, 16)
            base = x_v[pl.ds(r0, 16), pl.ds(pl.multiple_of(yi * half, 128), half)].astype(f32)
            m = rs_fin(one, h, base)
            ag_start(one, h, m)
            m = m.astype(f32)
            ss = jnp.sum(m * m, axis=1, keepdims=True)
            tile = pack_column([ss[:8], ss[8:]])
            st_own[h] = tile
            st_in[h, mx] = tile
            for d in range(1, 4):
                rcopy(st_own.at[h], st_in.at[h, mx], send_sem.at[3], st_sem.at[h], {"mx": (mx + d) % 4}).start()

    def stat_gather(h):
        with jax.named_scope("m_stat_gather"):
            three = st_in.at[h, pl.ds(0, 3)]
            rcopy(three, three, send_sem.at[3], st_sem.at[h], core_dev).wait_recv()
            total = st_in[h, 0] + st_in[h, 1] + st_in[h, 2] + st_in[h, 3]
            st_sum[h] = total
            st_all[h, my] = total
            for peer in peers:
                rcopy(st_sum.at[h], st_all.at[h, my], send_sem.at[1], sg_sem.at[h], {"my": peer}).start()

    def norm(h):
        with jax.named_scope("m_norm"):
            seven = st_all.at[h, pl.ds(0, n_my - 1)]
            rcopy(seven, seven, send_sem.at[1], sg_sem.at[h], y_dev).wait_recv()
            ag_fin(one, h)
            for z in range(4):
                scale = lax.rsqrt((st_all[h, 2 * z] + st_all[h, 2 * z + 1]) / hidden + NORM_EPS)
                col = jnp.concatenate([unpack_column(scale, 0), unpack_column(scale, 1)], axis=0)
                for y in range(2):
                    gain = gain_ref[pl.ds(y * half, half)].astype(f32).reshape(1, half)
                    h2[h, 16 * z:16 * z + 16, y * half:(y + 1) * half] = (ag1[h, 2 * z + y].astype(f32) * col * gain).astype(bf)

    def transpose(i, carry):
        with jax.named_scope("m_transpose"):
            rows = pl.ds(pl.multiple_of(i * TILE, TILE), TILE)
            for k in range(n_k):
                flipped = [lax.dot_general(eye[...], w[k, rows, :], (((1,), (1,)), ((), ())), preferred_element_type=f32).astype(bf) for w in (wg_v, wu_v)]
                for w, val in zip((wg_v, wu_v), flipped):
                    w[k, rows, :] = val
            return carry

    def stage_a(s):
        with jax.named_scope("m_stage_a"):
            h, j = s // n_j, s % n_j
            lhs = h2[h]
            for i, w in enumerate((wg_v, wu_v)):
                cols = []
                for n in range(CHUNK // TILE):
                    rows = pl.ds(pl.multiple_of(j * CHUNK + n * TILE, TILE), TILE)
                    acc = jnp.dot(lhs[:, :TILE], w[0, rows, :], preferred_element_type=f32)
                    for k in range(1, n_k):
                        acc += jnp.dot(lhs[:, TILE * k:TILE * (k + 1)], w[k, rows, :], preferred_element_type=f32)
                    cols.append(acc.astype(bf))
                val = jnp.concatenate(cols, axis=1)
                for m in range(4):
                    pp[s, m % 2, m // 2, :, i * CHUNK:(i + 1) * CHUNK] = val[16 * m:16 * m + 16]
            rcopy(pp.at[s, 1 - ci], dr.at[s], send_sem.at[4], d_sem.at[s], core_dev).start()

    def stage_b(s):
        with jax.named_scope("m_stage_b"):
            rcopy(pp.at[s, 1 - ci], dr.at[s], send_sem.at[4], d_sem.at[s], core_dev).wait_recv()
            xs[s] = (pp[s, ci, 1 - xi].astype(f32) + dr[s, 1 - xi].astype(f32)).astype(bf)
            rcopy(xs.at[s], xr.at[s], send_sem.at[5], x_sem.at[s], x_dev).start()
            own[s] = pp[s, ci, xi].astype(f32) + dr[s, xi].astype(f32)

    def stage_c(s):
        with jax.named_scope("m_stage_c"):
            rcopy(xs.at[s], xr.at[s], send_sem.at[5], x_sem.at[s], x_dev).wait_recv()
            g = own[s, :, :CHUNK] + xr[s, :, :CHUNK].astype(f32)
            u = own[s, :, CHUNK:] + xr[s, :, CHUNK:].astype(f32)
            act[s, mx] = (jax.nn.silu(g) * u).astype(bf)
            rcopy(act.at[s, mx], act.at[s, mx], send_sem.at[6], ax_sem.at[s], x_dev).start()
            rcopy(act.at[s, mx], act.at[s, mx], send_sem.at[7], ad_sem.at[s], core_dev).start()

            @pl.when(s >= steps - DIRECT)
            def _():
                rcopy(act.at[s, mx], act.at[s, mx], send_sem.at[8], af_sem.at[s], {"mx": 2 * (1 - xi) + (1 - ci)}).start()

    def stage_d(s):
        with jax.named_scope("m_stage_d"):
            rcopy(act.at[s, xpeer], act.at[s, xpeer], send_sem.at[6], ax_sem.at[s], x_dev).wait_recv()

            @pl.when(s < steps - DIRECT)
            def _():
                rcopy(act.at[s, xpeer], act.at[s, xpeer], send_sem.at[8], af_sem.at[s], core_dev).start()

    def stage_e(s):
        with jax.named_scope("m_stage_e"):
            h, j = s // n_j, s % n_j
            rcopy(act.at[s, 0], act.at[s, 0], send_sem.at[7], ad_sem.at[s], core_dev).wait_recv()
            rcopy(act.at[s, 0], act.at[s, 0], send_sem.at[8], af_sem.at[s], core_dev).wait_recv()
            lhs = act[s].reshape(ROWS, CHUNK)
            dacc[h] += jnp.dot(lhs, wd_v[pl.ds(pl.multiple_of(j * CHUNK, CHUNK), CHUNK), :], preferred_element_type=f32)

    def rs2_send(h):
        with jax.named_scope("m_rs2_send"):
            for z in range(4):
                for y in range(2):
                    p2[h, 2 * z + y] = dacc[h, 16 * z:16 * z + 16, y * half:(y + 1) * half].astype(bf)
            rs_start(two, h)

    def rs2_finish(h):
        with jax.named_scope("m_rs2_finish"):
            ag_start(two, h, rs_fin(two, h, mp[h].astype(f32)))

    n_t = n_j * (CHUNK // TILE)
    def flip(lo, hi):
        lax.fori_loop(lo, hi, transpose, 0)

    project(0)
    rs_start(one, 0)
    project(1)
    rs_start(one, 1)
    project(2)
    for ld in loads[:-1]:
        ld.wait()
    flip(0, 2)
    rs_mid(one, 0)
    flip(2, 5)
    rs_mid(one, 1)
    flip(5, 7)
    rs1_finish(0)
    rs_start(one, 2)
    flip(7, 10)
    rs1_finish(1)
    stat_gather(0)
    flip(10, 12)
    rs_mid(one, 2)
    ag_mid(one, 0)
    flip(12, n_t)
    stat_gather(1)
    norm(0)

    def body(t, carry):
        @pl.when(t == n_j)
        def _():
            norm(1)

        @pl.when(t == 2 * n_j)
        def _():
            norm(2)

        @pl.when(t == 1)
        def _():
            ag_mid(one, 1)

        @pl.when(t == 2)
        def _():
            rs1_finish(2)

        @pl.when(t == 5)
        def _():
            stat_gather(2)

        @pl.when(t == n_j + 1)
        def _():
            ag_mid(one, 2)

        @pl.when(t < steps)
        def _():
            stage_a(t)

        @pl.when((t >= LAG_B) & (t < steps + LAG_B))
        def _():
            stage_b(t - LAG_B)

        @pl.when((t >= LAG_C) & (t < steps + LAG_C))
        def _():
            stage_c(t - LAG_C)

        @pl.when((t >= LAG_D) & (t < steps + LAG_D))
        def _():
            stage_d(t - LAG_D)

        @pl.when(t == LAG_E)
        def _():
            loads[-1].wait()

        @pl.when(t >= LAG_E)
        def _():
            s = t - LAG_E
            stage_e(s)

            @pl.when(s % n_j == n_j - 1)
            def _():
                rs2_send(s // n_j)

        after = t - LAG_E - (n_j - 1)

        @pl.when((after >= LAG_M) & ((after - LAG_M) % n_j == 0))
        def _():
            rs_mid(two, (after - LAG_M) // n_j)

        @pl.when((after >= LAG_F) & ((after - LAG_F) % n_j == 0))
        def _():
            rs2_finish((after - LAG_F) // n_j)

        return carry

    total_t = steps + LAG_E
    lax.fori_loop(0, total_t, body, 0)
    rs2_finish(1)
    ag_mid(two, 0)
    rs_mid(two, 2)
    ag_mid(two, 1)
    rs2_finish(2)
    ag_mid(two, 2)
    for h in range(n_h):
        ag_fin(two, h)
    seven = pl.ds(0, n_my - 1)
    for k, ref in ((0, attn_v.at[:, pl.ds(0, 48)]), (1, st_all.at[:, seven]), (3, st_in.at[:, pl.ds(0, 3)]), (4, dr), (5, xs), (6, act.at[:, 0]), (7, act.at[:, 0]), (8, act.at[:, 0]),
                   (9, yb1), (10, zb1), (11, ag1.at[:, seven]), (12, yb2), (13, zb2), (14, ag2.at[:, seven])):
        rcopy(ref, ref, send_sem.at[k], at_sem.at[0], core_dev).wait_send()


def mlp_call(x_in, gain, attn, w_o, w_gate, w_up, w_down, hidden):
    rows, cols = x_in.shape
    ff = w_gate.shape[0]
    n_j = pl.cdiv(ff, CHUNK)
    n_h = rows // ROWS
    steps = n_h * n_j
    half = cols // 2
    bf, f32 = jnp.bfloat16, jnp.float32
    hbm, vmem = pl.BlockSpec(memory_space=pltpu.HBM), pl.BlockSpec(memory_space=pltpu.VMEM)
    dma = pltpu.SemaphoreType.DMA
    return pl.pallas_call(
        functools.partial(mlp_kernel, hidden),
        name="mlp",
        out_shape=jax.ShapeDtypeStruct((n_h, 8, 16, half), bf),
        in_specs=[vmem, vmem, vmem, vmem, hbm, hbm, hbm],
        out_specs=vmem,
        scratch_shapes=[
            pltpu.VMEM((cols // TILE, n_j * CHUNK, TILE), bf), pltpu.VMEM((cols // TILE, n_j * CHUNK, TILE), bf),
            pltpu.VMEM((n_j * CHUNK, cols), bf), pltpu.VMEM((n_h, 64, attn.shape[1]), bf),
            pltpu.VMEM((n_h, 8, 16, half), bf), pltpu.VMEM((n_h, 4, 16, half), bf), pltpu.VMEM((n_h, 3, 16, half), bf), pltpu.VMEM((n_h, 3, 16, half), bf), pltpu.VMEM((n_h, 16, half), bf), pltpu.VMEM((n_h, 8, 16, half), bf),
            pltpu.VMEM((n_h, 8, 128), f32), pltpu.VMEM((n_h, 4, 8, 128), f32), pltpu.VMEM((n_h, 8, 128), f32), pltpu.VMEM((n_h, 8, 8, 128), f32), pltpu.VMEM((n_h, ROWS, cols), bf),
            pltpu.VMEM((steps, 2, 2, 16, 2 * CHUNK), bf), pltpu.VMEM((steps, 2, 16, 2 * CHUNK), bf), pltpu.VMEM((steps, 16, 2 * CHUNK), f32),
            pltpu.VMEM((steps, 16, 2 * CHUNK), bf), pltpu.VMEM((steps, 16, 2 * CHUNK), bf), pltpu.VMEM((steps, 4, 16, CHUNK), bf),
            pltpu.VMEM((n_h, ROWS, cols), f32),
            pltpu.VMEM((n_h, 8, 16, half), bf), pltpu.VMEM((n_h, 4, 16, half), bf), pltpu.VMEM((n_h, 3, 16, half), bf), pltpu.VMEM((n_h, 3, 16, half), bf), pltpu.VMEM((n_h, 16, half), bf), pltpu.VMEM((TILE, TILE), bf),
            dma((1 + 2 * (cols // TILE),)), dma((15,)), dma((n_h,)), dma((n_h,)), dma((n_h,)), dma((n_h, 4)), dma((n_h,)), dma((n_h, 3)), dma((n_h,)), dma((n_h, 4)), dma((n_h,)), dma((n_h, 3)), dma((n_h,)),
            dma((steps,)), dma((steps,)), dma((steps,)), dma((steps,)), dma((steps,)),
        ],
        compiler_params=pltpu.CompilerParams(collective_id=1, has_side_effects=True, vmem_limit_bytes=MLP_LIMIT),
    )(x_in, gain, attn, w_o, pinned(w_gate), pinned(w_up), pinned(w_down))


def place_kernel(pieces_ref, out_ref):
    n_h, _, _, half = pieces_ref.shape
    for h in range(n_h):
        for z in range(4):
            for y in range(2):
                r0 = z * 16 * n_h + h * 16
                out_ref[r0:r0 + 16, y * half:(y + 1) * half] = pieces_ref[h, 2 * z + y]


def place_call(pieces, shape):
    vmem = pl.BlockSpec(memory_space=pltpu.VMEM)
    return pl.pallas_call(place_kernel, name="place", out_shape=jax.ShapeDtypeStruct(shape, pieces.dtype), in_specs=[vmem], out_specs=vmem, compiler_params=pltpu.CompilerParams(vmem_limit_bytes=4 * 1024 * 1024))(pieces)


GROUP_ROWS = 16


def attn_kernel(seq_ref, proj_ref, bq_ref, bk_ref, bv_ref, freq_ref, k_ref, v_ref, attn_ref, ko_hbm, vo_hbm, qs, kn, vn, os, pos, patch, out_sem, patch_sem):
    f32, bf = jnp.float32, jnp.bfloat16
    rows, seq = k_ref.shape[0], k_ref.shape[1]
    heads = attn_ref.shape[1] // HEAD
    groups = rows // GROUP_ROWS
    outs = [ko_hbm, vo_hbm]

    def bulk(g):
        part = pl.ds(g * GROUP_ROWS, GROUP_ROWS)
        return [pltpu.make_async_copy(src.at[part], dst.at[part], out_sem.at[i, g]) for i, (src, dst) in enumerate(zip((k_ref, v_ref), outs))]

    for g in range(groups):
        for cp in bulk(g):
            cp.start()
    for b in range(rows):
        pos[b:b + 1, :] = jnp.full((1, HEAD), seq_ref[b], jnp.int32).astype(f32)
    angles = pos[...] * freq_ref[...]
    lower = lax.broadcasted_iota(jnp.int32, (rows, HEAD), 1) < HEAD // 2
    cos_tab = jnp.cos(angles)
    sin_tab = jnp.sin(angles)
    sin_tab = jnp.where(lower, -sin_tab, sin_tab)

    def column(c, bias_ref, k):
        bias = bias_ref[pl.ds(k * HEAD, HEAD)].astype(f32).reshape(1, HEAD)
        return proj_ref[:, c * HEAD:(c + 1) * HEAD] + bias

    def rotate(v):
        return (v * cos_tab + pltpu.roll(v, HEAD // 2, 1) * sin_tab).astype(bf).astype(f32)

    with jax.named_scope('a_pre'):
        qs[...] = jnp.zeros_like(qs)
    for h in range(heads):
        qs[:, h, :] = rotate(column(h, bq_ref, h))
    kn[...] = rotate(column(heads, bk_ref, 0))
    vn[...] = column(heads + 1, bv_ref, 0).astype(bf).astype(f32)

    def slab_of(b):
        p = seq_ref[b]
        return p, pl.multiple_of((p // 16) * 16, 16)

    def body(g, carry):
        times = lax.broadcasted_iota(jnp.int32, (8, seq), 1)
        slots = lax.broadcasted_iota(jnp.int32, (16, HEAD), 0)
        scores, news, hits = [], [], []
        for r in range(GROUP_ROWS):
            b = g * GROUP_ROWS + r
            p, slab = slab_of(b)
            hit = slots == p - slab
            for i, (cache, new) in enumerate(((k_ref, kn), (v_ref, vn))):
                old = cache[b, pl.ds(slab, 16), :].astype(f32)
                patch[i, b] = jnp.where(hit, new[pl.ds(b, 1), :], old).astype(bf)
            q = qs[b]
            s = lax.dot_general(q.astype(bf), k_ref[b], (((1,), (1,)), ((), ())), preferred_element_type=f32) * HEAD ** -0.5
            s_new = jnp.sum(q * kn[pl.ds(b, 1), :], axis=1, keepdims=True) * HEAD ** -0.5
            hits.append(times == p)
            news.append(s_new)
            scores.append(jnp.where(hits[r], s_new, jnp.where(times < p, s, -jnp.inf)))
        s = jnp.concatenate(scores, axis=0)
        top = jnp.max(s, axis=1, keepdims=True)
        w = jnp.exp(s - top)
        total = jnp.sum(w, axis=1, keepdims=True)
        w_new = jnp.exp(jnp.concatenate(news, axis=0) - top).astype(bf).astype(f32)
        w = jnp.where(jnp.concatenate(hits, axis=0), 0.0, w).astype(bf)
        for r in range(GROUP_ROWS):
            b = g * GROUP_ROWS + r
            part = slice(8 * r, 8 * r + 8)
            o = jnp.dot(w[part], v_ref[b], preferred_element_type=f32) + w_new[part] * vn[pl.ds(b, 1), :]
            os[b] = o / total[part]
        return carry

    with jax.named_scope('a_main'):
        lax.fori_loop(0, groups, body, 0)
    for h in range(heads):
        attn_ref[:, h * HEAD:(h + 1) * HEAD] = os[:, h, :].astype(bf)

    def patches(b):
        slab = slab_of(b)[1]
        return [pltpu.make_async_copy(patch.at[i, b], dst.at[b, pl.ds(slab, 16)], patch_sem.at[i]) for i, dst in enumerate(outs)]

    for g in range(groups):
        with jax.named_scope('a_bulk'):
            for cp in bulk(g):
                cp.wait()
        for b in range(g * GROUP_ROWS, (g + 1) * GROUP_ROWS):
            for cp in patches(b):
                cp.start()
    with jax.named_scope('a_patch'):
        for b in range(rows):
            for cp in patches(b):
                cp.wait()


def attn_call(seq_lens, projected, b_q, b_k, b_v, k_cache, v_cache):
    rows, seq = k_cache.shape[0], k_cache.shape[1]
    f32, bf = jnp.float32, jnp.bfloat16
    freq = (ROPE_THETA ** (-2.0 * np.arange(HEAD // 2) / HEAD)).astype(np.float32)
    freq = jnp.asarray(np.concatenate([freq, freq])[None])
    any_spec, vmem, smem = pl.BlockSpec(memory_space=pl.ANY), pl.BlockSpec(memory_space=pltpu.VMEM), pl.BlockSpec(memory_space=pltpu.SMEM)
    dma = pltpu.SemaphoreType.DMA
    cache = jax.ShapeDtypeStruct((rows, seq, HEAD), bf)
    return pl.pallas_call(
        attn_kernel,
        name="attn",
        out_shape=(jax.ShapeDtypeStruct((rows, b_q.shape[0]), bf), cache, cache),
        in_specs=[smem, vmem, vmem, vmem, vmem, vmem, vmem, vmem],
        out_specs=(vmem, any_spec, any_spec),
        scratch_shapes=[
            pltpu.VMEM((rows, 8, HEAD), f32), pltpu.VMEM((rows, HEAD), f32),
            pltpu.VMEM((rows, HEAD), f32), pltpu.VMEM((rows, 8, HEAD), f32), pltpu.VMEM((rows, HEAD), f32), pltpu.VMEM((2, rows, 16, HEAD), bf),
            dma((2, rows // GROUP_ROWS)), dma((2,)),
        ],
        compiler_params=pltpu.CompilerParams(vmem_limit_bytes=ATTN_LIMIT),
    )(seq_lens, projected, b_q, b_k, b_v, freq, k_cache.reshape(rows, seq, HEAD), v_cache.reshape(rows, seq, HEAD))


def solution(mesh):
    mx_size = mesh.shape["mx"]
    act_spec = P(None, "mx")
    cache_spec = P("mx", None, "my", None)
    in_specs = (act_spec, P("mx"), P("mx"), P("mx"), P("mx", "my"), P("my"), P("mx", "my"), P("my"), P("mx", "my"), P("my"), P("my", "mx"), P("mx", "my"), P("mx", "my"), P("my", "mx"), cache_spec, cache_spec)
    out_specs = (act_spec, cache_spec, cache_spec)

    def local_layer(x_in, seq_lens, gain_attn, gain_mlp, w_q, b_q, w_k, b_k, w_v, b_v, w_o, w_gate, w_up, w_down, k_cache, v_cache):
        hidden = x_in.shape[1] * mx_size
        projected = qkv_call(x_in, gain_attn, w_q, w_k, w_v, hidden)
        attn_rows, k_out, v_out = attn_call(seq_lens, projected, b_q, b_k, b_v, k_cache, v_cache)
        pieces = mlp_call(x_in, gain_mlp, attn_rows, w_o, w_gate.T, w_up.T, w_down, hidden)
        x_out = place_call(pieces, x_in.shape)
        k_cache_out, v_cache_out = k_out.reshape(k_cache.shape), v_out.reshape(v_cache.shape)
        return x_out, k_cache_out, v_cache_out

    return jax.shard_map(local_layer, mesh=mesh, in_specs=in_specs, out_specs=out_specs, check_vma=False)
```

```python
import functools
import types

import jax
import jax.numpy as jnp
import numpy as np
from jax import lax
from jax.experimental import pallas as pl
from jax.experimental.pallas import tpu as pltpu
from jax.sharding import PartitionSpec as P

HEAD = 128
NORM_EPS = 1e-6
ROPE_THETA = 1000000.0
MESH = pl.DeviceIdType.MESH
CHUNK = 512
TILE = 256
DIRECT = 2
ROWS = 64
LAG_B, LAG_C, LAG_D, LAG_E, LAG_M, LAG_F = 1, 4, 7, 8, 3, 9
VMEM_LIMIT = 67043328
MLP_LIMIT = 48 * 1024 * 1024
ATTN_LIMIT = 14 * 1024 * 1024
QKV_LIMIT = 8 * 1024 * 1024


def rcopy(src, dst, send_sem, recv_sem, dev):
    return pltpu.make_async_remote_copy(src_ref=src, dst_ref=dst, send_sem=send_sem, recv_sem=recv_sem, device_id=dev, device_id_type=MESH)


def pinned(x):
    return pltpu.with_memory_space_constraint(x, pltpu.HBM)


def lane_ids():
    return lax.broadcasted_iota(jnp.int32, (8, 128), 1)


def pack_column(blocks):
    tile = jnp.zeros((8, 128), jnp.float32)
    lanes = lane_ids()
    for k, block in enumerate(blocks):
        tile = jnp.where(lanes == k, block, tile)
    return tile


def unpack_column(tile, k):
    return jnp.sum(jnp.where(lane_ids() == k, tile, 0.0), axis=1, keepdims=True)


def qkv_kernel(hidden, x_hbm, gain_hbm, wq_hbm, wk_hbm, wv_hbm, out_ref, gain_ref, x_v, wq_v, wk_v, wv_v, st_own, st_in, nrm, pp, dr, own, xs, xr, ld_sem, send_sem, st_sem, d_sem, x_sem):
    mx = lax.axis_index("mx")
    xi, ci = mx // 2, mx % 2
    partner, xpeer = 2 * xi + (1 - ci), 2 * (1 - xi) + ci
    loads = [pltpu.make_async_copy(s, d, ld_sem.at[i]) for i, (s, d) in enumerate([(x_hbm, x_v), (gain_hbm, gain_ref), (wq_hbm, wq_v), (wk_hbm, wk_v), (wv_hbm, wv_v)])]
    for ld in loads:
        ld.start()
    barrier = pltpu.get_barrier_semaphore()
    for d in range(1, 4):
        pl.semaphore_signal(barrier, inc=1, device_id={"mx": (mx + d) % 4}, device_id_type=MESH)
    pl.semaphore_wait(barrier, 3)

    rows = x_v.shape[0]
    loads[0].wait()
    blocks = []
    for k in range(rows // 8):
        v = x_v[8 * k:8 * k + 8, :].astype(jnp.float32)
        blocks.append(jnp.sum(v * v, axis=1, keepdims=True))
    tile = pack_column(blocks)
    st_own[...] = tile
    st_in[mx] = tile
    for d in range(1, 4):
        rcopy(st_own, st_in.at[mx], send_sem.at[0], st_sem, {"mx": (mx + d) % 4}).start()
    for ld in loads[1:]:
        ld.wait()
    rcopy(st_in.at[pl.ds(0, 3)], st_in.at[pl.ds(0, 3)], send_sem.at[0], st_sem, {"mx": partner}).wait()
    total = st_in[0] + st_in[1] + st_in[2] + st_in[3]
    scale = lax.rsqrt(total / hidden + NORM_EPS)
    gain = gain_ref[...].astype(jnp.float32).reshape(1, x_v.shape[1])
    for k in range(0, rows // 8, 2):
        col = jnp.concatenate([unpack_column(scale, k), unpack_column(scale, k + 1)], axis=0)
        nrm[8 * k:8 * k + 16, :] = (x_v[8 * k:8 * k + 16, :].astype(jnp.float32) * col * gain).astype(jnp.bfloat16)

    lhs = nrm[...]
    part = rows // 4
    width = out_ref.shape[1]
    offs = [0, wq_v.shape[1], wq_v.shape[1] + wk_v.shape[1]]
    pieces = [(w, c0, min(c0 + TILE, w.shape[1]), off) for w, off in zip((wq_v, wk_v, wv_v), offs) for c0 in range(0, w.shape[1], TILE)]
    cut = 2 * TILE
    parts = ((0, cut), (cut, width))

    def swap(i):
        cols = pl.ds(parts[i][0], parts[i][1] - parts[i][0])
        return rcopy(pp.at[1 - ci, :, :, cols], dr.at[:, :, cols], send_sem.at[1], d_sem.at[i], {"mx": partner})

    def cross(i):
        cols = pl.ds(parts[i][0], parts[i][1] - parts[i][0])
        return rcopy(xs.at[:, cols], xr.at[:, cols], send_sem.at[2], x_sem.at[i], {"mx": xpeer})

    for i, (lo, hi) in enumerate(parts):
        for w, c0, c1, off in pieces:
            if lo <= off + c0 < hi:
                r = jnp.dot(lhs, w[:, c0:c1], preferred_element_type=jnp.float32).astype(jnp.bfloat16)
                for m in range(4):
                    pp[m % 2, m // 2, :, off + c0:off + c1] = r[m * part:(m + 1) * part]
        swap(i).start()
    for i, (lo, hi) in enumerate(parts):
        swap(i).wait_recv()
        xs[:, lo:hi] = (pp[ci, 1 - xi, :, lo:hi].astype(jnp.float32) + dr[1 - xi, :, lo:hi].astype(jnp.float32)).astype(jnp.bfloat16)
        cross(i).start()
        own[:, lo:hi] = pp[ci, xi, :, lo:hi].astype(jnp.float32) + dr[xi, :, lo:hi].astype(jnp.float32)
    for i, (lo, hi) in enumerate(parts):
        cross(i).wait_recv()
        out_ref[:, lo:hi] = own[:, lo:hi] + xr[:, lo:hi].astype(jnp.float32)
    for i in range(2):
        swap(i).wait_send()
        cross(i).wait_send()


def qkv_call(x_in, gain, w_q, w_k, w_v, hidden):
    rows, cols = x_in.shape
    width = w_q.shape[1] + w_k.shape[1] + w_v.shape[1]
    bf, f32 = jnp.bfloat16, jnp.float32
    any_spec, vmem = pl.BlockSpec(memory_space=pl.ANY), pl.BlockSpec(memory_space=pltpu.VMEM)
    part = rows // 4
    return pl.pallas_call(
        functools.partial(qkv_kernel, hidden),
        name="qkv",
        out_shape=jax.ShapeDtypeStruct((part, width), f32),
        in_specs=[any_spec] * 5,
        out_specs=vmem,
        scratch_shapes=[
            pltpu.VMEM(gain.shape, bf),
            pltpu.VMEM((rows, cols), bf), pltpu.VMEM(w_q.shape, bf), pltpu.VMEM(w_k.shape, bf), pltpu.VMEM(w_v.shape, bf),
            pltpu.VMEM((8, 128), f32), pltpu.VMEM((4, 8, 128), f32), pltpu.VMEM((rows, cols), bf),
            pltpu.VMEM((2, 2, part, width), bf), pltpu.VMEM((2, part, width), bf), pltpu.VMEM((part, width), f32),
            pltpu.VMEM((part, width), bf), pltpu.VMEM((part, width), bf),
            pltpu.SemaphoreType.DMA((5,)), pltpu.SemaphoreType.DMA((3,)), pltpu.SemaphoreType.DMA, pltpu.SemaphoreType.DMA((2,)), pltpu.SemaphoreType.DMA((2,)),
        ],
        compiler_params=pltpu.CompilerParams(collective_id=0, has_side_effects=True, vmem_limit_bytes=QKV_LIMIT),
        cost_estimate=pl.CostEstimate(flops=10 ** 10, bytes_accessed=3 * 10 ** 6, transcendentals=0),
    )(pinned(x_in), pinned(gain), pinned(w_q), pinned(w_k), pinned(w_v))


def mlp_kernel(hidden, x_v, gain_ref, attn_ref, wo_v, wg_hbm, wu_hbm, wd_hbm, ag2,
               wg_v, wu_v, wd_v, attn_v, p1, yb1, zs1, zb1, mp, ag1, st_own, st_in, st_sum, st_all, h2,
               pp, dr, own, xs, xr, act, dacc, p2, yb2, zs2, zb2, mo, eye,
               ld_sem, send_sem, at_sem, st_sem, sg_sem, ysem1, zsem1, agz1, agy1, ysem2, zsem2, agz2, agy2, d_sem, x_sem, ax_sem, ad_sem, af_sem):
    my, mx = lax.axis_index("my"), lax.axis_index("mx")
    n_my = 8
    xi, ci = mx // 2, mx % 2
    zi, yi = my // 2, my % 2
    partner, xpeer = 2 * xi + (1 - ci), 2 * (1 - xi) + ci
    core_dev, x_dev = {"mx": partner}, {"mx": xpeer}
    n_h = h2.shape[0]
    ff = wg_hbm.shape[0]
    n_j = pl.cdiv(ff, CHUNK)
    steps = n_h * n_j
    half = x_v.shape[1] // 2
    brows = attn_ref.shape[0]
    f32, bf = jnp.float32, jnp.bfloat16

    n_k = wg_v.shape[0]
    tiles = [(src.at[:, pl.ds(TILE * k, TILE)], dst.at[k, pl.ds(0, ff)]) for src, dst in ((wg_hbm, wg_v), (wu_hbm, wu_v)) for k in range(n_k)]
    loads = [pltpu.make_async_copy(s, d, ld_sem.at[i]) for i, (s, d) in enumerate(tiles + [(wd_hbm, wd_v.at[pl.ds(0, ff)])])]
    for ld in loads:
        ld.start()
    barrier = pltpu.get_barrier_semaphore()
    for d in range(1, 4):
        pl.semaphore_signal(barrier, inc=1, device_id={"mx": (mx + d) % 4}, device_id_type=MESH)
    for d in range(1, n_my):
        pl.semaphore_signal(barrier, inc=1, device_id={"my": (my + d) % n_my}, device_id_type=MESH)
    pl.semaphore_wait(barrier, 3 + n_my - 1)

    mine = pl.ds(pl.multiple_of(mx * 16, 16), 16)
    for h in range(n_h):
        for d in range(1, 4):
            rcopy(attn_ref.at[pl.ds(16 * h, 16)], attn_v.at[h, mine], send_sem.at[0], at_sem.at[h], {"mx": (mx + d) % 4}).start()
    for h in range(n_h):
        attn_v[h, mine, :] = attn_ref[16 * h:16 * h + 16, :]
    dacc[...] = jnp.zeros_like(dacc)
    wd_v[ff:, :] = jnp.zeros((wd_v.shape[0] - ff, wd_v.shape[1]), bf)
    for w in (wg_v, wu_v):
        for k in range(n_k):
            w[k, ff:, :] = jnp.zeros((w.shape[1] - ff, TILE), bf)
    eye[...] = (lax.broadcasted_iota(jnp.int32, (TILE, TILE), 0) == lax.broadcasted_iota(jnp.int32, (TILE, TILE), 1)).astype(f32).astype(bf)

    zs = (3 - zi, (zi + 2) % 4, zi + 1 - 2 * (zi % 2), zi)
    peers = [2 * z + y for z in zs for y in (1 - yi, yi)][:-1]
    y_peer = 2 * zi + 1 - yi
    y_dev = {"my": y_peer}
    z_devs = [{"my": 2 * z + yi} for z in zs[:3]]

    def project(h):
        gathered = attn_v.at[h, pl.ds(0, 48)]
        rcopy(gathered, gathered, send_sem.at[0], at_sem.at[h], core_dev).wait_recv()
        for y in range(2):
            r = jnp.dot(attn_v[h], wo_v[:, y * half:(y + 1) * half], preferred_element_type=f32).astype(bf)
            for z in range(4):
                p1[h, 2 * z + y] = r[16 * z:16 * z + 16]

    parts = ((0, TILE), (TILE, half))
    spans = [pl.ds(lo, hi - lo) for lo, hi in parts]

    def rs_start(r, h):
        for i, cols in enumerate(spans):
            for k, z in enumerate(zs):
                rcopy(r.part.at[h, 2 * z + 1 - yi, :, cols], r.ybuf.at[h, k, :, cols], send_sem.at[r.sem], r.ysem.at[h, i, k], y_dev).start()

    def wait_y(r, h, i, k):
        got = r.ybuf.at[h, k, :, spans[i]]
        rcopy(got, got, send_sem.at[r.sem], r.ysem.at[h, i, k], y_dev).wait_recv()

    def rs_mid(r, h):
        for i, (lo, hi) in enumerate(parts):
            for k in range(3):
                wait_y(r, h, i, k)
                r.zsend[h, k, :, lo:hi] = (r.part[h, 2 * zs[k] + yi, :, lo:hi].astype(f32) + r.ybuf[h, k, :, lo:hi].astype(f32)).astype(bf)
                rcopy(r.zsend.at[h, k, :, spans[i]], r.zbuf.at[h, k, :, spans[i]], send_sem.at[r.sem + 1], r.zsem.at[h, i], z_devs[k]).start()

    def rs_fin(r, h, i, base):
        lo, hi = parts[i]
        wait_y(r, h, i, 3)
        got = r.zbuf.at[h, :, :, spans[i]]
        rcopy(got, got, send_sem.at[r.sem + 1], r.zsem.at[h, i], y_dev).wait_recv()
        total = r.part[h, my, :, lo:hi].astype(f32) + r.ybuf[h, 3, :, lo:hi].astype(f32)
        for k in range(3):
            total += r.zbuf[h, k, :, lo:hi].astype(f32)
        return (base + total).astype(bf)

    def ag_start(r, h, i, val):
        lo, hi = parts[i]
        r.piece[h, :, lo:hi] = val
        r.all[h, my, :, lo:hi] = val
        src, dst = r.piece.at[h, :, spans[i]], r.all.at[h, my, :, spans[i]]
        for k in range(3):
            rcopy(src, dst, send_sem.at[r.sem + 2], r.agz.at[h, i, k], z_devs[k]).start()
        rcopy(src, dst, send_sem.at[r.sem + 2], r.agy.at[h, i], y_dev).start()

    def ag_mid(r, h):
        for i in range(2):
            for k in (2, 1, 0):
                got = r.all.at[h, 2 * zs[k] + yi, :, spans[i]]
                rcopy(got, got, send_sem.at[r.sem + 2], r.agz.at[h, i, k], y_dev).wait_recv()
                rcopy(got, got, send_sem.at[r.sem + 2], r.agy.at[h, i], y_dev).start()

    def ag_fin(r, h):
        for i in range(2):
            four = r.all.at[h, pl.ds(0, 4), :, spans[i]]
            rcopy(four, four, send_sem.at[r.sem + 2], r.agy.at[h, i], y_dev).wait_recv()

    one = types.SimpleNamespace(part=p1, ybuf=yb1, zsend=zs1, zbuf=zb1, piece=mp, all=ag1, ysem=ysem1, zsem=zsem1, agz=agz1, agy=agy1, sem=9)
    two = types.SimpleNamespace(part=p2, ybuf=yb2, zsend=zs2, zbuf=zb2, piece=mo, all=ag2, ysem=ysem2, zsem=zsem2, agz=agz2, agy=agy2, sem=12)

    def rs1_finish(h):
        r0 = pl.multiple_of(zi * brows + h * 16, 16)
        ss = jnp.zeros((16, 1), f32)
        for i, (lo, hi) in enumerate(parts):
            base = x_v[pl.ds(r0, 16), pl.ds(pl.multiple_of(yi * half + lo, 128), hi - lo)].astype(f32)
            m = rs_fin(one, h, i, base)
            ag_start(one, h, i, m)
            m = m.astype(f32)
            ss += jnp.sum(m * m, axis=1, keepdims=True)
        tile = pack_column([ss[:8], ss[8:]])
        st_own[h] = tile
        st_in[h, mx] = tile
        for d in range(1, 4):
            rcopy(st_own.at[h], st_in.at[h, mx], send_sem.at[3], st_sem.at[h], {"mx": (mx + d) % 4}).start()

    def stat_gather(h):
        three = st_in.at[h, pl.ds(0, 3)]
        rcopy(three, three, send_sem.at[3], st_sem.at[h], core_dev).wait_recv()
        total = st_in[h, 0] + st_in[h, 1] + st_in[h, 2] + st_in[h, 3]
        st_sum[h] = total
        st_all[h, my] = total
        for peer in peers:
            rcopy(st_sum.at[h], st_all.at[h, my], send_sem.at[1], sg_sem.at[h], {"my": peer}).start()

    def norm(h):
        seven = st_all.at[h, pl.ds(0, n_my - 1)]
        rcopy(seven, seven, send_sem.at[1], sg_sem.at[h], y_dev).wait_recv()
        ag_fin(one, h)
        for z in range(4):
            scale = lax.rsqrt((st_all[h, 2 * z] + st_all[h, 2 * z + 1]) / hidden + NORM_EPS)
            col = jnp.concatenate([unpack_column(scale, 0), unpack_column(scale, 1)], axis=0)
            for y in range(2):
                gain = gain_ref[pl.ds(y * half, half)].astype(f32).reshape(1, half)
                h2[h, 16 * z:16 * z + 16, y * half:(y + 1) * half] = (ag1[h, 2 * z + y].astype(f32) * col * gain).astype(bf)

    def transpose(i, carry):
        rows = pl.ds(pl.multiple_of(i * TILE, TILE), TILE)
        for k in range(n_k):
            flipped = [lax.dot_general(eye[...], w[k, rows, :], (((1,), (1,)), ((), ())), preferred_element_type=f32).astype(bf) for w in (wg_v, wu_v)]
            for w, val in zip((wg_v, wu_v), flipped):
                w[k, rows, :] = val
        return carry

    def stage_a(s):
        h, j = s // n_j, s % n_j
        lhs = h2[h]
        for i, w in enumerate((wg_v, wu_v)):
            cols = []
            for n in range(CHUNK // TILE):
                rows = pl.ds(pl.multiple_of(j * CHUNK + n * TILE, TILE), TILE)
                acc = jnp.dot(lhs[:, :TILE], w[0, rows, :], preferred_element_type=f32)
                for k in range(1, n_k):
                    acc += jnp.dot(lhs[:, TILE * k:TILE * (k + 1)], w[k, rows, :], preferred_element_type=f32)
                cols.append(acc.astype(bf))
            val = jnp.concatenate(cols, axis=1)
            for m in range(4):
                pp[s, m % 2, m // 2, :, i * CHUNK:(i + 1) * CHUNK] = val[16 * m:16 * m + 16]
        rcopy(pp.at[s, 1 - ci], dr.at[s], send_sem.at[4], d_sem.at[s], core_dev).start()

    def stage_b(s):
        rcopy(pp.at[s, 1 - ci], dr.at[s], send_sem.at[4], d_sem.at[s], core_dev).wait_recv()
        xs[s] = (pp[s, ci, 1 - xi].astype(f32) + dr[s, 1 - xi].astype(f32)).astype(bf)
        rcopy(xs.at[s], xr.at[s], send_sem.at[5], x_sem.at[s], x_dev).start()
        own[s] = pp[s, ci, xi].astype(f32) + dr[s, xi].astype(f32)

    def stage_c(s):
        rcopy(xs.at[s], xr.at[s], send_sem.at[5], x_sem.at[s], x_dev).wait_recv()
        g = own[s, :, :CHUNK] + xr[s, :, :CHUNK].astype(f32)
        u = own[s, :, CHUNK:] + xr[s, :, CHUNK:].astype(f32)
        act[s, mx] = (jax.nn.silu(g) * u).astype(bf)
        rcopy(act.at[s, mx], act.at[s, mx], send_sem.at[6], ax_sem.at[s], x_dev).start()
        rcopy(act.at[s, mx], act.at[s, mx], send_sem.at[7], ad_sem.at[s], core_dev).start()

        @pl.when(s >= steps - DIRECT)
        def _():
            rcopy(act.at[s, mx], act.at[s, mx], send_sem.at[8], af_sem.at[s], {"mx": 2 * (1 - xi) + (1 - ci)}).start()

    def stage_d(s):
        rcopy(act.at[s, xpeer], act.at[s, xpeer], send_sem.at[6], ax_sem.at[s], x_dev).wait_recv()

        @pl.when(s < steps - DIRECT)
        def _():
            rcopy(act.at[s, xpeer], act.at[s, xpeer], send_sem.at[8], af_sem.at[s], core_dev).start()

    def stage_e(s):
        h, j = s // n_j, s % n_j
        rcopy(act.at[s, 0], act.at[s, 0], send_sem.at[7], ad_sem.at[s], core_dev).wait_recv()
        rcopy(act.at[s, 0], act.at[s, 0], send_sem.at[8], af_sem.at[s], core_dev).wait_recv()
        lhs = act[s].reshape(ROWS, CHUNK)
        dacc[h] += jnp.dot(lhs, wd_v[pl.ds(pl.multiple_of(j * CHUNK, CHUNK), CHUNK), :], preferred_element_type=f32)

    def rs2_send(h):
        for z in range(4):
            for y in range(2):
                p2[h, 2 * z + y] = dacc[h, 16 * z:16 * z + 16, y * half:(y + 1) * half].astype(bf)
        rs_start(two, h)

    def rs2_finish(h):
        for i, (lo, hi) in enumerate(parts):
            ag_start(two, h, i, rs_fin(two, h, i, mp[h, :, lo:hi].astype(f32)))

    n_t = n_j * (CHUNK // TILE)
    def flip(lo, hi):
        lax.fori_loop(lo, hi, transpose, 0)

    project(0)
    rs_start(one, 0)
    project(1)
    rs_start(one, 1)
    project(2)
    for ld in loads[:-1]:
        ld.wait()
    flip(0, 2)
    rs_mid(one, 0)
    flip(2, 5)
    rs_mid(one, 1)
    flip(5, 8)
    rs1_finish(0)
    rs_start(one, 2)
    flip(8, 10)
    rs1_finish(1)
    stat_gather(0)
    flip(10, 12)
    rs_mid(one, 2)
    ag_mid(one, 0)
    flip(12, n_t)
    stat_gather(1)
    norm(0)

    def body(t, carry):
        @pl.when(t == n_j)
        def _():
            norm(1)

        @pl.when(t == 2 * n_j)
        def _():
            norm(2)

        @pl.when(t == 1)
        def _():
            ag_mid(one, 1)

        @pl.when(t == 2)
        def _():
            rs1_finish(2)

        @pl.when(t == 5)
        def _():
            stat_gather(2)

        @pl.when(t == n_j + 1)
        def _():
            ag_mid(one, 2)

        @pl.when(t < steps)
        def _():
            stage_a(t)

        @pl.when((t >= LAG_B) & (t < steps + LAG_B))
        def _():
            stage_b(t - LAG_B)

        @pl.when((t >= LAG_C) & (t < steps + LAG_C))
        def _():
            stage_c(t - LAG_C)

        @pl.when((t >= LAG_D) & (t < steps + LAG_D))
        def _():
            stage_d(t - LAG_D)

        @pl.when(t == LAG_E)
        def _():
            loads[-1].wait()

        @pl.when(t >= LAG_E)
        def _():
            s = t - LAG_E
            stage_e(s)

            @pl.when(s % n_j == n_j - 1)
            def _():
                rs2_send(s // n_j)

        after = t - LAG_E - (n_j - 1)

        @pl.when((after >= LAG_M) & ((after - LAG_M) % n_j == 0))
        def _():
            rs_mid(two, (after - LAG_M) // n_j)

        @pl.when((after >= LAG_F) & ((after - LAG_F) % n_j == 0))
        def _():
            rs2_finish((after - LAG_F) // n_j)

        return carry

    total_t = steps + LAG_E
    lax.fori_loop(0, total_t, body, 0)
    rs_mid(two, 2)
    rs2_finish(1)
    ag_mid(two, 0)
    rs2_finish(2)
    ag_mid(two, 1)
    ag_mid(two, 2)
    for h in range(n_h):
        ag_fin(two, h)
    seven = pl.ds(0, n_my - 1)
    for k, ref in ((0, attn_v.at[:, pl.ds(0, 48)]), (1, st_all.at[:, seven]), (3, st_in.at[:, pl.ds(0, 3)]), (4, dr), (5, xs), (6, act.at[:, 0]), (7, act.at[:, 0]), (8, act.at[:, 0]),
                   (9, yb1), (10, zb1), (11, ag1.at[:, seven]), (12, yb2), (13, zb2), (14, ag2.at[:, seven])):
        rcopy(ref, ref, send_sem.at[k], at_sem.at[0], core_dev).wait_send()


def mlp_call(x_in, gain, attn, w_o, w_gate, w_up, w_down, hidden):
    rows, cols = x_in.shape
    ff = w_gate.shape[0]
    n_j = pl.cdiv(ff, CHUNK)
    n_h = rows // ROWS
    steps = n_h * n_j
    half = cols // 2
    bf, f32 = jnp.bfloat16, jnp.float32
    hbm, vmem = pl.BlockSpec(memory_space=pltpu.HBM), pl.BlockSpec(memory_space=pltpu.VMEM)
    dma = pltpu.SemaphoreType.DMA
    return pl.pallas_call(
        functools.partial(mlp_kernel, hidden),
        name="mlp",
        out_shape=jax.ShapeDtypeStruct((n_h, 8, 16, half), bf),
        in_specs=[vmem, vmem, vmem, vmem, hbm, hbm, hbm],
        out_specs=vmem,
        scratch_shapes=[
            pltpu.VMEM((cols // TILE, n_j * CHUNK, TILE), bf), pltpu.VMEM((cols // TILE, n_j * CHUNK, TILE), bf),
            pltpu.VMEM((n_j * CHUNK, cols), bf), pltpu.VMEM((n_h, 64, attn.shape[1]), bf),
            pltpu.VMEM((n_h, 8, 16, half), bf), pltpu.VMEM((n_h, 4, 16, half), bf), pltpu.VMEM((n_h, 3, 16, half), bf), pltpu.VMEM((n_h, 3, 16, half), bf), pltpu.VMEM((n_h, 16, half), bf), pltpu.VMEM((n_h, 8, 16, half), bf),
            pltpu.VMEM((n_h, 8, 128), f32), pltpu.VMEM((n_h, 4, 8, 128), f32), pltpu.VMEM((n_h, 8, 128), f32), pltpu.VMEM((n_h, 8, 8, 128), f32), pltpu.VMEM((n_h, ROWS, cols), bf),
            pltpu.VMEM((steps, 2, 2, 16, 2 * CHUNK), bf), pltpu.VMEM((steps, 2, 16, 2 * CHUNK), bf), pltpu.VMEM((steps, 16, 2 * CHUNK), f32),
            pltpu.VMEM((steps, 16, 2 * CHUNK), bf), pltpu.VMEM((steps, 16, 2 * CHUNK), bf), pltpu.VMEM((steps, 4, 16, CHUNK), bf),
            pltpu.VMEM((n_h, ROWS, cols), f32),
            pltpu.VMEM((n_h, 8, 16, half), bf), pltpu.VMEM((n_h, 4, 16, half), bf), pltpu.VMEM((n_h, 3, 16, half), bf), pltpu.VMEM((n_h, 3, 16, half), bf), pltpu.VMEM((n_h, 16, half), bf), pltpu.VMEM((TILE, TILE), bf),
            dma((1 + 2 * (cols // TILE),)), dma((15,)), dma((n_h,)), dma((n_h,)), dma((n_h,)), dma((n_h, 2, 4)), dma((n_h, 2)), dma((n_h, 2, 3)), dma((n_h, 2)), dma((n_h, 2, 4)), dma((n_h, 2)), dma((n_h, 2, 3)), dma((n_h, 2)),
            dma((steps,)), dma((steps,)), dma((steps,)), dma((steps,)), dma((steps,)),
        ],
        compiler_params=pltpu.CompilerParams(collective_id=1, has_side_effects=True, vmem_limit_bytes=MLP_LIMIT),
    )(x_in, gain, attn, w_o, pinned(w_gate), pinned(w_up), pinned(w_down))


def place_kernel(pieces_ref, out_ref):
    n_h, _, _, half = pieces_ref.shape
    for h in range(n_h):
        for z in range(4):
            for y in range(2):
                r0 = z * 16 * n_h + h * 16
                out_ref[r0:r0 + 16, y * half:(y + 1) * half] = pieces_ref[h, 2 * z + y]


def place_call(pieces, shape):
    vmem = pl.BlockSpec(memory_space=pltpu.VMEM)
    return pl.pallas_call(place_kernel, name="place", out_shape=jax.ShapeDtypeStruct(shape, pieces.dtype), in_specs=[vmem], out_specs=vmem, compiler_params=pltpu.CompilerParams(vmem_limit_bytes=4 * 1024 * 1024))(pieces)


GROUP_ROWS = 16


def attn_kernel(seq_ref, proj_ref, bq_ref, bk_ref, bv_ref, freq_ref, k_ref, v_ref, attn_ref, ko_hbm, vo_hbm, qs, kn, vn, os, pos, patch, out_sem, patch_sem):
    f32, bf = jnp.float32, jnp.bfloat16
    rows, seq = k_ref.shape[0], k_ref.shape[1]
    heads = attn_ref.shape[1] // HEAD
    groups = rows // GROUP_ROWS
    outs = [ko_hbm, vo_hbm]

    def bulk(g):
        part = pl.ds(g * GROUP_ROWS, GROUP_ROWS)
        return [pltpu.make_async_copy(src.at[part], dst.at[part], out_sem.at[i, g]) for i, (src, dst) in enumerate(zip((k_ref, v_ref), outs))]

    for g in range(groups):
        for cp in bulk(g):
            cp.start()
    for b in range(rows):
        pos[b:b + 1, :] = jnp.full((1, HEAD), seq_ref[b], jnp.int32).astype(f32)
    angles = pos[...] * freq_ref[...]
    lower = lax.broadcasted_iota(jnp.int32, (rows, HEAD), 1) < HEAD // 2
    cos_tab = jnp.cos(angles)
    sin_tab = jnp.sin(angles)
    sin_tab = jnp.where(lower, -sin_tab, sin_tab)

    def column(c, bias_ref, k):
        bias = bias_ref[pl.ds(k * HEAD, HEAD)].astype(f32).reshape(1, HEAD)
        return proj_ref[:, c * HEAD:(c + 1) * HEAD] + bias

    def rotate(v):
        return (v * cos_tab + pltpu.roll(v, HEAD // 2, 1) * sin_tab).astype(bf).astype(f32)

    qs[...] = jnp.zeros_like(qs)
    for h in range(heads):
        qs[:, h, :] = rotate(column(h, bq_ref, h))
    kn[...] = rotate(column(heads, bk_ref, 0))
    vn[...] = column(heads + 1, bv_ref, 0).astype(bf).astype(f32)

    def slab_of(b):
        p = seq_ref[b]
        return p, pl.multiple_of((p // 16) * 16, 16)

    def body(g, carry):
        times = lax.broadcasted_iota(jnp.int32, (8, seq), 1)
        slots = lax.broadcasted_iota(jnp.int32, (16, HEAD), 0)
        scores, news, hits = [], [], []
        for r in range(GROUP_ROWS):
            b = g * GROUP_ROWS + r
            p, slab = slab_of(b)
            hit = slots == p - slab
            for i, (cache, new) in enumerate(((k_ref, kn), (v_ref, vn))):
                old = cache[b, pl.ds(slab, 16), :].astype(f32)
                patch[i, b] = jnp.where(hit, new[pl.ds(b, 1), :], old).astype(bf)
            q = qs[b]
            s = lax.dot_general(q.astype(bf), k_ref[b], (((1,), (1,)), ((), ())), preferred_element_type=f32) * HEAD ** -0.5
            s_new = jnp.sum(q * kn[pl.ds(b, 1), :], axis=1, keepdims=True) * HEAD ** -0.5
            hits.append(times == p)
            news.append(s_new)
            scores.append(jnp.where(hits[r], s_new, jnp.where(times < p, s, -jnp.inf)))
        s = jnp.concatenate(scores, axis=0)
        top = jnp.max(s, axis=1, keepdims=True)
        w = jnp.exp(s - top)
        total = jnp.sum(w, axis=1, keepdims=True)
        w_new = jnp.exp(jnp.concatenate(news, axis=0) - top).astype(bf).astype(f32)
        w = jnp.where(jnp.concatenate(hits, axis=0), 0.0, w).astype(bf)
        for r in range(GROUP_ROWS):
            b = g * GROUP_ROWS + r
            part = slice(8 * r, 8 * r + 8)
            o = jnp.dot(w[part], v_ref[b], preferred_element_type=f32) + w_new[part] * vn[pl.ds(b, 1), :]
            os[b] = o / total[part]
        return carry

    lax.fori_loop(0, groups, body, 0)
    for h in range(heads):
        attn_ref[:, h * HEAD:(h + 1) * HEAD] = os[:, h, :].astype(bf)

    def patches(b):
        slab = slab_of(b)[1]
        return [pltpu.make_async_copy(patch.at[i, b], dst.at[b, pl.ds(slab, 16)], patch_sem.at[i]) for i, dst in enumerate(outs)]

    for g in range(groups):
        for cp in bulk(g):
            cp.wait()
        for b in range(g * GROUP_ROWS, (g + 1) * GROUP_ROWS):
            for cp in patches(b):
                cp.start()
    for b in range(rows):
        for cp in patches(b):
            cp.wait()


def attn_call(seq_lens, projected, b_q, b_k, b_v, k_cache, v_cache):
    rows, seq = k_cache.shape[0], k_cache.shape[1]
    f32, bf = jnp.float32, jnp.bfloat16
    freq = (ROPE_THETA ** (-2.0 * np.arange(HEAD // 2) / HEAD)).astype(np.float32)
    freq = jnp.asarray(np.concatenate([freq, freq])[None])
    any_spec, vmem, smem = pl.BlockSpec(memory_space=pl.ANY), pl.BlockSpec(memory_space=pltpu.VMEM), pl.BlockSpec(memory_space=pltpu.SMEM)
    dma = pltpu.SemaphoreType.DMA
    cache = jax.ShapeDtypeStruct((rows, seq, HEAD), bf)
    return pl.pallas_call(
        attn_kernel,
        name="attn",
        out_shape=(jax.ShapeDtypeStruct((rows, b_q.shape[0]), bf), cache, cache),
        in_specs=[smem, vmem, vmem, vmem, vmem, vmem, vmem, vmem],
        out_specs=(vmem, any_spec, any_spec),
        scratch_shapes=[
            pltpu.VMEM((rows, 8, HEAD), f32), pltpu.VMEM((rows, HEAD), f32),
            pltpu.VMEM((rows, HEAD), f32), pltpu.VMEM((rows, 8, HEAD), f32), pltpu.VMEM((rows, HEAD), f32), pltpu.VMEM((2, rows, 16, HEAD), bf),
            dma((2, rows // GROUP_ROWS)), dma((2,)),
        ],
        compiler_params=pltpu.CompilerParams(vmem_limit_bytes=ATTN_LIMIT),
    )(seq_lens, projected, b_q, b_k, b_v, freq, k_cache.reshape(rows, seq, HEAD), v_cache.reshape(rows, seq, HEAD))


def solution(mesh):
    mx_size = mesh.shape["mx"]
    act_spec = P(None, "mx")
    cache_spec = P("mx", None, "my", None)
    in_specs = (act_spec, P("mx"), P("mx"), P("mx"), P("mx", "my"), P("my"), P("mx", "my"), P("my"), P("mx", "my"), P("my"), P("my", "mx"), P("mx", "my"), P("mx", "my"), P("my", "mx"), cache_spec, cache_spec)
    out_specs = (act_spec, cache_spec, cache_spec)

    def local_layer(x_in, seq_lens, gain_attn, gain_mlp, w_q, b_q, w_k, b_k, w_v, b_v, w_o, w_gate, w_up, w_down, k_cache, v_cache):
        hidden = x_in.shape[1] * mx_size
        projected = qkv_call(x_in, gain_attn, w_q, w_k, w_v, hidden)
        attn_rows, k_out, v_out = attn_call(seq_lens, projected, b_q, b_k, b_v, k_cache, v_cache)
        pieces = mlp_call(x_in, gain_mlp, attn_rows, w_o, w_gate.T, w_up.T, w_down, hidden)
        x_out = place_call(pieces, x_in.shape)
        k_cache_out, v_cache_out = k_out.reshape(k_cache.shape), v_out.reshape(v_cache.shape)
        return x_out, k_cache_out, v_cache_out

    return jax.shard_map(local_layer, mesh=mesh, in_specs=in_specs, out_specs=out_specs, check_vma=False)
```

```python
import functools
import types

import jax
import jax.numpy as jnp
import numpy as np
from jax import lax
from jax.experimental import pallas as pl
from jax.experimental.pallas import tpu as pltpu
from jax.sharding import PartitionSpec as P

HEAD = 128
NORM_EPS = 1e-6
ROPE_THETA = 1000000.0
MESH = pl.DeviceIdType.MESH
CHUNK = 512
TILE = 256
DIRECT = 2
ROWS = 64
LAG_B, LAG_C, LAG_D, LAG_E, LAG_M, LAG_F = 1, 4, 7, 8, 3, 8
VMEM_LIMIT = 67043328
MLP_LIMIT = 48 * 1024 * 1024
ATTN_LIMIT = 14 * 1024 * 1024
QKV_LIMIT = 8 * 1024 * 1024


def rcopy(src, dst, send_sem, recv_sem, dev):
    return pltpu.make_async_remote_copy(src_ref=src, dst_ref=dst, send_sem=send_sem, recv_sem=recv_sem, device_id=dev, device_id_type=MESH)


def pinned(x):
    return pltpu.with_memory_space_constraint(x, pltpu.HBM)


def lane_ids():
    return lax.broadcasted_iota(jnp.int32, (8, 128), 1)


def pack_column(blocks):
    tile = jnp.zeros((8, 128), jnp.float32)
    lanes = lane_ids()
    for k, block in enumerate(blocks):
        tile = jnp.where(lanes == k, block, tile)
    return tile


def unpack_column(tile, k):
    return jnp.sum(jnp.where(lane_ids() == k, tile, 0.0), axis=1, keepdims=True)


def qkv_kernel(hidden, x_hbm, gain_hbm, wq_hbm, wk_hbm, wv_hbm, out_ref, gain_ref, x_v, wq_v, wk_v, wv_v, st_own, st_in, nrm, pp, dr, own, xs, xr, ld_sem, send_sem, st_sem, d_sem, x_sem):
    mx = lax.axis_index("mx")
    xi, ci = mx // 2, mx % 2
    partner, xpeer = 2 * xi + (1 - ci), 2 * (1 - xi) + ci
    loads = [pltpu.make_async_copy(s, d, ld_sem.at[i]) for i, (s, d) in enumerate([(x_hbm, x_v), (gain_hbm, gain_ref), (wq_hbm, wq_v), (wk_hbm, wk_v), (wv_hbm, wv_v)])]
    for ld in loads:
        ld.start()
    barrier = pltpu.get_barrier_semaphore()
    for d in range(1, 4):
        pl.semaphore_signal(barrier, inc=1, device_id={"mx": (mx + d) % 4}, device_id_type=MESH)
    with jax.named_scope('q_barrier'):
        pl.semaphore_wait(barrier, 3)

    rows = x_v.shape[0]
    with jax.named_scope('q_xload'):
        loads[0].wait()
    blocks = []
    for k in range(rows // 8):
        v = x_v[8 * k:8 * k + 8, :].astype(jnp.float32)
        blocks.append(jnp.sum(v * v, axis=1, keepdims=True))
    tile = pack_column(blocks)
    st_own[...] = tile
    st_in[mx] = tile
    for d in range(1, 4):
        rcopy(st_own, st_in.at[mx], send_sem.at[0], st_sem, {"mx": (mx + d) % 4}).start()
    with jax.named_scope('q_wload'):
        for ld in loads[1:]:
            ld.wait()
    with jax.named_scope('q_stat'):
        rcopy(st_in.at[pl.ds(0, 3)], st_in.at[pl.ds(0, 3)], send_sem.at[0], st_sem, {"mx": partner}).wait()
    total = st_in[0] + st_in[1] + st_in[2] + st_in[3]
    scale = lax.rsqrt(total / hidden + NORM_EPS)
    gain = gain_ref[...].astype(jnp.float32).reshape(1, x_v.shape[1])
    for k in range(0, rows // 8, 2):
        col = jnp.concatenate([unpack_column(scale, k), unpack_column(scale, k + 1)], axis=0)
        nrm[8 * k:8 * k + 16, :] = (x_v[8 * k:8 * k + 16, :].astype(jnp.float32) * col * gain).astype(jnp.bfloat16)

    lhs = nrm[...]
    part = rows // 4
    width = out_ref.shape[1]
    offs = [0, wq_v.shape[1], wq_v.shape[1] + wk_v.shape[1]]
    pieces = [(w, c0, min(c0 + TILE, w.shape[1]), off) for w, off in zip((wq_v, wk_v, wv_v), offs) for c0 in range(0, w.shape[1], TILE)]
    cut = 2 * TILE
    parts = ((0, cut), (cut, width))

    def swap(i):
        cols = pl.ds(parts[i][0], parts[i][1] - parts[i][0])
        return rcopy(pp.at[1 - ci, :, :, cols], dr.at[:, :, cols], send_sem.at[1], d_sem.at[i], {"mx": partner})

    def cross(i):
        cols = pl.ds(parts[i][0], parts[i][1] - parts[i][0])
        return rcopy(xs.at[:, cols], xr.at[:, cols], send_sem.at[2], x_sem.at[i], {"mx": xpeer})

    for i, (lo, hi) in enumerate(parts):
        for w, c0, c1, off in pieces:
            if lo <= off + c0 < hi:
                r = jnp.dot(lhs, w[:, c0:c1], preferred_element_type=jnp.float32).astype(jnp.bfloat16)
                for m in range(4):
                    pp[m % 2, m // 2, :, off + c0:off + c1] = r[m * part:(m + 1) * part]
        swap(i).start()
    for i, (lo, hi) in enumerate(parts):
        with jax.named_scope('q_d2d'):
            swap(i).wait_recv()
        xs[:, lo:hi] = (pp[ci, 1 - xi, :, lo:hi].astype(jnp.float32) + dr[1 - xi, :, lo:hi].astype(jnp.float32)).astype(jnp.bfloat16)
        cross(i).start()
        own[:, lo:hi] = pp[ci, xi, :, lo:hi].astype(jnp.float32) + dr[xi, :, lo:hi].astype(jnp.float32)
    for i, (lo, hi) in enumerate(parts):
        with jax.named_scope('q_x'):
            cross(i).wait_recv()
        out_ref[:, lo:hi] = own[:, lo:hi] + xr[:, lo:hi].astype(jnp.float32)
    for i in range(2):
        swap(i).wait_send()
        cross(i).wait_send()


def qkv_call(x_in, gain, w_q, w_k, w_v, hidden):
    rows, cols = x_in.shape
    width = w_q.shape[1] + w_k.shape[1] + w_v.shape[1]
    bf, f32 = jnp.bfloat16, jnp.float32
    any_spec, vmem = pl.BlockSpec(memory_space=pl.ANY), pl.BlockSpec(memory_space=pltpu.VMEM)
    part = rows // 4
    return pl.pallas_call(
        functools.partial(qkv_kernel, hidden),
        name="qkv",
        out_shape=jax.ShapeDtypeStruct((part, width), f32),
        in_specs=[any_spec] * 5,
        out_specs=vmem,
        scratch_shapes=[
            pltpu.VMEM(gain.shape, bf),
            pltpu.VMEM((rows, cols), bf), pltpu.VMEM(w_q.shape, bf), pltpu.VMEM(w_k.shape, bf), pltpu.VMEM(w_v.shape, bf),
            pltpu.VMEM((8, 128), f32), pltpu.VMEM((4, 8, 128), f32), pltpu.VMEM((rows, cols), bf),
            pltpu.VMEM((2, 2, part, width), bf), pltpu.VMEM((2, part, width), bf), pltpu.VMEM((part, width), f32),
            pltpu.VMEM((part, width), bf), pltpu.VMEM((part, width), bf),
            pltpu.SemaphoreType.DMA((5,)), pltpu.SemaphoreType.DMA((3,)), pltpu.SemaphoreType.DMA, pltpu.SemaphoreType.DMA((2,)), pltpu.SemaphoreType.DMA((2,)),
        ],
        compiler_params=pltpu.CompilerParams(collective_id=0, has_side_effects=True, vmem_limit_bytes=QKV_LIMIT),
        cost_estimate=pl.CostEstimate(flops=10 ** 10, bytes_accessed=3 * 10 ** 6, transcendentals=0),
    )(pinned(x_in), pinned(gain), pinned(w_q), pinned(w_k), pinned(w_v))


def mlp_kernel(hidden, x_v, gain_ref, attn_ref, wo_v, wg_hbm, wu_hbm, wd_hbm, ag2,
               wg_v, wu_v, wd_v, attn_v, p1, yb1, zs1, zb1, db1, mp, ag1, st_own, st_in, st_sum, st_all, h2,
               pp, dr, own, xs, xr, act, dacc, p2, yb2, zs2, zb2, db2, mo, eye,
               ld_sem, send_sem, at_sem, st_sem, sg_sem, ysem1, zsem1, agz1, agy1, ysem2, zsem2, agz2, agy2, dsem, d_sem, x_sem, ax_sem, ad_sem, af_sem):
    my, mx = lax.axis_index("my"), lax.axis_index("mx")
    n_my = 8
    xi, ci = mx // 2, mx % 2
    zi, yi = my // 2, my % 2
    partner, xpeer = 2 * xi + (1 - ci), 2 * (1 - xi) + ci
    core_dev, x_dev = {"mx": partner}, {"mx": xpeer}
    n_h = h2.shape[0]
    ff = wg_hbm.shape[0]
    n_j = pl.cdiv(ff, CHUNK)
    steps = n_h * n_j
    half = x_v.shape[1] // 2
    brows = attn_ref.shape[0]
    f32, bf = jnp.float32, jnp.bfloat16

    n_k = wg_v.shape[0]
    tiles = [(src.at[:, pl.ds(TILE * k, TILE)], dst.at[k, pl.ds(0, ff)]) for src, dst in ((wg_hbm, wg_v), (wu_hbm, wu_v)) for k in range(n_k)]
    loads = [pltpu.make_async_copy(s, d, ld_sem.at[i]) for i, (s, d) in enumerate(tiles + [(wd_hbm, wd_v.at[pl.ds(0, ff)])])]
    for ld in loads:
        ld.start()
    barrier = pltpu.get_barrier_semaphore()
    for d in range(1, 4):
        pl.semaphore_signal(barrier, inc=1, device_id={"mx": (mx + d) % 4}, device_id_type=MESH)
    for d in range(1, n_my):
        pl.semaphore_signal(barrier, inc=1, device_id={"my": (my + d) % n_my}, device_id_type=MESH)
    with jax.named_scope('m_barrier'):
        pl.semaphore_wait(barrier, 3 + n_my - 1)

    mine = pl.ds(pl.multiple_of(mx * 16, 16), 16)
    for h in range(n_h):
        for d in range(1, 4):
            rcopy(attn_ref.at[pl.ds(16 * h, 16)], attn_v.at[h, mine], send_sem.at[0], at_sem.at[h], {"mx": (mx + d) % 4}).start()
    for h in range(n_h):
        attn_v[h, mine, :] = attn_ref[16 * h:16 * h + 16, :]
    dacc[...] = jnp.zeros_like(dacc)
    wd_v[ff:, :] = jnp.zeros((wd_v.shape[0] - ff, wd_v.shape[1]), bf)
    for w in (wg_v, wu_v):
        for k in range(n_k):
            w[k, ff:, :] = jnp.zeros((w.shape[1] - ff, TILE), bf)
    eye[...] = (lax.broadcasted_iota(jnp.int32, (TILE, TILE), 0) == lax.broadcasted_iota(jnp.int32, (TILE, TILE), 1)).astype(f32).astype(bf)

    zs = (3 - zi, (zi + 2) % 4, zi + 1 - 2 * (zi % 2), zi)
    peers = [2 * z + y for z in zs for y in (1 - yi, yi)][:-1]
    y_peer = 2 * zi + 1 - yi
    y_dev = {"my": y_peer}
    z_devs = [{"my": 2 * z + yi} for z in zs[:3]]

    def project(h):
        with jax.named_scope("m_project"):
            gathered = attn_v.at[h, pl.ds(0, 48)]
            rcopy(gathered, gathered, send_sem.at[0], at_sem.at[h], core_dev).wait_recv()
            for y in range(2):
                r = jnp.dot(attn_v[h], wo_v[:, y * half:(y + 1) * half], preferred_element_type=f32).astype(bf)
                for z in range(4):
                    p1[h, 2 * z + y] = r[16 * z:16 * z + 16]

    def rs_start(r, h):
        with jax.named_scope("m_rs_start"):
            for k, z in enumerate(zs):
                rcopy(r.part.at[h, 2 * z + 1 - yi], r.ybuf.at[h, k], send_sem.at[r.sem], r.ysem.at[h, k], y_dev).start()

    def wait_y(r, h, k):
        rcopy(r.ybuf.at[h, k], r.ybuf.at[h, k], send_sem.at[r.sem], r.ysem.at[h, k], y_dev).wait_recv()

    def rs_mid(r, h):
        with jax.named_scope("m_rs_mid"):
            for k in range(3):
                wait_y(r, h, k)
                r.zsend[h, k] = (r.part[h, 2 * zs[k] + yi].astype(f32) + r.ybuf[h, k].astype(f32)).astype(bf)
                rcopy(r.zsend.at[h, k], r.zbuf.at[h, k], send_sem.at[r.sem + 1], r.zsem.at[h], z_devs[k]).start()

    def rs_fin(r, h, base):
        wait_y(r, h, 3)
        rcopy(r.zbuf.at[h], r.zbuf.at[h], send_sem.at[r.sem + 1], r.zsem.at[h], y_dev).wait_recv()
        total = r.part[h, my].astype(f32) + r.ybuf[h, 3].astype(f32)
        for k in range(3):
            total += r.zbuf[h, k].astype(f32)
        return (base + total).astype(bf)

    def direct_start(r, h):
        with jax.named_scope("m_direct_start"):
            for k, peer in enumerate(peers):
                rcopy(r.part.at[h, peer], r.dbuf.at[k], send_sem.at[2], r.dsem, {"my": peer}).start()

    def direct_fin(r, h, base):
        with jax.named_scope("m_direct_fin"):
            rcopy(r.dbuf, r.dbuf, send_sem.at[2], r.dsem, y_dev).wait_recv()
            total = r.part[h, my].astype(f32)
            for k in range(n_my - 1):
                total += r.dbuf[k].astype(f32)
            return (base + total).astype(bf)

    def ag_start(r, h, val):
        r.piece[h] = val
        r.all[h, my] = val
        for k in range(3):
            rcopy(r.piece.at[h], r.all.at[h, my], send_sem.at[r.sem + 2], r.agz.at[h, k], z_devs[k]).start()
        rcopy(r.piece.at[h], r.all.at[h, my], send_sem.at[r.sem + 2], r.agy.at[h], y_dev).start()

    def ag_mid(r, h):
        with jax.named_scope("m_ag_mid"):
            for k in (2, 1, 0):
                got = r.all.at[h, 2 * zs[k] + yi]
                rcopy(got, got, send_sem.at[r.sem + 2], r.agz.at[h, k], y_dev).wait_recv()
                rcopy(got, got, send_sem.at[r.sem + 2], r.agy.at[h], y_dev).start()

    def ag_fin(r, h):
        with jax.named_scope("m_ag_fin"):
            four = r.all.at[h, pl.ds(0, 4)]
            rcopy(four, four, send_sem.at[r.sem + 2], r.agy.at[h], y_dev).wait_recv()

    one = types.SimpleNamespace(part=p1, ybuf=yb1, zsend=zs1, zbuf=zb1, piece=mp, all=ag1, ysem=ysem1, zsem=zsem1, agz=agz1, agy=agy1, dbuf=db1, dsem=dsem.at[0], sem=9)
    two = types.SimpleNamespace(part=p2, ybuf=yb2, zsend=zs2, zbuf=zb2, piece=mo, all=ag2, ysem=ysem2, zsem=zsem2, agz=agz2, agy=agy2, dbuf=db2, dsem=dsem.at[1], sem=12)

    def rs1_finish(h, fin=rs_fin):
        with jax.named_scope("m_rs1_finish"):
            r0 = pl.multiple_of(zi * brows + h * 16, 16)
            base = x_v[pl.ds(r0, 16), pl.ds(pl.multiple_of(yi * half, 128), half)].astype(f32)
            m = fin(one, h, base)
            ag_start(one, h, m)
            m = m.astype(f32)
            ss = jnp.sum(m * m, axis=1, keepdims=True)
            tile = pack_column([ss[:8], ss[8:]])
            st_own[h] = tile
            st_in[h, mx] = tile
            for d in range(1, 4):
                rcopy(st_own.at[h], st_in.at[h, mx], send_sem.at[3], st_sem.at[h], {"mx": (mx + d) % 4}).start()

    def stat_gather(h):
        with jax.named_scope("m_stat_gather"):
            three = st_in.at[h, pl.ds(0, 3)]
            rcopy(three, three, send_sem.at[3], st_sem.at[h], core_dev).wait_recv()
            total = st_in[h, 0] + st_in[h, 1] + st_in[h, 2] + st_in[h, 3]
            st_sum[h] = total
            st_all[h, my] = total
            for peer in peers:
                rcopy(st_sum.at[h], st_all.at[h, my], send_sem.at[1], sg_sem.at[h], {"my": peer}).start()

    def norm(h):
        with jax.named_scope("m_norm"):
            seven = st_all.at[h, pl.ds(0, n_my - 1)]
            rcopy(seven, seven, send_sem.at[1], sg_sem.at[h], y_dev).wait_recv()
            ag_fin(one, h)
            for z in range(4):
                scale = lax.rsqrt((st_all[h, 2 * z] + st_all[h, 2 * z + 1]) / hidden + NORM_EPS)
                col = jnp.concatenate([unpack_column(scale, 0), unpack_column(scale, 1)], axis=0)
                for y in range(2):
                    gain = gain_ref[pl.ds(y * half, half)].astype(f32).reshape(1, half)
                    h2[h, 16 * z:16 * z + 16, y * half:(y + 1) * half] = (ag1[h, 2 * z + y].astype(f32) * col * gain).astype(bf)

    def transpose(i, carry):
        with jax.named_scope("m_transpose"):
            rows = pl.ds(pl.multiple_of(i * TILE, TILE), TILE)
            for k in range(n_k):
                flipped = [lax.dot_general(eye[...], w[k, rows, :], (((1,), (1,)), ((), ())), preferred_element_type=f32).astype(bf) for w in (wg_v, wu_v)]
                for w, val in zip((wg_v, wu_v), flipped):
                    w[k, rows, :] = val
            return carry

    def stage_a(s):
        with jax.named_scope("m_stage_a"):
            h, j = s // n_j, s % n_j
            lhs = h2[h]
            for i, w in enumerate((wg_v, wu_v)):
                cols = []
                for n in range(CHUNK // TILE):
                    rows = pl.ds(pl.multiple_of(j * CHUNK + n * TILE, TILE), TILE)
                    acc = jnp.dot(lhs[:, :TILE], w[0, rows, :], preferred_element_type=f32)
                    for k in range(1, n_k):
                        acc += jnp.dot(lhs[:, TILE * k:TILE * (k + 1)], w[k, rows, :], preferred_element_type=f32)
                    cols.append(acc.astype(bf))
                val = jnp.concatenate(cols, axis=1)
                for m in range(4):
                    pp[s, m % 2, m // 2, :, i * CHUNK:(i + 1) * CHUNK] = val[16 * m:16 * m + 16]
            rcopy(pp.at[s, 1 - ci], dr.at[s], send_sem.at[4], d_sem.at[s], core_dev).start()

    def stage_b(s):
        with jax.named_scope("m_stage_b"):
            rcopy(pp.at[s, 1 - ci], dr.at[s], send_sem.at[4], d_sem.at[s], core_dev).wait_recv()
            xs[s] = (pp[s, ci, 1 - xi].astype(f32) + dr[s, 1 - xi].astype(f32)).astype(bf)
            rcopy(xs.at[s], xr.at[s], send_sem.at[5], x_sem.at[s], x_dev).start()
            own[s] = pp[s, ci, xi].astype(f32) + dr[s, xi].astype(f32)

    def stage_c(s):
        with jax.named_scope("m_stage_c"):
            rcopy(xs.at[s], xr.at[s], send_sem.at[5], x_sem.at[s], x_dev).wait_recv()
            g = own[s, :, :CHUNK] + xr[s, :, :CHUNK].astype(f32)
            u = own[s, :, CHUNK:] + xr[s, :, CHUNK:].astype(f32)
            act[s, mx] = (jax.nn.silu(g) * u).astype(bf)
            rcopy(act.at[s, mx], act.at[s, mx], send_sem.at[6], ax_sem.at[s], x_dev).start()
            rcopy(act.at[s, mx], act.at[s, mx], send_sem.at[7], ad_sem.at[s], core_dev).start()

            @pl.when(s >= steps - DIRECT)
            def _():
                rcopy(act.at[s, mx], act.at[s, mx], send_sem.at[8], af_sem.at[s], {"mx": 2 * (1 - xi) + (1 - ci)}).start()

    def stage_d(s):
        with jax.named_scope("m_stage_d"):
            rcopy(act.at[s, xpeer], act.at[s, xpeer], send_sem.at[6], ax_sem.at[s], x_dev).wait_recv()

            @pl.when(s < steps - DIRECT)
            def _():
                rcopy(act.at[s, xpeer], act.at[s, xpeer], send_sem.at[8], af_sem.at[s], core_dev).start()

    def stage_e(s):
        with jax.named_scope("m_stage_e"):
            h, j = s // n_j, s % n_j
            rcopy(act.at[s, 0], act.at[s, 0], send_sem.at[7], ad_sem.at[s], core_dev).wait_recv()
            rcopy(act.at[s, 0], act.at[s, 0], send_sem.at[8], af_sem.at[s], core_dev).wait_recv()
            lhs = act[s].reshape(ROWS, CHUNK)
            dacc[h] += jnp.dot(lhs, wd_v[pl.ds(pl.multiple_of(j * CHUNK, CHUNK), CHUNK), :], preferred_element_type=f32)

    def rs2_send(h):
        with jax.named_scope("m_rs2_send"):
            for z in range(4):
                for y in range(2):
                    p2[h, 2 * z + y] = dacc[h, 16 * z:16 * z + 16, y * half:(y + 1) * half].astype(bf)

            @pl.when(h < n_h - 1)
            def _():
                rs_start(two, h)

            @pl.when(h == n_h - 1)
            def _():
                direct_start(two, h)

    def rs2_finish(h, fin=rs_fin):
        with jax.named_scope("m_rs2_finish"):
            ag_start(two, h, fin(two, h, mp[h].astype(f32)))

    n_t = n_j * (CHUNK // TILE)
    def flip(lo, hi):
        lax.fori_loop(lo, hi, transpose, 0)

    project(0)
    direct_start(one, 0)
    project(1)
    rs_start(one, 1)
    project(2)
    for ld in loads[:-1]:
        ld.wait()
    flip(0, 6)
    rs1_finish(0, direct_fin)
    rs_mid(one, 1)
    rs_start(one, 2)
    flip(6, 10)
    stat_gather(0)
    flip(10, 12)
    ag_mid(one, 0)
    rs1_finish(1)
    rs_mid(one, 2)
    flip(12, n_t)
    norm(0)

    def body(t, carry):
        @pl.when(t == n_j)
        def _():
            norm(1)

        @pl.when(t == 2 * n_j)
        def _():
            norm(2)

        @pl.when(t == 1)
        def _():
            stat_gather(1)
            ag_mid(one, 1)

        @pl.when(t == 2)
        def _():
            rs1_finish(2)

        @pl.when(t == 5)
        def _():
            stat_gather(2)

        @pl.when(t == n_j + 1)
        def _():
            ag_mid(one, 2)

        @pl.when(t < steps)
        def _():
            stage_a(t)

        @pl.when((t >= LAG_B) & (t < steps + LAG_B))
        def _():
            stage_b(t - LAG_B)

        @pl.when((t >= LAG_C) & (t < steps + LAG_C))
        def _():
            stage_c(t - LAG_C)

        @pl.when((t >= LAG_D) & (t < steps + LAG_D))
        def _():
            stage_d(t - LAG_D)

        @pl.when(t == LAG_E)
        def _():
            loads[-1].wait()

        @pl.when(t >= LAG_E)
        def _():
            s = t - LAG_E
            stage_e(s)

            @pl.when(s % n_j == n_j - 1)
            def _():
                rs2_send(s // n_j)

        after = t - LAG_E - (n_j - 1)

        @pl.when((after >= LAG_M) & ((after - LAG_M) % n_j == 0))
        def _():
            rs_mid(two, (after - LAG_M) // n_j)

        @pl.when((after >= LAG_F) & ((after - LAG_F) % n_j == 0))
        def _():
            rs2_finish((after - LAG_F) // n_j)

        return carry

    total_t = steps + LAG_E
    lax.fori_loop(0, total_t, body, 0)
    ag_mid(two, 0)
    rs2_finish(1)
    rs2_finish(2, direct_fin)
    ag_mid(two, 1)
    ag_mid(two, 2)
    for h in range(n_h):
        ag_fin(two, h)
    seven = pl.ds(0, n_my - 1)
    for k, ref in ((0, attn_v.at[:, pl.ds(0, 48)]), (1, st_all.at[:, seven]), (3, st_in.at[:, pl.ds(0, 3)]), (4, dr), (5, xs), (6, act.at[:, 0]), (7, act.at[:, 0]), (8, act.at[:, 0]),
                   (9, yb1.at[pl.ds(1, n_h - 1)]), (10, zb1.at[pl.ds(1, n_h - 1)]), (11, ag1.at[:, seven]), (12, yb2.at[pl.ds(0, n_h - 1)]), (13, zb2.at[pl.ds(0, n_h - 1)]), (2, db1), (2, db2), (14, ag2.at[:, seven])):
        rcopy(ref, ref, send_sem.at[k], at_sem.at[0], core_dev).wait_send()


def mlp_call(x_in, gain, attn, w_o, w_gate, w_up, w_down, hidden):
    rows, cols = x_in.shape
    ff = w_gate.shape[0]
    n_j = pl.cdiv(ff, CHUNK)
    n_h = rows // ROWS
    steps = n_h * n_j
    half = cols // 2
    bf, f32 = jnp.bfloat16, jnp.float32
    hbm, vmem = pl.BlockSpec(memory_space=pltpu.HBM), pl.BlockSpec(memory_space=pltpu.VMEM)
    dma = pltpu.SemaphoreType.DMA
    return pl.pallas_call(
        functools.partial(mlp_kernel, hidden),
        name="mlp",
        out_shape=jax.ShapeDtypeStruct((n_h, 8, 16, half), bf),
        in_specs=[vmem, vmem, vmem, vmem, hbm, hbm, hbm],
        out_specs=vmem,
        scratch_shapes=[
            pltpu.VMEM((cols // TILE, n_j * CHUNK, TILE), bf), pltpu.VMEM((cols // TILE, n_j * CHUNK, TILE), bf),
            pltpu.VMEM((n_j * CHUNK, cols), bf), pltpu.VMEM((n_h, 64, attn.shape[1]), bf),
            pltpu.VMEM((n_h, 8, 16, half), bf), pltpu.VMEM((n_h, 4, 16, half), bf), pltpu.VMEM((n_h, 3, 16, half), bf), pltpu.VMEM((n_h, 3, 16, half), bf), pltpu.VMEM((7, 16, half), bf), pltpu.VMEM((n_h, 16, half), bf), pltpu.VMEM((n_h, 8, 16, half), bf),
            pltpu.VMEM((n_h, 8, 128), f32), pltpu.VMEM((n_h, 4, 8, 128), f32), pltpu.VMEM((n_h, 8, 128), f32), pltpu.VMEM((n_h, 8, 8, 128), f32), pltpu.VMEM((n_h, ROWS, cols), bf),
            pltpu.VMEM((steps, 2, 2, 16, 2 * CHUNK), bf), pltpu.VMEM((steps, 2, 16, 2 * CHUNK), bf), pltpu.VMEM((steps, 16, 2 * CHUNK), f32),
            pltpu.VMEM((steps, 16, 2 * CHUNK), bf), pltpu.VMEM((steps, 16, 2 * CHUNK), bf), pltpu.VMEM((steps, 4, 16, CHUNK), bf),
            pltpu.VMEM((n_h, ROWS, cols), f32),
            pltpu.VMEM((n_h, 8, 16, half), bf), pltpu.VMEM((n_h, 4, 16, half), bf), pltpu.VMEM((n_h, 3, 16, half), bf), pltpu.VMEM((n_h, 3, 16, half), bf), pltpu.VMEM((7, 16, half), bf), pltpu.VMEM((n_h, 16, half), bf), pltpu.VMEM((TILE, TILE), bf),
            dma((1 + 2 * (cols // TILE),)), dma((15,)), dma((n_h,)), dma((n_h,)), dma((n_h,)), dma((n_h, 4)), dma((n_h,)), dma((n_h, 3)), dma((n_h,)), dma((n_h, 4)), dma((n_h,)), dma((n_h, 3)), dma((n_h,)), dma((2,)),
            dma((steps,)), dma((steps,)), dma((steps,)), dma((steps,)), dma((steps,)),
        ],
        compiler_params=pltpu.CompilerParams(collective_id=1, has_side_effects=True, vmem_limit_bytes=MLP_LIMIT),
    )(x_in, gain, attn, w_o, pinned(w_gate), pinned(w_up), pinned(w_down))


def place_kernel(pieces_ref, out_ref):
    n_h, _, _, half = pieces_ref.shape
    for h in range(n_h):
        for z in range(4):
            for y in range(2):
                r0 = z * 16 * n_h + h * 16
                out_ref[r0:r0 + 16, y * half:(y + 1) * half] = pieces_ref[h, 2 * z + y]


def place_call(pieces, shape):
    vmem = pl.BlockSpec(memory_space=pltpu.VMEM)
    return pl.pallas_call(place_kernel, name="place", out_shape=jax.ShapeDtypeStruct(shape, pieces.dtype), in_specs=[vmem], out_specs=vmem, compiler_params=pltpu.CompilerParams(vmem_limit_bytes=4 * 1024 * 1024))(pieces)


GROUP_ROWS = 16


def attn_kernel(seq_ref, proj_ref, bq_ref, bk_ref, bv_ref, freq_ref, k_ref, v_ref, attn_ref, ko_hbm, vo_hbm, qs, kn, vn, os, pos, patch, out_sem, patch_sem):
    f32, bf = jnp.float32, jnp.bfloat16
    rows, seq = k_ref.shape[0], k_ref.shape[1]
    heads = attn_ref.shape[1] // HEAD
    groups = rows // GROUP_ROWS
    outs = [ko_hbm, vo_hbm]

    def bulk(g):
        part = pl.ds(g * GROUP_ROWS, GROUP_ROWS)
        return [pltpu.make_async_copy(src.at[part], dst.at[part], out_sem.at[i, g]) for i, (src, dst) in enumerate(zip((k_ref, v_ref), outs))]

    for g in range(groups):
        for cp in bulk(g):
            cp.start()
    for b in range(rows):
        pos[b:b + 1, :] = jnp.full((1, HEAD), seq_ref[b], jnp.int32).astype(f32)
    angles = pos[...] * freq_ref[...]
    lower = lax.broadcasted_iota(jnp.int32, (rows, HEAD), 1) < HEAD // 2
    cos_tab = jnp.cos(angles)
    sin_tab = jnp.sin(angles)
    sin_tab = jnp.where(lower, -sin_tab, sin_tab)

    def column(c, bias_ref, k):
        bias = bias_ref[pl.ds(k * HEAD, HEAD)].astype(f32).reshape(1, HEAD)
        return proj_ref[:, c * HEAD:(c + 1) * HEAD] + bias

    def rotate(v):
        return (v * cos_tab + pltpu.roll(v, HEAD // 2, 1) * sin_tab).astype(bf).astype(f32)

    with jax.named_scope('a_pre'):
        qs[...] = jnp.zeros_like(qs)
    for h in range(heads):
        qs[:, h, :] = rotate(column(h, bq_ref, h))
    kn[...] = rotate(column(heads, bk_ref, 0))
    vn[...] = column(heads + 1, bv_ref, 0).astype(bf).astype(f32)

    def slab_of(b):
        p = seq_ref[b]
        return p, pl.multiple_of((p // 16) * 16, 16)

    def body(g, carry):
        times = lax.broadcasted_iota(jnp.int32, (8, seq), 1)
        slots = lax.broadcasted_iota(jnp.int32, (16, HEAD), 0)
        scores, news, hits = [], [], []
        for r in range(GROUP_ROWS):
            b = g * GROUP_ROWS + r
            p, slab = slab_of(b)
            hit = slots == p - slab
            for i, (cache, new) in enumerate(((k_ref, kn), (v_ref, vn))):
                old = cache[b, pl.ds(slab, 16), :].astype(f32)
                patch[i, b] = jnp.where(hit, new[pl.ds(b, 1), :], old).astype(bf)
            q = qs[b]
            s = lax.dot_general(q.astype(bf), k_ref[b], (((1,), (1,)), ((), ())), preferred_element_type=f32) * HEAD ** -0.5
            s_new = jnp.sum(q * kn[pl.ds(b, 1), :], axis=1, keepdims=True) * HEAD ** -0.5
            hits.append(times == p)
            news.append(s_new)
            scores.append(jnp.where(hits[r], s_new, jnp.where(times < p, s, -jnp.inf)))
        s = jnp.concatenate(scores, axis=0)
        top = jnp.max(s, axis=1, keepdims=True)
        w = jnp.exp(s - top)
        total = jnp.sum(w, axis=1, keepdims=True)
        w_new = jnp.exp(jnp.concatenate(news, axis=0) - top).astype(bf).astype(f32)
        w = jnp.where(jnp.concatenate(hits, axis=0), 0.0, w).astype(bf)
        for r in range(GROUP_ROWS):
            b = g * GROUP_ROWS + r
            part = slice(8 * r, 8 * r + 8)
            o = jnp.dot(w[part], v_ref[b], preferred_element_type=f32) + w_new[part] * vn[pl.ds(b, 1), :]
            os[b] = o / total[part]
        return carry

    with jax.named_scope('a_main'):
        lax.fori_loop(0, groups, body, 0)
    for h in range(heads):
        attn_ref[:, h * HEAD:(h + 1) * HEAD] = os[:, h, :].astype(bf)

    def patches(b):
        slab = slab_of(b)[1]
        return [pltpu.make_async_copy(patch.at[i, b], dst.at[b, pl.ds(slab, 16)], patch_sem.at[i]) for i, dst in enumerate(outs)]

    for g in range(groups):
        with jax.named_scope('a_bulk'):
            for cp in bulk(g):
                cp.wait()
        for b in range(g * GROUP_ROWS, (g + 1) * GROUP_ROWS):
            for cp in patches(b):
                cp.start()
    with jax.named_scope('a_patch'):
        for b in range(rows):
            for cp in patches(b):
                cp.wait()


def attn_call(seq_lens, projected, b_q, b_k, b_v, k_cache, v_cache):
    rows, seq = k_cache.shape[0], k_cache.shape[1]
    f32, bf = jnp.float32, jnp.bfloat16
    freq = (ROPE_THETA ** (-2.0 * np.arange(HEAD // 2) / HEAD)).astype(np.float32)
    freq = jnp.asarray(np.concatenate([freq, freq])[None])
    any_spec, vmem, smem = pl.BlockSpec(memory_space=pl.ANY), pl.BlockSpec(memory_space=pltpu.VMEM), pl.BlockSpec(memory_space=pltpu.SMEM)
    dma = pltpu.SemaphoreType.DMA
    cache = jax.ShapeDtypeStruct((rows, seq, HEAD), bf)
    return pl.pallas_call(
        attn_kernel,
        name="attn",
        out_shape=(jax.ShapeDtypeStruct((rows, b_q.shape[0]), bf), cache, cache),
        in_specs=[smem, vmem, vmem, vmem, vmem, vmem, vmem, vmem],
        out_specs=(vmem, any_spec, any_spec),
        scratch_shapes=[
            pltpu.VMEM((rows, 8, HEAD), f32), pltpu.VMEM((rows, HEAD), f32),
            pltpu.VMEM((rows, HEAD), f32), pltpu.VMEM((rows, 8, HEAD), f32), pltpu.VMEM((rows, HEAD), f32), pltpu.VMEM((2, rows, 16, HEAD), bf),
            dma((2, rows // GROUP_ROWS)), dma((2,)),
        ],
        compiler_params=pltpu.CompilerParams(vmem_limit_bytes=ATTN_LIMIT),
    )(seq_lens, projected, b_q, b_k, b_v, freq, k_cache.reshape(rows, seq, HEAD), v_cache.reshape(rows, seq, HEAD))


def solution(mesh):
    mx_size = mesh.shape["mx"]
    act_spec = P(None, "mx")
    cache_spec = P("mx", None, "my", None)
    in_specs = (act_spec, P("mx"), P("mx"), P("mx"), P("mx", "my"), P("my"), P("mx", "my"), P("my"), P("mx", "my"), P("my"), P("my", "mx"), P("mx", "my"), P("mx", "my"), P("my", "mx"), cache_spec, cache_spec)
    out_specs = (act_spec, cache_spec, cache_spec)

    def local_layer(x_in, seq_lens, gain_attn, gain_mlp, w_q, b_q, w_k, b_k, w_v, b_v, w_o, w_gate, w_up, w_down, k_cache, v_cache):
        hidden = x_in.shape[1] * mx_size
        projected = qkv_call(x_in, gain_attn, w_q, w_k, w_v, hidden)
        attn_rows, k_out, v_out = attn_call(seq_lens, projected, b_q, b_k, b_v, k_cache, v_cache)
        pieces = mlp_call(x_in, gain_mlp, attn_rows, w_o, w_gate.T, w_up.T, w_down, hidden)
        x_out = place_call(pieces, x_in.shape)
        k_cache_out, v_cache_out = k_out.reshape(k_cache.shape), v_out.reshape(v_cache.shape)
        return x_out, k_cache_out, v_cache_out

    return jax.shard_map(local_layer, mesh=mesh, in_specs=in_specs, out_specs=out_specs, check_vma=False)
```

```python
import functools
import types

import jax
import jax.numpy as jnp
import numpy as np
from jax import lax
from jax.experimental import pallas as pl
from jax.experimental.pallas import tpu as pltpu
from jax.sharding import PartitionSpec as P

HEAD = 128
NORM_EPS = 1e-6
ROPE_THETA = 1000000.0
MESH = pl.DeviceIdType.MESH
CHUNK = 512
TILE = 256
DIRECT = 2
ROWS = 64
LAG_B, LAG_C, LAG_D, LAG_E, LAG_M, LAG_F = 1, 4, 7, 8, 4, 8
VMEM_LIMIT = 67043328
MLP_LIMIT = 48 * 1024 * 1024
ATTN_LIMIT = 14 * 1024 * 1024
QKV_LIMIT = 8 * 1024 * 1024


def rcopy(src, dst, send_sem, recv_sem, dev):
    return pltpu.make_async_remote_copy(src_ref=src, dst_ref=dst, send_sem=send_sem, recv_sem=recv_sem, device_id=dev, device_id_type=MESH)


def pinned(x):
    return pltpu.with_memory_space_constraint(x, pltpu.HBM)


def lane_ids():
    return lax.broadcasted_iota(jnp.int32, (8, 128), 1)


def pack_column(blocks):
    tile = jnp.zeros((8, 128), jnp.float32)
    lanes = lane_ids()
    for k, block in enumerate(blocks):
        tile = jnp.where(lanes == k, block, tile)
    return tile


def unpack_column(tile, k):
    return jnp.sum(jnp.where(lane_ids() == k, tile, 0.0), axis=1, keepdims=True)


def qkv_kernel(hidden, x_hbm, gain_hbm, wq_hbm, wk_hbm, wv_hbm, out_ref, gain_ref, x_v, wq_v, wk_v, wv_v, st_own, st_in, nrm, pp, dr, own, xs, xr, ld_sem, send_sem, st_sem, d_sem, x_sem):
    mx = lax.axis_index("mx")
    xi, ci = mx // 2, mx % 2
    partner, xpeer = 2 * xi + (1 - ci), 2 * (1 - xi) + ci
    loads = [pltpu.make_async_copy(s, d, ld_sem.at[i]) for i, (s, d) in enumerate([(x_hbm, x_v), (gain_hbm, gain_ref), (wq_hbm, wq_v), (wk_hbm, wk_v), (wv_hbm, wv_v)])]
    for ld in loads:
        ld.start()
    barrier = pltpu.get_barrier_semaphore()
    for d in range(1, 4):
        pl.semaphore_signal(barrier, inc=1, device_id={"mx": (mx + d) % 4}, device_id_type=MESH)
    pl.semaphore_wait(barrier, 3)

    rows = x_v.shape[0]
    loads[0].wait()
    blocks = []
    for k in range(rows // 8):
        v = x_v[8 * k:8 * k + 8, :].astype(jnp.float32)
        blocks.append(jnp.sum(v * v, axis=1, keepdims=True))
    tile = pack_column(blocks)
    st_own[...] = tile
    st_in[mx] = tile
    for d in range(1, 4):
        rcopy(st_own, st_in.at[mx], send_sem.at[0], st_sem, {"mx": (mx + d) % 4}).start()
    for ld in loads[1:]:
        ld.wait()
    rcopy(st_in.at[pl.ds(0, 3)], st_in.at[pl.ds(0, 3)], send_sem.at[0], st_sem, {"mx": partner}).wait()
    total = st_in[0] + st_in[1] + st_in[2] + st_in[3]
    scale = lax.rsqrt(total / hidden + NORM_EPS)
    gain = gain_ref[...].astype(jnp.float32).reshape(1, x_v.shape[1])
    for k in range(0, rows // 8, 2):
        col = jnp.concatenate([unpack_column(scale, k), unpack_column(scale, k + 1)], axis=0)
        nrm[8 * k:8 * k + 16, :] = (x_v[8 * k:8 * k + 16, :].astype(jnp.float32) * col * gain).astype(jnp.bfloat16)

    lhs = nrm[...]
    part = rows // 4
    width = out_ref.shape[1]
    offs = [0, wq_v.shape[1], wq_v.shape[1] + wk_v.shape[1]]
    pieces = [(w, c0, min(c0 + TILE, w.shape[1]), off) for w, off in zip((wq_v, wk_v, wv_v), offs) for c0 in range(0, w.shape[1], TILE)]
    cut = 2 * TILE
    parts = ((0, cut), (cut, width))

    def swap(i):
        cols = pl.ds(parts[i][0], parts[i][1] - parts[i][0])
        return rcopy(pp.at[1 - ci, :, :, cols], dr.at[:, :, cols], send_sem.at[1], d_sem.at[i], {"mx": partner})

    def cross(i):
        cols = pl.ds(parts[i][0], parts[i][1] - parts[i][0])
        return rcopy(xs.at[:, cols], xr.at[:, cols], send_sem.at[2], x_sem.at[i], {"mx": xpeer})

    for i, (lo, hi) in enumerate(parts):
        for w, c0, c1, off in pieces:
            if lo <= off + c0 < hi:
                r = jnp.dot(lhs, w[:, c0:c1], preferred_element_type=jnp.float32).astype(jnp.bfloat16)
                for m in range(4):
                    pp[m % 2, m // 2, :, off + c0:off + c1] = r[m * part:(m + 1) * part]
        swap(i).start()
    for i, (lo, hi) in enumerate(parts):
        swap(i).wait_recv()
        xs[:, lo:hi] = (pp[ci, 1 - xi, :, lo:hi].astype(jnp.float32) + dr[1 - xi, :, lo:hi].astype(jnp.float32)).astype(jnp.bfloat16)
        cross(i).start()
        own[:, lo:hi] = pp[ci, xi, :, lo:hi].astype(jnp.float32) + dr[xi, :, lo:hi].astype(jnp.float32)
    for i, (lo, hi) in enumerate(parts):
        cross(i).wait_recv()
        out_ref[:, lo:hi] = own[:, lo:hi] + xr[:, lo:hi].astype(jnp.float32)
    for i in range(2):
        swap(i).wait_send()
        cross(i).wait_send()


def qkv_call(x_in, gain, w_q, w_k, w_v, hidden):
    rows, cols = x_in.shape
    width = w_q.shape[1] + w_k.shape[1] + w_v.shape[1]
    bf, f32 = jnp.bfloat16, jnp.float32
    any_spec, vmem = pl.BlockSpec(memory_space=pl.ANY), pl.BlockSpec(memory_space=pltpu.VMEM)
    part = rows // 4
    return pl.pallas_call(
        functools.partial(qkv_kernel, hidden),
        name="qkv",
        out_shape=jax.ShapeDtypeStruct((part, width), f32),
        in_specs=[any_spec] * 5,
        out_specs=vmem,
        scratch_shapes=[
            pltpu.VMEM(gain.shape, bf),
            pltpu.VMEM((rows, cols), bf), pltpu.VMEM(w_q.shape, bf), pltpu.VMEM(w_k.shape, bf), pltpu.VMEM(w_v.shape, bf),
            pltpu.VMEM((8, 128), f32), pltpu.VMEM((4, 8, 128), f32), pltpu.VMEM((rows, cols), bf),
            pltpu.VMEM((2, 2, part, width), bf), pltpu.VMEM((2, part, width), bf), pltpu.VMEM((part, width), f32),
            pltpu.VMEM((part, width), bf), pltpu.VMEM((part, width), bf),
            pltpu.SemaphoreType.DMA((5,)), pltpu.SemaphoreType.DMA((3,)), pltpu.SemaphoreType.DMA, pltpu.SemaphoreType.DMA((2,)), pltpu.SemaphoreType.DMA((2,)),
        ],
        compiler_params=pltpu.CompilerParams(collective_id=0, has_side_effects=True, vmem_limit_bytes=QKV_LIMIT),
        cost_estimate=pl.CostEstimate(flops=10 ** 10, bytes_accessed=3 * 10 ** 6, transcendentals=0),
    )(pinned(x_in), pinned(gain), pinned(w_q), pinned(w_k), pinned(w_v))


def mlp_kernel(hidden, x_v, gain_ref, attn_ref, wo_v, wg_hbm, wu_hbm, wd_hbm, ag2,
               wg_v, wu_v, wd_v, attn_v, p1, yb1, zs1, zb1, db1, mp, ag1, st_own, st_in, st_sum, st_all, h2,
               pp, dr, own, xs, xr, act, dacc, p2, yb2, zs2, zb2, db2, mo, eye,
               ld_sem, send_sem, at_sem, st_sem, sg_sem, ysem1, zsem1, agz1, agy1, ysem2, zsem2, agz2, agy2, dsem, d_sem, x_sem, ax_sem, ad_sem, af_sem):
    my, mx = lax.axis_index("my"), lax.axis_index("mx")
    n_my = 8
    xi, ci = mx // 2, mx % 2
    zi, yi = my // 2, my % 2
    partner, xpeer = 2 * xi + (1 - ci), 2 * (1 - xi) + ci
    core_dev, x_dev = {"mx": partner}, {"mx": xpeer}
    n_h = h2.shape[0]
    ff = wg_hbm.shape[0]
    n_j = pl.cdiv(ff, CHUNK)
    steps = n_h * n_j
    half = x_v.shape[1] // 2
    brows = attn_ref.shape[0]
    f32, bf = jnp.float32, jnp.bfloat16

    n_k = wg_v.shape[0]
    tiles = [(src.at[:, pl.ds(TILE * k, TILE)], dst.at[k, pl.ds(0, ff)]) for src, dst in ((wg_hbm, wg_v), (wu_hbm, wu_v)) for k in range(n_k)]
    loads = [pltpu.make_async_copy(s, d, ld_sem.at[i]) for i, (s, d) in enumerate(tiles + [(wd_hbm, wd_v.at[pl.ds(0, ff)])])]
    for ld in loads:
        ld.start()
    barrier = pltpu.get_barrier_semaphore()
    for d in range(1, 4):
        pl.semaphore_signal(barrier, inc=1, device_id={"mx": (mx + d) % 4}, device_id_type=MESH)
    for d in range(1, n_my):
        pl.semaphore_signal(barrier, inc=1, device_id={"my": (my + d) % n_my}, device_id_type=MESH)
    pl.semaphore_wait(barrier, 3 + n_my - 1)

    mine = pl.ds(pl.multiple_of(mx * 16, 16), 16)
    for h in range(n_h):
        for d in range(1, 4):
            rcopy(attn_ref.at[pl.ds(16 * h, 16)], attn_v.at[h, mine], send_sem.at[0], at_sem.at[h], {"mx": (mx + d) % 4}).start()
    for h in range(n_h):
        attn_v[h, mine, :] = attn_ref[16 * h:16 * h + 16, :]
    dacc[...] = jnp.zeros_like(dacc)
    wd_v[ff:, :] = jnp.zeros((wd_v.shape[0] - ff, wd_v.shape[1]), bf)
    for w in (wg_v, wu_v):
        for k in range(n_k):
            w[k, ff:, :] = jnp.zeros((w.shape[1] - ff, TILE), bf)
    eye[...] = (lax.broadcasted_iota(jnp.int32, (TILE, TILE), 0) == lax.broadcasted_iota(jnp.int32, (TILE, TILE), 1)).astype(f32).astype(bf)

    zs = (3 - zi, (zi + 2) % 4, zi + 1 - 2 * (zi % 2), zi)
    peers = [2 * z + y for z in zs for y in (1 - yi, yi)][:-1]
    y_peer = 2 * zi + 1 - yi
    y_dev = {"my": y_peer}
    z_devs = [{"my": 2 * z + yi} for z in zs[:3]]

    def project(h):
        gathered = attn_v.at[h, pl.ds(0, 48)]
        rcopy(gathered, gathered, send_sem.at[0], at_sem.at[h], core_dev).wait_recv()
        for y in range(2):
            r = jnp.dot(attn_v[h], wo_v[:, y * half:(y + 1) * half], preferred_element_type=f32).astype(bf)
            for z in range(4):
                p1[h, 2 * z + y] = r[16 * z:16 * z + 16]

    def rs_start(r, h):
        for k, z in enumerate(zs):
            rcopy(r.part.at[h, 2 * z + 1 - yi], r.ybuf.at[h, k], send_sem.at[r.sem], r.ysem.at[h, k], y_dev).start()

    def wait_y(r, h, k):
        rcopy(r.ybuf.at[h, k], r.ybuf.at[h, k], send_sem.at[r.sem], r.ysem.at[h, k], y_dev).wait_recv()

    def rs_mid(r, h):
        for k in range(3):
            wait_y(r, h, k)
            r.zsend[h, k] = (r.part[h, 2 * zs[k] + yi].astype(f32) + r.ybuf[h, k].astype(f32)).astype(bf)
            rcopy(r.zsend.at[h, k], r.zbuf.at[h, k], send_sem.at[r.sem + 1], r.zsem.at[h], z_devs[k]).start()

    def rs_fin(r, h, base):
        wait_y(r, h, 3)
        rcopy(r.zbuf.at[h], r.zbuf.at[h], send_sem.at[r.sem + 1], r.zsem.at[h], y_dev).wait_recv()
        total = r.part[h, my].astype(f32) + r.ybuf[h, 3].astype(f32)
        for k in range(3):
            total += r.zbuf[h, k].astype(f32)
        return (base + total).astype(bf)

    def direct_start(r, h):
        for k, peer in enumerate(peers):
            rcopy(r.part.at[h, peer], r.dbuf.at[k], send_sem.at[2], r.dsem, {"my": peer}).start()

    def direct_fin(r, h, base):
        rcopy(r.dbuf, r.dbuf, send_sem.at[2], r.dsem, y_dev).wait_recv()
        total = r.part[h, my].astype(f32)
        for k in range(n_my - 1):
            total += r.dbuf[k].astype(f32)
        return (base + total).astype(bf)

    def ag_start(r, h, val):
        r.piece[h] = val
        r.all[h, my] = val
        for k in range(3):
            rcopy(r.piece.at[h], r.all.at[h, my], send_sem.at[r.sem + 2], r.agz.at[h, k], z_devs[k]).start()
        rcopy(r.piece.at[h], r.all.at[h, my], send_sem.at[r.sem + 2], r.agy.at[h], y_dev).start()

    def ag_mid(r, h):
        for k in (2, 1, 0):
            got = r.all.at[h, 2 * zs[k] + yi]
            rcopy(got, got, send_sem.at[r.sem + 2], r.agz.at[h, k], y_dev).wait_recv()
            rcopy(got, got, send_sem.at[r.sem + 2], r.agy.at[h], y_dev).start()

    def ag_fin(r, h):
        four = r.all.at[h, pl.ds(0, 4)]
        rcopy(four, four, send_sem.at[r.sem + 2], r.agy.at[h], y_dev).wait_recv()

    one = types.SimpleNamespace(part=p1, ybuf=yb1, zsend=zs1, zbuf=zb1, piece=mp, all=ag1, ysem=ysem1, zsem=zsem1, agz=agz1, agy=agy1, dbuf=db1, dsem=dsem.at[0], sem=9)
    two = types.SimpleNamespace(part=p2, ybuf=yb2, zsend=zs2, zbuf=zb2, piece=mo, all=ag2, ysem=ysem2, zsem=zsem2, agz=agz2, agy=agy2, dbuf=db2, dsem=dsem.at[1], sem=12)

    def rs1_finish(h, fin=rs_fin):
        r0 = pl.multiple_of(zi * brows + h * 16, 16)
        base = x_v[pl.ds(r0, 16), pl.ds(pl.multiple_of(yi * half, 128), half)].astype(f32)
        m = fin(one, h, base)
        ag_start(one, h, m)
        m = m.astype(f32)
        ss = jnp.sum(m * m, axis=1, keepdims=True)
        tile = pack_column([ss[:8], ss[8:]])
        st_own[h] = tile
        st_in[h, mx] = tile
        for d in range(1, 4):
            rcopy(st_own.at[h], st_in.at[h, mx], send_sem.at[3], st_sem.at[h], {"mx": (mx + d) % 4}).start()

    def stat_gather(h):
        three = st_in.at[h, pl.ds(0, 3)]
        rcopy(three, three, send_sem.at[3], st_sem.at[h], core_dev).wait_recv()
        total = st_in[h, 0] + st_in[h, 1] + st_in[h, 2] + st_in[h, 3]
        st_sum[h] = total
        st_all[h, my] = total
        for peer in peers:
            rcopy(st_sum.at[h], st_all.at[h, my], send_sem.at[1], sg_sem.at[h], {"my": peer}).start()

    def norm(h):
        seven = st_all.at[h, pl.ds(0, n_my - 1)]
        rcopy(seven, seven, send_sem.at[1], sg_sem.at[h], y_dev).wait_recv()
        ag_fin(one, h)
        for z in range(4):
            scale = lax.rsqrt((st_all[h, 2 * z] + st_all[h, 2 * z + 1]) / hidden + NORM_EPS)
            col = jnp.concatenate([unpack_column(scale, 0), unpack_column(scale, 1)], axis=0)
            for y in range(2):
                gain = gain_ref[pl.ds(y * half, half)].astype(f32).reshape(1, half)
                h2[h, 16 * z:16 * z + 16, y * half:(y + 1) * half] = (ag1[h, 2 * z + y].astype(f32) * col * gain).astype(bf)

    def transpose(i, carry):
        rows = pl.ds(pl.multiple_of(i * TILE, TILE), TILE)
        for k in range(n_k):
            flipped = [lax.dot_general(eye[...], w[k, rows, :], (((1,), (1,)), ((), ())), preferred_element_type=f32).astype(bf) for w in (wg_v, wu_v)]
            for w, val in zip((wg_v, wu_v), flipped):
                w[k, rows, :] = val
        return carry

    def stage_a(s):
        h, j = s // n_j, s % n_j
        lhs = h2[h]
        for i, w in enumerate((wg_v, wu_v)):
            cols = []
            for n in range(CHUNK // TILE):
                rows = pl.ds(pl.multiple_of(j * CHUNK + n * TILE, TILE), TILE)
                acc = jnp.dot(lhs[:, :TILE], w[0, rows, :], preferred_element_type=f32)
                for k in range(1, n_k):
                    acc += jnp.dot(lhs[:, TILE * k:TILE * (k + 1)], w[k, rows, :], preferred_element_type=f32)
                cols.append(acc.astype(bf))
            val = jnp.concatenate(cols, axis=1)
            for m in range(4):
                pp[s, m % 2, m // 2, :, i * CHUNK:(i + 1) * CHUNK] = val[16 * m:16 * m + 16]
        rcopy(pp.at[s, 1 - ci], dr.at[s], send_sem.at[4], d_sem.at[s], core_dev).start()

    def stage_b(s):
        rcopy(pp.at[s, 1 - ci], dr.at[s], send_sem.at[4], d_sem.at[s], core_dev).wait_recv()
        xs[s] = (pp[s, ci, 1 - xi].astype(f32) + dr[s, 1 - xi].astype(f32)).astype(bf)
        rcopy(xs.at[s], xr.at[s], send_sem.at[5], x_sem.at[s], x_dev).start()
        own[s] = pp[s, ci, xi].astype(f32) + dr[s, xi].astype(f32)

    def stage_c(s):
        rcopy(xs.at[s], xr.at[s], send_sem.at[5], x_sem.at[s], x_dev).wait_recv()
        g = own[s, :, :CHUNK] + xr[s, :, :CHUNK].astype(f32)
        u = own[s, :, CHUNK:] + xr[s, :, CHUNK:].astype(f32)
        act[s, mx] = (jax.nn.silu(g) * u).astype(bf)
        rcopy(act.at[s, mx], act.at[s, mx], send_sem.at[6], ax_sem.at[s], x_dev).start()
        rcopy(act.at[s, mx], act.at[s, mx], send_sem.at[7], ad_sem.at[s], core_dev).start()

        @pl.when(s >= steps - DIRECT)
        def _():
            rcopy(act.at[s, mx], act.at[s, mx], send_sem.at[8], af_sem.at[s], {"mx": 2 * (1 - xi) + (1 - ci)}).start()

    def stage_d(s):
        rcopy(act.at[s, xpeer], act.at[s, xpeer], send_sem.at[6], ax_sem.at[s], x_dev).wait_recv()

        @pl.when(s < steps - DIRECT)
        def _():
            rcopy(act.at[s, xpeer], act.at[s, xpeer], send_sem.at[8], af_sem.at[s], core_dev).start()

    def stage_e(s):
        h, j = s // n_j, s % n_j
        rcopy(act.at[s, 0], act.at[s, 0], send_sem.at[7], ad_sem.at[s], core_dev).wait_recv()
        rcopy(act.at[s, 0], act.at[s, 0], send_sem.at[8], af_sem.at[s], core_dev).wait_recv()
        lhs = act[s].reshape(ROWS, CHUNK)
        dacc[h] += jnp.dot(lhs, wd_v[pl.ds(pl.multiple_of(j * CHUNK, CHUNK), CHUNK), :], preferred_element_type=f32)

    def rs2_send(h):
        for z in range(4):
            for y in range(2):
                p2[h, 2 * z + y] = dacc[h, 16 * z:16 * z + 16, y * half:(y + 1) * half].astype(bf)

        @pl.when(h < n_h - 1)
        def _():
            rs_start(two, h)

        @pl.when(h == n_h - 1)
        def _():
            direct_start(two, h)

    def rs2_finish(h, fin=rs_fin):
        ag_start(two, h, fin(two, h, mp[h].astype(f32)))

    n_t = n_j * (CHUNK // TILE)
    def flip(lo, hi):
        lax.fori_loop(lo, hi, transpose, 0)

    project(0)
    direct_start(one, 0)
    project(1)
    rs_start(one, 1)
    project(2)
    for ld in loads[:-1]:
        ld.wait()
    flip(0, 6)
    rs1_finish(0, direct_fin)
    rs_mid(one, 1)
    rs_start(one, 2)
    flip(6, 10)
    stat_gather(0)
    flip(10, 12)
    ag_mid(one, 0)
    rs1_finish(1)
    rs_mid(one, 2)
    flip(12, n_t)
    norm(0)

    def body(t, carry):
        @pl.when(t == n_j)
        def _():
            norm(1)

        @pl.when(t == 2 * n_j)
        def _():
            norm(2)

        @pl.when(t == 2)
        def _():
            stat_gather(1)
            ag_mid(one, 1)

        @pl.when(t == 3)
        def _():
            rs1_finish(2)

        @pl.when(t == 6)
        def _():
            stat_gather(2)

        @pl.when(t == n_j + 1)
        def _():
            ag_mid(one, 2)

        @pl.when(t < steps)
        def _():
            stage_a(t)

        @pl.when((t >= LAG_B) & (t < steps + LAG_B))
        def _():
            stage_b(t - LAG_B)

        @pl.when((t >= LAG_C) & (t < steps + LAG_C))
        def _():
            stage_c(t - LAG_C)

        @pl.when((t >= LAG_D) & (t < steps + LAG_D))
        def _():
            stage_d(t - LAG_D)

        @pl.when(t == LAG_E)
        def _():
            loads[-1].wait()

        @pl.when(t >= LAG_E)
        def _():
            s = t - LAG_E
            stage_e(s)

            @pl.when(s % n_j == n_j - 1)
            def _():
                rs2_send(s // n_j)

        after = t - LAG_E - (n_j - 1)

        @pl.when((after >= LAG_M) & ((after - LAG_M) % n_j == 0))
        def _():
            rs_mid(two, (after - LAG_M) // n_j)

        @pl.when((after >= LAG_F) & ((after - LAG_F) % n_j == 0))
        def _():
            rs2_finish((after - LAG_F) // n_j)

        return carry

    total_t = steps + LAG_E
    lax.fori_loop(0, total_t, body, 0)
    ag_mid(two, 0)
    rs2_finish(1)
    rs2_finish(2, direct_fin)
    ag_mid(two, 1)
    ag_mid(two, 2)
    for h in range(n_h):
        ag_fin(two, h)
    seven = pl.ds(0, n_my - 1)
    for k, ref in ((0, attn_v.at[:, pl.ds(0, 48)]), (1, st_all.at[:, seven]), (3, st_in.at[:, pl.ds(0, 3)]), (4, dr), (5, xs), (6, act.at[:, 0]), (7, act.at[:, 0]), (8, act.at[:, 0]),
                   (9, yb1.at[pl.ds(1, n_h - 1)]), (10, zb1.at[pl.ds(1, n_h - 1)]), (11, ag1.at[:, seven]), (12, yb2.at[pl.ds(0, n_h - 1)]), (13, zb2.at[pl.ds(0, n_h - 1)]), (2, db1), (2, db2), (14, ag2.at[:, seven])):
        rcopy(ref, ref, send_sem.at[k], at_sem.at[0], core_dev).wait_send()


def mlp_call(x_in, gain, attn, w_o, w_gate, w_up, w_down, hidden):
    rows, cols = x_in.shape
    ff = w_gate.shape[0]
    n_j = pl.cdiv(ff, CHUNK)
    n_h = rows // ROWS
    steps = n_h * n_j
    half = cols // 2
    bf, f32 = jnp.bfloat16, jnp.float32
    hbm, vmem = pl.BlockSpec(memory_space=pltpu.HBM), pl.BlockSpec(memory_space=pltpu.VMEM)
    dma = pltpu.SemaphoreType.DMA
    return pl.pallas_call(
        functools.partial(mlp_kernel, hidden),
        name="mlp",
        out_shape=jax.ShapeDtypeStruct((n_h, 8, 16, half), bf),
        in_specs=[vmem, vmem, vmem, vmem, hbm, hbm, hbm],
        out_specs=vmem,
        scratch_shapes=[
            pltpu.VMEM((cols // TILE, n_j * CHUNK, TILE), bf), pltpu.VMEM((cols // TILE, n_j * CHUNK, TILE), bf),
            pltpu.VMEM((n_j * CHUNK, cols), bf), pltpu.VMEM((n_h, 64, attn.shape[1]), bf),
            pltpu.VMEM((n_h, 8, 16, half), bf), pltpu.VMEM((n_h, 4, 16, half), bf), pltpu.VMEM((n_h, 3, 16, half), bf), pltpu.VMEM((n_h, 3, 16, half), bf), pltpu.VMEM((7, 16, half), bf), pltpu.VMEM((n_h, 16, half), bf), pltpu.VMEM((n_h, 8, 16, half), bf),
            pltpu.VMEM((n_h, 8, 128), f32), pltpu.VMEM((n_h, 4, 8, 128), f32), pltpu.VMEM((n_h, 8, 128), f32), pltpu.VMEM((n_h, 8, 8, 128), f32), pltpu.VMEM((n_h, ROWS, cols), bf),
            pltpu.VMEM((steps, 2, 2, 16, 2 * CHUNK), bf), pltpu.VMEM((steps, 2, 16, 2 * CHUNK), bf), pltpu.VMEM((steps, 16, 2 * CHUNK), f32),
            pltpu.VMEM((steps, 16, 2 * CHUNK), bf), pltpu.VMEM((steps, 16, 2 * CHUNK), bf), pltpu.VMEM((steps, 4, 16, CHUNK), bf),
            pltpu.VMEM((n_h, ROWS, cols), f32),
            pltpu.VMEM((n_h, 8, 16, half), bf), pltpu.VMEM((n_h, 4, 16, half), bf), pltpu.VMEM((n_h, 3, 16, half), bf), pltpu.VMEM((n_h, 3, 16, half), bf), pltpu.VMEM((7, 16, half), bf), pltpu.VMEM((n_h, 16, half), bf), pltpu.VMEM((TILE, TILE), bf),
            dma((1 + 2 * (cols // TILE),)), dma((15,)), dma((n_h,)), dma((n_h,)), dma((n_h,)), dma((n_h, 4)), dma((n_h,)), dma((n_h, 3)), dma((n_h,)), dma((n_h, 4)), dma((n_h,)), dma((n_h, 3)), dma((n_h,)), dma((2,)),
            dma((steps,)), dma((steps,)), dma((steps,)), dma((steps,)), dma((steps,)),
        ],
        compiler_params=pltpu.CompilerParams(collective_id=1, has_side_effects=True, vmem_limit_bytes=MLP_LIMIT),
    )(x_in, gain, attn, w_o, pinned(w_gate), pinned(w_up), pinned(w_down))


def place_kernel(pieces_ref, out_ref):
    n_h, _, _, half = pieces_ref.shape
    for h in range(n_h):
        for z in range(4):
            for y in range(2):
                r0 = z * 16 * n_h + h * 16
                out_ref[r0:r0 + 16, y * half:(y + 1) * half] = pieces_ref[h, 2 * z + y]


def place_call(pieces, shape):
    vmem = pl.BlockSpec(memory_space=pltpu.VMEM)
    return pl.pallas_call(place_kernel, name="place", out_shape=jax.ShapeDtypeStruct(shape, pieces.dtype), in_specs=[vmem], out_specs=vmem, compiler_params=pltpu.CompilerParams(vmem_limit_bytes=4 * 1024 * 1024))(pieces)


GROUP_ROWS = 16


def attn_kernel(seq_ref, proj_ref, bq_ref, bk_ref, bv_ref, freq_ref, k_ref, v_ref, attn_ref, ko_hbm, vo_hbm, qs, kn, vn, os, pos, patch, out_sem, patch_sem):
    f32, bf = jnp.float32, jnp.bfloat16
    rows, seq = k_ref.shape[0], k_ref.shape[1]
    heads = attn_ref.shape[1] // HEAD
    groups = rows // GROUP_ROWS
    outs = [ko_hbm, vo_hbm]

    def bulk(g):
        part = pl.ds(g * GROUP_ROWS, GROUP_ROWS)
        return [pltpu.make_async_copy(src.at[part], dst.at[part], out_sem.at[i, g]) for i, (src, dst) in enumerate(zip((k_ref, v_ref), outs))]

    for g in range(groups):
        for cp in bulk(g):
            cp.start()
    for b in range(rows):
        pos[b:b + 1, :] = jnp.full((1, HEAD), seq_ref[b], jnp.int32).astype(f32)
    angles = pos[...] * freq_ref[...]
    lower = lax.broadcasted_iota(jnp.int32, (rows, HEAD), 1) < HEAD // 2
    cos_tab = jnp.cos(angles)
    sin_tab = jnp.sin(angles)
    sin_tab = jnp.where(lower, -sin_tab, sin_tab)

    def column(c, bias_ref, k):
        bias = bias_ref[pl.ds(k * HEAD, HEAD)].astype(f32).reshape(1, HEAD)
        return proj_ref[:, c * HEAD:(c + 1) * HEAD] + bias

    def rotate(v):
        return (v * cos_tab + pltpu.roll(v, HEAD // 2, 1) * sin_tab).astype(bf).astype(f32)

    qs[...] = jnp.zeros_like(qs)
    for h in range(heads):
        qs[:, h, :] = rotate(column(h, bq_ref, h))
    kn[...] = rotate(column(heads, bk_ref, 0))
    vn[...] = column(heads + 1, bv_ref, 0).astype(bf).astype(f32)

    def slab_of(b):
        p = seq_ref[b]
        return p, pl.multiple_of((p // 16) * 16, 16)

    def body(g, carry):
        times = lax.broadcasted_iota(jnp.int32, (8, seq), 1)
        slots = lax.broadcasted_iota(jnp.int32, (16, HEAD), 0)
        scores, news, hits = [], [], []
        for r in range(GROUP_ROWS):
            b = g * GROUP_ROWS + r
            p, slab = slab_of(b)
            hit = slots == p - slab
            for i, (cache, new) in enumerate(((k_ref, kn), (v_ref, vn))):
                old = cache[b, pl.ds(slab, 16), :].astype(f32)
                patch[i, b] = jnp.where(hit, new[pl.ds(b, 1), :], old).astype(bf)
            q = qs[b]
            s = lax.dot_general(q.astype(bf), k_ref[b], (((1,), (1,)), ((), ())), preferred_element_type=f32) * HEAD ** -0.5
            s_new = jnp.sum(q * kn[pl.ds(b, 1), :], axis=1, keepdims=True) * HEAD ** -0.5
            hits.append(times == p)
            news.append(s_new)
            scores.append(jnp.where(hits[r], s_new, jnp.where(times < p, s, -jnp.inf)))
        s = jnp.concatenate(scores, axis=0)
        top = jnp.max(s, axis=1, keepdims=True)
        w = jnp.exp(s - top)
        total = jnp.sum(w, axis=1, keepdims=True)
        w_new = jnp.exp(jnp.concatenate(news, axis=0) - top).astype(bf).astype(f32)
        w = jnp.where(jnp.concatenate(hits, axis=0), 0.0, w).astype(bf)
        for r in range(GROUP_ROWS):
            b = g * GROUP_ROWS + r
            part = slice(8 * r, 8 * r + 8)
            o = jnp.dot(w[part], v_ref[b], preferred_element_type=f32) + w_new[part] * vn[pl.ds(b, 1), :]
            os[b] = o / total[part]
        return carry

    lax.fori_loop(0, groups, body, 0)
    for h in range(heads):
        attn_ref[:, h * HEAD:(h + 1) * HEAD] = os[:, h, :].astype(bf)

    def patches(b):
        slab = slab_of(b)[1]
        return [pltpu.make_async_copy(patch.at[i, b], dst.at[b, pl.ds(slab, 16)], patch_sem.at[i]) for i, dst in enumerate(outs)]

    for g in range(groups):
        for cp in bulk(g):
            cp.wait()
        for b in range(g * GROUP_ROWS, (g + 1) * GROUP_ROWS):
            for cp in patches(b):
                cp.start()
    for b in range(rows):
        for cp in patches(b):
            cp.wait()


def attn_call(seq_lens, projected, b_q, b_k, b_v, k_cache, v_cache):
    rows, seq = k_cache.shape[0], k_cache.shape[1]
    f32, bf = jnp.float32, jnp.bfloat16
    freq = (ROPE_THETA ** (-2.0 * np.arange(HEAD // 2) / HEAD)).astype(np.float32)
    freq = jnp.asarray(np.concatenate([freq, freq])[None])
    any_spec, vmem, smem = pl.BlockSpec(memory_space=pl.ANY), pl.BlockSpec(memory_space=pltpu.VMEM), pl.BlockSpec(memory_space=pltpu.SMEM)
    dma = pltpu.SemaphoreType.DMA
    cache = jax.ShapeDtypeStruct((rows, seq, HEAD), bf)
    return pl.pallas_call(
        attn_kernel,
        name="attn",
        out_shape=(jax.ShapeDtypeStruct((rows, b_q.shape[0]), bf), cache, cache),
        in_specs=[smem, vmem, vmem, vmem, vmem, vmem, vmem, vmem],
        out_specs=(vmem, any_spec, any_spec),
        scratch_shapes=[
            pltpu.VMEM((rows, 8, HEAD), f32), pltpu.VMEM((rows, HEAD), f32),
            pltpu.VMEM((rows, HEAD), f32), pltpu.VMEM((rows, 8, HEAD), f32), pltpu.VMEM((rows, HEAD), f32), pltpu.VMEM((2, rows, 16, HEAD), bf),
            dma((2, rows // GROUP_ROWS)), dma((2,)),
        ],
        compiler_params=pltpu.CompilerParams(vmem_limit_bytes=ATTN_LIMIT),
    )(seq_lens, projected, b_q, b_k, b_v, freq, k_cache.reshape(rows, seq, HEAD), v_cache.reshape(rows, seq, HEAD))


def solution(mesh):
    mx_size = mesh.shape["mx"]
    act_spec = P(None, "mx")
    cache_spec = P("mx", None, "my", None)
    in_specs = (act_spec, P("mx"), P("mx"), P("mx"), P("mx", "my"), P("my"), P("mx", "my"), P("my"), P("mx", "my"), P("my"), P("my", "mx"), P("mx", "my"), P("mx", "my"), P("my", "mx"), cache_spec, cache_spec)
    out_specs = (act_spec, cache_spec, cache_spec)

    def local_layer(x_in, seq_lens, gain_attn, gain_mlp, w_q, b_q, w_k, b_k, w_v, b_v, w_o, w_gate, w_up, w_down, k_cache, v_cache):
        hidden = x_in.shape[1] * mx_size
        projected = qkv_call(x_in, gain_attn, w_q, w_k, w_v, hidden)
        attn_rows, k_out, v_out = attn_call(seq_lens, projected, b_q, b_k, b_v, k_cache, v_cache)
        pieces = mlp_call(x_in, gain_mlp, attn_rows, w_o, w_gate.T, w_up.T, w_down, hidden)
        x_out = place_call(pieces, x_in.shape)
        k_cache_out, v_cache_out = k_out.reshape(k_cache.shape), v_out.reshape(v_cache.shape)
        return x_out, k_cache_out, v_cache_out

    return jax.shard_map(local_layer, mesh=mesh, in_specs=in_specs, out_specs=out_specs, check_vma=False)
```

```python
import functools
import types

import jax
import jax.numpy as jnp
import numpy as np
from jax import lax
from jax.experimental import pallas as pl
from jax.experimental.pallas import tpu as pltpu
from jax.sharding import PartitionSpec as P

HEAD = 128
NORM_EPS = 1e-6
ROPE_THETA = 1000000.0
MESH = pl.DeviceIdType.MESH
CHUNK = 512
TILE = 256
DIRECT = 2
ROWS = 64
LAG_B, LAG_C, LAG_D, LAG_E, LAG_M, LAG_F = 1, 4, 7, 8, 4, 8
VMEM_LIMIT = 67043328
MLP_LIMIT = 48 * 1024 * 1024
ATTN_LIMIT = 14 * 1024 * 1024
QKV_LIMIT = 8 * 1024 * 1024


def rcopy(src, dst, send_sem, recv_sem, dev):
    return pltpu.make_async_remote_copy(src_ref=src, dst_ref=dst, send_sem=send_sem, recv_sem=recv_sem, device_id=dev, device_id_type=MESH)


def pinned(x):
    return pltpu.with_memory_space_constraint(x, pltpu.HBM)


def lane_ids():
    return lax.broadcasted_iota(jnp.int32, (8, 128), 1)


def pack_column(blocks):
    tile = jnp.zeros((8, 128), jnp.float32)
    lanes = lane_ids()
    for k, block in enumerate(blocks):
        tile = jnp.where(lanes == k, block, tile)
    return tile


def unpack_column(tile, k):
    return jnp.sum(jnp.where(lane_ids() == k, tile, 0.0), axis=1, keepdims=True)


def qkv_kernel(hidden, x_hbm, gain_hbm, wq_hbm, wk_hbm, wv_hbm, out_ref, gain_ref, x_v, wq_v, wk_v, wv_v, st_own, st_in, nrm, pp, dr, own, xs, xr, ld_sem, send_sem, st_sem, d_sem, x_sem):
    mx = lax.axis_index("mx")
    xi, ci = mx // 2, mx % 2
    partner, xpeer = 2 * xi + (1 - ci), 2 * (1 - xi) + ci
    loads = [pltpu.make_async_copy(s, d, ld_sem.at[i]) for i, (s, d) in enumerate([(x_hbm, x_v), (gain_hbm, gain_ref), (wq_hbm, wq_v), (wk_hbm, wk_v), (wv_hbm, wv_v)])]
    for ld in loads:
        ld.start()
    barrier = pltpu.get_barrier_semaphore()
    for d in range(1, 4):
        pl.semaphore_signal(barrier, inc=1, device_id={"mx": (mx + d) % 4}, device_id_type=MESH)
    pl.semaphore_wait(barrier, 3)

    rows = x_v.shape[0]
    loads[0].wait()
    blocks = []
    for k in range(rows // 8):
        v = x_v[8 * k:8 * k + 8, :].astype(jnp.float32)
        blocks.append(jnp.sum(v * v, axis=1, keepdims=True))
    tile = pack_column(blocks)
    st_own[...] = tile
    st_in[mx] = tile
    for d in range(1, 4):
        rcopy(st_own, st_in.at[mx], send_sem.at[0], st_sem, {"mx": (mx + d) % 4}).start()
    for ld in loads[1:]:
        ld.wait()
    rcopy(st_in.at[pl.ds(0, 3)], st_in.at[pl.ds(0, 3)], send_sem.at[0], st_sem, {"mx": partner}).wait()
    total = st_in[0] + st_in[1] + st_in[2] + st_in[3]
    scale = lax.rsqrt(total / hidden + NORM_EPS)
    gain = gain_ref[...].astype(jnp.float32).reshape(1, x_v.shape[1])
    for k in range(0, rows // 8, 2):
        col = jnp.concatenate([unpack_column(scale, k), unpack_column(scale, k + 1)], axis=0)
        nrm[8 * k:8 * k + 16, :] = (x_v[8 * k:8 * k + 16, :].astype(jnp.float32) * col * gain).astype(jnp.bfloat16)

    lhs = nrm[...]
    part = rows // 4
    width = out_ref.shape[1]
    offs = [0, wq_v.shape[1], wq_v.shape[1] + wk_v.shape[1]]
    pieces = [(w, c0, min(c0 + TILE, w.shape[1]), off) for w, off in zip((wq_v, wk_v, wv_v), offs) for c0 in range(0, w.shape[1], TILE)]
    cut = 2 * TILE
    parts = ((0, cut), (cut, width))

    def swap(i):
        cols = pl.ds(parts[i][0], parts[i][1] - parts[i][0])
        return rcopy(pp.at[1 - ci, :, :, cols], dr.at[:, :, cols], send_sem.at[1], d_sem.at[i], {"mx": partner})

    def cross(i):
        cols = pl.ds(parts[i][0], parts[i][1] - parts[i][0])
        return rcopy(xs.at[:, cols], xr.at[:, cols], send_sem.at[2], x_sem.at[i], {"mx": xpeer})

    for i, (lo, hi) in enumerate(parts):
        for w, c0, c1, off in pieces:
            if lo <= off + c0 < hi:
                r = jnp.dot(lhs, w[:, c0:c1], preferred_element_type=jnp.float32).astype(jnp.bfloat16)
                for m in range(4):
                    pp[m % 2, m // 2, :, off + c0:off + c1] = r[m * part:(m + 1) * part]
        swap(i).start()
    for i, (lo, hi) in enumerate(parts):
        swap(i).wait_recv()
        xs[:, lo:hi] = (pp[ci, 1 - xi, :, lo:hi].astype(jnp.float32) + dr[1 - xi, :, lo:hi].astype(jnp.float32)).astype(jnp.bfloat16)
        cross(i).start()
        own[:, lo:hi] = pp[ci, xi, :, lo:hi].astype(jnp.float32) + dr[xi, :, lo:hi].astype(jnp.float32)
    for i, (lo, hi) in enumerate(parts):
        cross(i).wait_recv()
        out_ref[:, lo:hi] = own[:, lo:hi] + xr[:, lo:hi].astype(jnp.float32)
    for i in range(2):
        swap(i).wait_send()
        cross(i).wait_send()


def qkv_call(x_in, gain, w_q, w_k, w_v, hidden):
    rows, cols = x_in.shape
    width = w_q.shape[1] + w_k.shape[1] + w_v.shape[1]
    bf, f32 = jnp.bfloat16, jnp.float32
    any_spec, vmem = pl.BlockSpec(memory_space=pl.ANY), pl.BlockSpec(memory_space=pltpu.VMEM)
    part = rows // 4
    return pl.pallas_call(
        functools.partial(qkv_kernel, hidden),
        name="qkv",
        out_shape=jax.ShapeDtypeStruct((part, width), f32),
        in_specs=[any_spec] * 5,
        out_specs=vmem,
        scratch_shapes=[
            pltpu.VMEM(gain.shape, bf),
            pltpu.VMEM((rows, cols), bf), pltpu.VMEM(w_q.shape, bf), pltpu.VMEM(w_k.shape, bf), pltpu.VMEM(w_v.shape, bf),
            pltpu.VMEM((8, 128), f32), pltpu.VMEM((4, 8, 128), f32), pltpu.VMEM((rows, cols), bf),
            pltpu.VMEM((2, 2, part, width), bf), pltpu.VMEM((2, part, width), bf), pltpu.VMEM((part, width), f32),
            pltpu.VMEM((part, width), bf), pltpu.VMEM((part, width), bf),
            pltpu.SemaphoreType.DMA((5,)), pltpu.SemaphoreType.DMA((3,)), pltpu.SemaphoreType.DMA, pltpu.SemaphoreType.DMA((2,)), pltpu.SemaphoreType.DMA((2,)),
        ],
        compiler_params=pltpu.CompilerParams(collective_id=0, has_side_effects=True, vmem_limit_bytes=QKV_LIMIT),
        cost_estimate=pl.CostEstimate(flops=10 ** 10, bytes_accessed=3 * 10 ** 6, transcendentals=0),
    )(pinned(x_in), pinned(gain), pinned(w_q), pinned(w_k), pinned(w_v))


def mlp_kernel(hidden, x_v, gain_ref, attn_ref, wo_v, wg_hbm, wu_hbm, wd_hbm, ag2,
               wg_v, wu_v, wd_v, attn_v, p1, yb1, zs1, zb1, db1, mp, ag1, st_own, st_in, st_sum, st_all, h2,
               pp, dr, own, xs, xr, act, dacc, p2, yb2, zs2, zb2, db2, mo, eye,
               ld_sem, send_sem, at_sem, st_sem, sg_sem, ysem1, zsem1, agz1, agy1, ysem2, zsem2, agz2, agy2, dsem, d_sem, x_sem, ax_sem, ad_sem, af_sem):
    my, mx = lax.axis_index("my"), lax.axis_index("mx")
    n_my = 8
    xi, ci = mx // 2, mx % 2
    zi, yi = my // 2, my % 2
    partner, xpeer = 2 * xi + (1 - ci), 2 * (1 - xi) + ci
    core_dev, x_dev = {"mx": partner}, {"mx": xpeer}
    n_h = h2.shape[0]
    ff = wg_hbm.shape[0]
    n_j = pl.cdiv(ff, CHUNK)
    steps = n_h * n_j
    half = x_v.shape[1] // 2
    brows = attn_ref.shape[0]
    f32, bf = jnp.float32, jnp.bfloat16

    n_k = wg_v.shape[0]
    tiles = [(src.at[:, pl.ds(TILE * k, TILE)], dst.at[k, pl.ds(0, ff)]) for src, dst in ((wg_hbm, wg_v), (wu_hbm, wu_v)) for k in range(n_k)]
    loads = [pltpu.make_async_copy(s, d, ld_sem.at[i]) for i, (s, d) in enumerate(tiles + [(wd_hbm, wd_v.at[pl.ds(0, ff)])])]
    for ld in loads:
        ld.start()
    barrier = pltpu.get_barrier_semaphore()
    for d in range(1, 4):
        pl.semaphore_signal(barrier, inc=1, device_id={"mx": (mx + d) % 4}, device_id_type=MESH)
    for d in range(1, n_my):
        pl.semaphore_signal(barrier, inc=1, device_id={"my": (my + d) % n_my}, device_id_type=MESH)
    pl.semaphore_wait(barrier, 3 + n_my - 1)

    mine = pl.ds(pl.multiple_of(mx * 16, 16), 16)
    for h in range(n_h):
        for d in range(1, 4):
            rcopy(attn_ref.at[pl.ds(16 * h, 16)], attn_v.at[h, mine], send_sem.at[0], at_sem.at[h], {"mx": (mx + d) % 4}).start()
    for h in range(n_h):
        attn_v[h, mine, :] = attn_ref[16 * h:16 * h + 16, :]
    dacc[...] = jnp.zeros_like(dacc)
    wd_v[ff:, :] = jnp.zeros((wd_v.shape[0] - ff, wd_v.shape[1]), bf)
    for w in (wg_v, wu_v):
        for k in range(n_k):
            w[k, ff:, :] = jnp.zeros((w.shape[1] - ff, TILE), bf)
    eye[...] = (lax.broadcasted_iota(jnp.int32, (TILE, TILE), 0) == lax.broadcasted_iota(jnp.int32, (TILE, TILE), 1)).astype(f32).astype(bf)

    zs = (3 - zi, (zi + 2) % 4, zi + 1 - 2 * (zi % 2), zi)
    peers = [2 * z + y for z in zs for y in (1 - yi, yi)][:-1]
    y_peer = 2 * zi + 1 - yi
    y_dev = {"my": y_peer}
    z_devs = [{"my": 2 * z + yi} for z in zs[:3]]

    def project(h):
        gathered = attn_v.at[h, pl.ds(0, 48)]
        rcopy(gathered, gathered, send_sem.at[0], at_sem.at[h], core_dev).wait_recv()
        for y in range(2):
            r = jnp.dot(attn_v[h], wo_v[:, y * half:(y + 1) * half], preferred_element_type=f32).astype(bf)
            for z in range(4):
                p1[h, 2 * z + y] = r[16 * z:16 * z + 16]

    def rs_start(r, h):
        for k, z in enumerate(zs):
            rcopy(r.part.at[h, 2 * z + 1 - yi], r.ybuf.at[h, k], send_sem.at[r.sem], r.ysem.at[h, k], y_dev).start()

    def wait_y(r, h, k):
        rcopy(r.ybuf.at[h, k], r.ybuf.at[h, k], send_sem.at[r.sem], r.ysem.at[h, k], y_dev).wait_recv()

    def rs_mid(r, h):
        for k in range(3):
            wait_y(r, h, k)
            r.zsend[h, k] = (r.part[h, 2 * zs[k] + yi].astype(f32) + r.ybuf[h, k].astype(f32)).astype(bf)
            rcopy(r.zsend.at[h, k], r.zbuf.at[h, k], send_sem.at[r.sem + 1], r.zsem.at[h], z_devs[k]).start()

    def rs_fin(r, h, base):
        wait_y(r, h, 3)
        rcopy(r.zbuf.at[h], r.zbuf.at[h], send_sem.at[r.sem + 1], r.zsem.at[h], y_dev).wait_recv()
        total = r.part[h, my].astype(f32) + r.ybuf[h, 3].astype(f32)
        for k in range(3):
            total += r.zbuf[h, k].astype(f32)
        return (base + total).astype(bf)

    def direct_start(r, h):
        for k, peer in enumerate(peers):
            rcopy(r.part.at[h, peer], r.dbuf.at[k], send_sem.at[2], r.dsem, {"my": peer}).start()

    def direct_fin(r, h, base):
        rcopy(r.dbuf, r.dbuf, send_sem.at[2], r.dsem, y_dev).wait_recv()
        total = r.part[h, my].astype(f32)
        for k in range(n_my - 1):
            total += r.dbuf[k].astype(f32)
        return (base + total).astype(bf)

    def ag_start(r, h, val):
        r.piece[h] = val
        r.all[h, my] = val
        for k in range(3):
            rcopy(r.piece.at[h], r.all.at[h, my], send_sem.at[r.sem + 2], r.agz.at[h, k], z_devs[k]).start()
        rcopy(r.piece.at[h], r.all.at[h, my], send_sem.at[r.sem + 2], r.agy.at[h], y_dev).start()

    def ag_mid(r, h):
        for k in (2, 1, 0):
            got = r.all.at[h, 2 * zs[k] + yi]
            rcopy(got, got, send_sem.at[r.sem + 2], r.agz.at[h, k], y_dev).wait_recv()
            rcopy(got, got, send_sem.at[r.sem + 2], r.agy.at[h], y_dev).start()

    def ag_fin(r, h):
        four = r.all.at[h, pl.ds(0, 4)]
        rcopy(four, four, send_sem.at[r.sem + 2], r.agy.at[h], y_dev).wait_recv()

    one = types.SimpleNamespace(part=p1, ybuf=yb1, zsend=zs1, zbuf=zb1, piece=mp, all=ag1, ysem=ysem1, zsem=zsem1, agz=agz1, agy=agy1, dbuf=db1, dsem=dsem.at[0], sem=9)
    two = types.SimpleNamespace(part=p2, ybuf=yb2, zsend=zs2, zbuf=zb2, piece=mo, all=ag2, ysem=ysem2, zsem=zsem2, agz=agz2, agy=agy2, dbuf=db2, dsem=dsem.at[1], sem=12)

    def rs1_finish(h, fin=rs_fin):
        r0 = pl.multiple_of(zi * brows + h * 16, 16)
        base = x_v[pl.ds(r0, 16), pl.ds(pl.multiple_of(yi * half, 128), half)].astype(f32)
        m = fin(one, h, base)
        ag_start(one, h, m)
        m = m.astype(f32)
        ss = jnp.sum(m * m, axis=1, keepdims=True)
        tile = pack_column([ss[:8], ss[8:]])
        st_own[h] = tile
        st_in[h, mx] = tile
        for d in range(1, 4):
            rcopy(st_own.at[h], st_in.at[h, mx], send_sem.at[3], st_sem.at[h], {"mx": (mx + d) % 4}).start()

    def stat_gather(h):
        three = st_in.at[h, pl.ds(0, 3)]
        rcopy(three, three, send_sem.at[3], st_sem.at[h], core_dev).wait_recv()
        total = st_in[h, 0] + st_in[h, 1] + st_in[h, 2] + st_in[h, 3]
        st_sum[h] = total
        st_all[h, my] = total
        for peer in peers:
            rcopy(st_sum.at[h], st_all.at[h, my], send_sem.at[1], sg_sem.at[h], {"my": peer}).start()

    def norm(h):
        seven = st_all.at[h, pl.ds(0, n_my - 1)]
        rcopy(seven, seven, send_sem.at[1], sg_sem.at[h], y_dev).wait_recv()
        ag_fin(one, h)
        for z in range(4):
            scale = lax.rsqrt((st_all[h, 2 * z] + st_all[h, 2 * z + 1]) / hidden + NORM_EPS)
            col = jnp.concatenate([unpack_column(scale, 0), unpack_column(scale, 1)], axis=0)
            for y in range(2):
                gain = gain_ref[pl.ds(y * half, half)].astype(f32).reshape(1, half)
                h2[h, 16 * z:16 * z + 16, y * half:(y + 1) * half] = (ag1[h, 2 * z + y].astype(f32) * col * gain).astype(bf)

    def transpose(i, carry):
        rows = pl.ds(pl.multiple_of(i * TILE, TILE), TILE)
        for k in range(n_k):
            flipped = [lax.dot_general(eye[...], w[k, rows, :], (((1,), (1,)), ((), ())), preferred_element_type=f32).astype(bf) for w in (wg_v, wu_v)]
            for w, val in zip((wg_v, wu_v), flipped):
                w[k, rows, :] = val
        return carry

    def stage_a(s):
        h, j = s // n_j, s % n_j
        lhs = h2[h]
        for i, w in enumerate((wg_v, wu_v)):
            cols = []
            for n in range(CHUNK // TILE):
                rows = pl.ds(pl.multiple_of(j * CHUNK + n * TILE, TILE), TILE)
                acc = jnp.dot(lhs[:, :TILE], w[0, rows, :], preferred_element_type=f32)
                for k in range(1, n_k):
                    acc += jnp.dot(lhs[:, TILE * k:TILE * (k + 1)], w[k, rows, :], preferred_element_type=f32)
                cols.append(acc.astype(bf))
            val = jnp.concatenate(cols, axis=1)
            for m in range(4):
                pp[s, m % 2, m // 2, :, i * CHUNK:(i + 1) * CHUNK] = val[16 * m:16 * m + 16]
        rcopy(pp.at[s, 1 - ci], dr.at[s], send_sem.at[4], d_sem.at[s], core_dev).start()

    def stage_b(s):
        rcopy(pp.at[s, 1 - ci], dr.at[s], send_sem.at[4], d_sem.at[s], core_dev).wait_recv()
        xs[s] = (pp[s, ci, 1 - xi].astype(f32) + dr[s, 1 - xi].astype(f32)).astype(bf)
        rcopy(xs.at[s], xr.at[s], send_sem.at[5], x_sem.at[s], x_dev).start()
        own[s] = pp[s, ci, xi].astype(f32) + dr[s, xi].astype(f32)

    def stage_c(s):
        rcopy(xs.at[s], xr.at[s], send_sem.at[5], x_sem.at[s], x_dev).wait_recv()
        g = own[s, :, :CHUNK] + xr[s, :, :CHUNK].astype(f32)
        u = own[s, :, CHUNK:] + xr[s, :, CHUNK:].astype(f32)
        act[s, mx] = (jax.nn.silu(g) * u).astype(bf)
        rcopy(act.at[s, mx], act.at[s, mx], send_sem.at[6], ax_sem.at[s], x_dev).start()
        rcopy(act.at[s, mx], act.at[s, mx], send_sem.at[7], ad_sem.at[s], core_dev).start()

        @pl.when(s >= steps - DIRECT)
        def _():
            rcopy(act.at[s, mx], act.at[s, mx], send_sem.at[8], af_sem.at[s], {"mx": 2 * (1 - xi) + (1 - ci)}).start()

    def stage_d(s):
        rcopy(act.at[s, xpeer], act.at[s, xpeer], send_sem.at[6], ax_sem.at[s], x_dev).wait_recv()

        @pl.when(s < steps - DIRECT)
        def _():
            rcopy(act.at[s, xpeer], act.at[s, xpeer], send_sem.at[8], af_sem.at[s], core_dev).start()

    def stage_e(s):
        h, j = s // n_j, s % n_j
        rcopy(act.at[s, 0], act.at[s, 0], send_sem.at[7], ad_sem.at[s], core_dev).wait_recv()
        rcopy(act.at[s, 0], act.at[s, 0], send_sem.at[8], af_sem.at[s], core_dev).wait_recv()
        lhs = act[s].reshape(ROWS, CHUNK)
        dacc[h] += jnp.dot(lhs, wd_v[pl.ds(pl.multiple_of(j * CHUNK, CHUNK), CHUNK), :], preferred_element_type=f32)

    def rs2_send(h):
        for z in range(4):
            for y in range(2):
                p2[h, 2 * z + y] = dacc[h, 16 * z:16 * z + 16, y * half:(y + 1) * half].astype(bf)

        @pl.when(h < n_h - 1)
        def _():
            rs_start(two, h)

        @pl.when(h == n_h - 1)
        def _():
            direct_start(two, h)

    def rs2_finish(h, fin=rs_fin):
        ag_start(two, h, fin(two, h, mp[h].astype(f32)))

    n_t = n_j * (CHUNK // TILE)
    def flip(lo, hi):
        lax.fori_loop(lo, hi, transpose, 0)

    project(0)
    direct_start(one, 0)
    project(1)
    rs_start(one, 1)
    project(2)
    for ld in loads[:-1]:
        ld.wait()
    flip(0, 6)
    rs1_finish(0, direct_fin)
    rs_mid(one, 1)
    rs_start(one, 2)
    flip(6, 10)
    stat_gather(0)
    flip(10, 12)
    ag_mid(one, 0)
    rs1_finish(1)
    rs_mid(one, 2)
    flip(12, n_t)
    norm(0)

    def body(t, carry):
        @pl.when(t == n_j)
        def _():
            norm(1)

        @pl.when(t == 2 * n_j)
        def _():
            norm(2)

        @pl.when(t == 2)
        def _():
            stat_gather(1)
            ag_mid(one, 1)

        @pl.when(t == 3)
        def _():
            rs1_finish(2)

        @pl.when(t == 6)
        def _():
            stat_gather(2)

        @pl.when(t == n_j + 1)
        def _():
            ag_mid(one, 2)

        @pl.when(t < steps)
        def _():
            stage_a(t)

        @pl.when((t >= LAG_B) & (t < steps + LAG_B))
        def _():
            stage_b(t - LAG_B)

        @pl.when((t >= LAG_C) & (t < steps + LAG_C))
        def _():
            stage_c(t - LAG_C)

        @pl.when((t >= LAG_D) & (t < steps + LAG_D))
        def _():
            stage_d(t - LAG_D)

        @pl.when(t == LAG_E)
        def _():
            loads[-1].wait()

        @pl.when(t >= LAG_E)
        def _():
            s = t - LAG_E
            stage_e(s)

            @pl.when(s % n_j == n_j - 1)
            def _():
                rs2_send(s // n_j)

        after = t - LAG_E - (n_j - 1)

        @pl.when((after >= LAG_M) & ((after - LAG_M) % n_j == 0))
        def _():
            rs_mid(two, (after - LAG_M) // n_j)

        @pl.when((after >= LAG_F) & ((after - LAG_F) % n_j == 0))
        def _():
            rs2_finish((after - LAG_F) // n_j)

        return carry

    total_t = steps + LAG_E
    lax.fori_loop(0, total_t, body, 0)
    ag_mid(two, 0)
    rs2_finish(1)
    rs2_finish(2, direct_fin)
    ag_mid(two, 1)
    ag_mid(two, 2)
    for h in range(n_h):
        ag_fin(two, h)
    seven = pl.ds(0, n_my - 1)
    for k, ref in ((0, attn_v.at[:, pl.ds(0, 48)]), (1, st_all.at[:, seven]), (3, st_in.at[:, pl.ds(0, 3)]), (4, dr), (5, xs), (6, act.at[:, 0]), (7, act.at[:, 0]), (8, act.at[:, 0]),
                   (9, yb1.at[pl.ds(1, n_h - 1)]), (10, zb1.at[pl.ds(1, n_h - 1)]), (11, ag1.at[:, seven]), (12, yb2.at[pl.ds(0, n_h - 1)]), (13, zb2.at[pl.ds(0, n_h - 1)]), (2, db1), (2, db2), (14, ag2.at[:, seven])):
        rcopy(ref, ref, send_sem.at[k], at_sem.at[0], core_dev).wait_send()


def mlp_call(x_in, gain, attn, w_o, w_gate, w_up, w_down, hidden):
    rows, cols = x_in.shape
    ff = w_gate.shape[0]
    n_j = pl.cdiv(ff, CHUNK)
    n_h = rows // ROWS
    steps = n_h * n_j
    half = cols // 2
    bf, f32 = jnp.bfloat16, jnp.float32
    hbm, vmem = pl.BlockSpec(memory_space=pltpu.HBM), pl.BlockSpec(memory_space=pltpu.VMEM)
    dma = pltpu.SemaphoreType.DMA
    return pl.pallas_call(
        functools.partial(mlp_kernel, hidden),
        name="mlp",
        out_shape=jax.ShapeDtypeStruct((n_h, 8, 16, half), bf),
        in_specs=[vmem, vmem, vmem, vmem, hbm, hbm, hbm],
        out_specs=vmem,
        scratch_shapes=[
            pltpu.VMEM((cols // TILE, n_j * CHUNK, TILE), bf), pltpu.VMEM((cols // TILE, n_j * CHUNK, TILE), bf),
            pltpu.VMEM((n_j * CHUNK, cols), bf), pltpu.VMEM((n_h, 64, attn.shape[1]), bf),
            pltpu.VMEM((n_h, 8, 16, half), bf), pltpu.VMEM((n_h, 4, 16, half), bf), pltpu.VMEM((n_h, 3, 16, half), bf), pltpu.VMEM((n_h, 3, 16, half), bf), pltpu.VMEM((7, 16, half), bf), pltpu.VMEM((n_h, 16, half), bf), pltpu.VMEM((n_h, 8, 16, half), bf),
            pltpu.VMEM((n_h, 8, 128), f32), pltpu.VMEM((n_h, 4, 8, 128), f32), pltpu.VMEM((n_h, 8, 128), f32), pltpu.VMEM((n_h, 8, 8, 128), f32), pltpu.VMEM((n_h, ROWS, cols), bf),
            pltpu.VMEM((steps, 2, 2, 16, 2 * CHUNK), bf), pltpu.VMEM((steps, 2, 16, 2 * CHUNK), bf), pltpu.VMEM((steps, 16, 2 * CHUNK), f32),
            pltpu.VMEM((steps, 16, 2 * CHUNK), bf), pltpu.VMEM((steps, 16, 2 * CHUNK), bf), pltpu.VMEM((steps, 4, 16, CHUNK), bf),
            pltpu.VMEM((n_h, ROWS, cols), f32),
            pltpu.VMEM((n_h, 8, 16, half), bf), pltpu.VMEM((n_h, 4, 16, half), bf), pltpu.VMEM((n_h, 3, 16, half), bf), pltpu.VMEM((n_h, 3, 16, half), bf), pltpu.VMEM((7, 16, half), bf), pltpu.VMEM((n_h, 16, half), bf), pltpu.VMEM((TILE, TILE), bf),
            dma((1 + 2 * (cols // TILE),)), dma((15,)), dma((n_h,)), dma((n_h,)), dma((n_h,)), dma((n_h, 4)), dma((n_h,)), dma((n_h, 3)), dma((n_h,)), dma((n_h, 4)), dma((n_h,)), dma((n_h, 3)), dma((n_h,)), dma((2,)),
            dma((steps,)), dma((steps,)), dma((steps,)), dma((steps,)), dma((steps,)),
        ],
        compiler_params=pltpu.CompilerParams(collective_id=1, has_side_effects=True, vmem_limit_bytes=MLP_LIMIT),
    )(x_in, gain, attn, w_o, pinned(w_gate), pinned(w_up), pinned(w_down))


def place_kernel(pieces_ref, out_hbm, sem):
    n_h, _, _, half = pieces_ref.shape
    copies = []
    for h in range(n_h):
        for z in range(4):
            for y in range(2):
                r0 = z * 16 * n_h + h * 16
                dst = out_hbm.at[pl.ds(r0, 16), pl.ds(y * half, half)]
                copies.append(pltpu.make_async_copy(pieces_ref.at[h, 2 * z + y], dst, sem.at[len(copies)]))
    for cp in copies:
        cp.start()
    for cp in copies:
        cp.wait()


def place_call(pieces, shape):
    return pl.pallas_call(
        place_kernel,
        name="place",
        out_shape=jax.ShapeDtypeStruct(shape, pieces.dtype),
        in_specs=[pl.BlockSpec(memory_space=pltpu.VMEM)],
        out_specs=pl.BlockSpec(memory_space=pl.ANY),
        scratch_shapes=[pltpu.SemaphoreType.DMA((pieces.shape[0] * pieces.shape[1],))],
        compiler_params=pltpu.CompilerParams(vmem_limit_bytes=4 * 1024 * 1024),
    )(pieces)


GROUP_ROWS = 24


def attn_kernel(seq_ref, proj_ref, bq_ref, bk_ref, bv_ref, freq_ref, k_ref, v_ref, attn_ref, ko_hbm, vo_hbm, qs, kn, vn, os, pos, patch, out_sem, patch_sem):
    f32, bf = jnp.float32, jnp.bfloat16
    rows, seq = k_ref.shape[0], k_ref.shape[1]
    heads = attn_ref.shape[1] // HEAD
    groups = rows // GROUP_ROWS
    outs = [ko_hbm, vo_hbm]

    def bulk(g):
        part = pl.ds(g * GROUP_ROWS, GROUP_ROWS)
        return [pltpu.make_async_copy(src.at[part], dst.at[part], out_sem.at[i, g]) for i, (src, dst) in enumerate(zip((k_ref, v_ref), outs))]

    for g in range(groups):
        for cp in bulk(g):
            cp.start()
    for b in range(rows):
        pos[b:b + 1, :] = jnp.full((1, HEAD), seq_ref[b], jnp.int32).astype(f32)
    angles = pos[...] * freq_ref[...]
    lower = lax.broadcasted_iota(jnp.int32, (rows, HEAD), 1) < HEAD // 2
    cos_tab = jnp.cos(angles)
    sin_tab = jnp.sin(angles)
    sin_tab = jnp.where(lower, -sin_tab, sin_tab)

    def column(c, bias_ref, k):
        bias = bias_ref[pl.ds(k * HEAD, HEAD)].astype(f32).reshape(1, HEAD)
        return proj_ref[:, c * HEAD:(c + 1) * HEAD] + bias

    def rotate(v):
        return (v * cos_tab + pltpu.roll(v, HEAD // 2, 1) * sin_tab).astype(bf).astype(f32)

    qs[...] = jnp.zeros_like(qs)
    for h in range(heads):
        qs[:, h, :] = rotate(column(h, bq_ref, h))
    kn[...] = rotate(column(heads, bk_ref, 0))
    vn[...] = column(heads + 1, bv_ref, 0).astype(bf).astype(f32)

    def slab_of(b):
        p = seq_ref[b]
        return p, pl.multiple_of((p // 16) * 16, 16)

    def body(g, carry):
        times = lax.broadcasted_iota(jnp.int32, (8, seq), 1)
        slots = lax.broadcasted_iota(jnp.int32, (16, HEAD), 0)
        scores, news, hits = [], [], []
        for r in range(GROUP_ROWS):
            b = g * GROUP_ROWS + r
            p, slab = slab_of(b)
            hit = slots == p - slab
            for i, (cache, new) in enumerate(((k_ref, kn), (v_ref, vn))):
                old = cache[b, pl.ds(slab, 16), :].astype(f32)
                patch[i, b] = jnp.where(hit, new[pl.ds(b, 1), :], old).astype(bf)
            q = qs[b]
            s = lax.dot_general(q.astype(bf), k_ref[b], (((1,), (1,)), ((), ())), preferred_element_type=f32) * HEAD ** -0.5
            s_new = jnp.sum(q * kn[pl.ds(b, 1), :], axis=1, keepdims=True) * HEAD ** -0.5
            hits.append(times == p)
            news.append(s_new)
            scores.append(jnp.where(hits[r], s_new, jnp.where(times < p, s, -jnp.inf)))
        s = jnp.concatenate(scores, axis=0)
        top = jnp.max(s, axis=1, keepdims=True)
        w = jnp.exp(s - top)
        total = jnp.sum(w, axis=1, keepdims=True)
        w_new = jnp.exp(jnp.concatenate(news, axis=0) - top).astype(bf).astype(f32)
        w = jnp.where(jnp.concatenate(hits, axis=0), 0.0, w).astype(bf)
        for r in range(GROUP_ROWS):
            b = g * GROUP_ROWS + r
            part = slice(8 * r, 8 * r + 8)
            o = jnp.dot(w[part], v_ref[b], preferred_element_type=f32) + w_new[part] * vn[pl.ds(b, 1), :]
            os[b] = o / total[part]
        return carry

    lax.fori_loop(0, groups, body, 0)
    for h in range(heads):
        attn_ref[:, h * HEAD:(h + 1) * HEAD] = os[:, h, :].astype(bf)

    def patches(b):
        slab = slab_of(b)[1]
        return [pltpu.make_async_copy(patch.at[i, b], dst.at[b, pl.ds(slab, 16)], patch_sem.at[i]) for i, dst in enumerate(outs)]

    for g in range(groups):
        for cp in bulk(g):
            cp.wait()
        for b in range(g * GROUP_ROWS, (g + 1) * GROUP_ROWS):
            for cp in patches(b):
                cp.start()
    for b in range(rows):
        for cp in patches(b):
            cp.wait()


def attn_call(seq_lens, projected, b_q, b_k, b_v, k_cache, v_cache):
    rows, seq = k_cache.shape[0], k_cache.shape[1]
    f32, bf = jnp.float32, jnp.bfloat16
    freq = (ROPE_THETA ** (-2.0 * np.arange(HEAD // 2) / HEAD)).astype(np.float32)
    freq = jnp.asarray(np.concatenate([freq, freq])[None])
    any_spec, vmem, smem = pl.BlockSpec(memory_space=pl.ANY), pl.BlockSpec(memory_space=pltpu.VMEM), pl.BlockSpec(memory_space=pltpu.SMEM)
    dma = pltpu.SemaphoreType.DMA
    cache = jax.ShapeDtypeStruct((rows, seq, HEAD), bf)
    return pl.pallas_call(
        attn_kernel,
        name="attn",
        out_shape=(jax.ShapeDtypeStruct((rows, b_q.shape[0]), bf), cache, cache),
        in_specs=[smem, vmem, vmem, vmem, vmem, vmem, vmem, vmem],
        out_specs=(vmem, any_spec, any_spec),
        scratch_shapes=[
            pltpu.VMEM((rows, 8, HEAD), f32), pltpu.VMEM((rows, HEAD), f32),
            pltpu.VMEM((rows, HEAD), f32), pltpu.VMEM((rows, 8, HEAD), f32), pltpu.VMEM((rows, HEAD), f32), pltpu.VMEM((2, rows, 16, HEAD), bf),
            dma((2, rows // GROUP_ROWS)), dma((2,)),
        ],
        compiler_params=pltpu.CompilerParams(vmem_limit_bytes=ATTN_LIMIT),
    )(seq_lens, projected, b_q, b_k, b_v, freq, k_cache.reshape(rows, seq, HEAD), v_cache.reshape(rows, seq, HEAD))


def solution(mesh):
    mx_size = mesh.shape["mx"]
    act_spec = P(None, "mx")
    cache_spec = P("mx", None, "my", None)
    in_specs = (act_spec, P("mx"), P("mx"), P("mx"), P("mx", "my"), P("my"), P("mx", "my"), P("my"), P("mx", "my"), P("my"), P("my", "mx"), P("mx", "my"), P("mx", "my"), P("my", "mx"), cache_spec, cache_spec)
    out_specs = (act_spec, cache_spec, cache_spec)

    def local_layer(x_in, seq_lens, gain_attn, gain_mlp, w_q, b_q, w_k, b_k, w_v, b_v, w_o, w_gate, w_up, w_down, k_cache, v_cache):
        hidden = x_in.shape[1] * mx_size
        projected = qkv_call(x_in, gain_attn, w_q, w_k, w_v, hidden)
        attn_rows, k_out, v_out = attn_call(seq_lens, projected, b_q, b_k, b_v, k_cache, v_cache)
        pieces = mlp_call(x_in, gain_mlp, attn_rows, w_o, w_gate.T, w_up.T, w_down, hidden)
        x_out = place_call(pieces, x_in.shape)
        k_cache_out, v_cache_out = k_out.reshape(k_cache.shape), v_out.reshape(v_cache.shape)
        return x_out, k_cache_out, v_cache_out

    return jax.shard_map(local_layer, mesh=mesh, in_specs=in_specs, out_specs=out_specs, check_vma=False)
```
